32 devices in a mesh: tm: 8 (over z, y), freq: 4 (over x, core).
Axes of the slice: x: 2, y: 2, z: 4, core: 2. Of those that a mesh axis runs over, the one named last changes fastest.
Arguments:
- snapshots: bfloat16 [4352, 3, 4096], P('tm', None, 'freq'), may hold values from -200 to 200
- block_starts: int32 [32], replicated, may hold values from 0 to 4032, as said below
- freq_index: int32 [16], replicated, may hold values from 0 to 128
Outputs:
- modes: bfloat16 [16, 32, 2, 3, 4096], P(None, None, None, None, ('freq', 'tm'))
- energy: float32 [16], replicated
The draws below stay inside these ranges and needn't reach their ends.
Inputs may be any that keep to these rules, and one draw needn't show every extreme that they name: `block_starts`: block b starts at b * 128 plus between 0 and 64.
All inputs are finite; a program needn't handle non-finite values.
Results may differ from the reference program's by a relative error of at most 0.0085.
Values may be sent and summed in bfloat16 or wider, within the bound.
A program may use at most 64 MiB of HBM per device.

```python
import math
import jax
import jax.numpy as jnp
from jax import lax

NB = 32
NFFT = 256
NF = 16
HOP = 128
JIT = 64
TT = 4352
NSIT = 6
P_DEV = 128
P_SIZE = 4096


def draw_snapshots(key, part):
    key_noise, key_space, key_time = jax.random.split(key, 3)
    rising = jnp.exp(math.log(3.0) * jnp.arange(P_SIZE, dtype=jnp.float32) / P_SIZE)
    space_scale = rising * jnp.exp(jax.random.uniform(key_space, (P_SIZE,), minval=0.0, maxval=math.log(10.0))) / 3.0
    time_scale = jnp.exp(jax.random.uniform(key_time, (TT,), minval=math.log(0.3), maxval=math.log(3.0)))
    values = jnp.clip(jax.random.normal(key_noise, (TT, 3, P_SIZE)), -5.0, 5.0)
    return (values * time_scale[:, None, None] * space_scale[None, None, :]).astype(jnp.bfloat16)


def draw_block_starts(key, part):
    jitter = jax.random.randint(key, (NB,), 0, JIT + 1)
    return (jnp.arange(NB, dtype=jnp.int32) * HOP + jitter).astype(jnp.int32)


def set_ends(drawn, rng, low, top_value):
    dims = drawn.shape
    index_at = [jax.random.randint(jax.random.fold_in(rng, axis), (), 0, dims[axis]) for axis in range(len(dims))]
    drawn = drawn.at[tuple(index_at)].set(low)
    longest = dims.index(max(dims))
    index_at[longest] = (index_at[longest] + 1) % dims[longest]
    return drawn.at[tuple(index_at)].set(top_value)


def setup_inputs(seed: int = 0) -> dict:
    key_list = jax.random.split(jax.random.key(seed), 4)
    return {
        "snapshots": draw_snapshots(jax.random.fold_in(key_list[3], 71), 0),
        "block_starts": draw_block_starts(jax.random.fold_in(key_list[3], 71), 0),
        "freq_index": set_ends(jax.random.randint(key_list[2], (NF,), 0, NFFT // 2 + 1), jax.random.fold_in(key_list[2], 1), 0, (NFFT // 2 + 1) - 1).astype(jnp.int32),
    }


def dft_rows(freq_index):
    times_idx = jnp.arange(NFFT, dtype=jnp.int32)
    phase_int = freq_index[:, None].astype(jnp.int32) * times_idx[None, :] % NFFT
    angles = 2.0 * math.pi / NFFT * phase_int.astype(jnp.float32)
    window = 0.5 - 0.5 * jnp.cos(2.0 * math.pi / NFFT * times_idx.astype(jnp.float32))
    scaling = 1.0 / jnp.sqrt(jnp.sum(window * window))
    cosine = window[None, :] * jnp.cos(angles) * scaling
    sine_rows = -window[None, :] * jnp.sin(angles) * scaling
    return jnp.stack([cosine, sine_rows], 1).reshape(2 * NF, NFFT).astype(jnp.bfloat16)

def block_rows(block_starts):
    return block_starts[:, None].astype(jnp.int32) + jnp.arange(NFFT, dtype=jnp.int32)[None, :]

def matmul_batch(left, right):
    return jnp.einsum('fij,fjk->fik', left, right, precision=lax.Precision.HIGHEST)

def whiten(summed, points):
    gram_re = summed[:, 0]
    gram_im = summed[:, 1]
    top_rows = jnp.concatenate([gram_re, -gram_im], 2)
    low_rows = jnp.concatenate([gram_im, gram_re], 2)
    hermit = jnp.concatenate([top_rows, low_rows], 1)
    frob = jnp.sqrt(lax.optimization_barrier(jnp.sum(hermit * hermit, axis=(1, 2))) + 1e-06)
    identity = jnp.eye(2 * NB, dtype=jnp.float32)[None]
    iterate = hermit / frob[:, None, None]
    inverse = jnp.broadcast_to(identity, hermit.shape)
    for iteration in range(NSIT):
        factor = 1.5 * identity - 0.5 * matmul_batch(inverse, iterate)
        iterate = matmul_batch(iterate, factor)
        inverse = matmul_batch(factor, inverse)
    columns = inverse[:, :, :NB] * jnp.sqrt(6.0 * points / frob)[:, None, None]
    upper = columns[:, :NB]
    lower = columns[:, NB:]
    coefficients = jnp.stack([jnp.stack([upper, -lower], 1), jnp.stack([lower, upper], 1)], 1)
    energy = jnp.trace(gram_re, axis1=1, axis2=2) / (3.0 * NB * points)
    return (coefficients, energy)

def reference(snapshots, block_starts, freq_index):
    dft_table = dft_rows(freq_index).astype(jnp.float32)
    offsets = block_rows(block_starts)
    columns_all = snapshots.reshape(TT, 3 * P_SIZE)
    block_cols = 16 * P_DEV

    def spectra_block(start):
        piece = lax.dynamic_slice_in_dim(columns_all, start, block_cols, 1)
        windows = jnp.take(piece, offsets, axis=0).astype(jnp.float32)
        return jnp.einsum('rt,btn->brn', dft_table, windows, precision=lax.Precision.HIGHEST).astype(jnp.bfloat16)
    starts = jnp.arange(3 * P_SIZE // block_cols, dtype=jnp.int32) * block_cols
    pieces = lax.map(spectra_block, starts)
    spectra = jnp.transpose(pieces, (1, 2, 0, 3)).reshape(NB, NF, 2, 3 * P_SIZE)
    by_freq = jnp.moveaxis(spectra, 1, 0)

    def gram_one(spec_f):
        real_part = spec_f[:, 0].astype(jnp.float32)
        imag_part = spec_f[:, 1].astype(jnp.float32)
        gram_re = jnp.dot(real_part, real_part.T, precision=lax.Precision.HIGHEST) + jnp.dot(imag_part, imag_part.T, precision=lax.Precision.HIGHEST)
        cross_terms = jnp.dot(real_part, imag_part.T, precision=lax.Precision.HIGHEST)
        return jnp.stack([gram_re, cross_terms - cross_terms.T])
    summed = lax.map(gram_one, by_freq)
    coefficients, energy = whiten(summed, float(P_SIZE))
    coef_bf = coefficients.astype(jnp.bfloat16)

    def modes_one(pair):
        coef_f, spec_f = pair
        return jnp.einsum('orbj,brn->jon', coef_f.astype(jnp.float32), spec_f.astype(jnp.float32), precision=lax.Precision.HIGHEST).astype(jnp.bfloat16)
    modes = lax.map(modes_one, (coef_bf, by_freq))
    return (modes.reshape(NF, NB, 2, 3, P_SIZE), energy)
```

```python
import functools
import math

import jax
import jax.numpy as jnp
import numpy as np
from jax import lax
from jax.experimental import pallas as pl
from jax.experimental.pallas import tpu as pltpu
from jax.sharding import PartitionSpec as P

NB = 32
NFFT = 256
NF = 16
NSIT = 6


def for_sending(shard):
    return jax.tree.map(lambda a: a.astype(jnp.bfloat16) if a.dtype == jnp.float32 else a, shard)


def dft_rows(freq_index):
    times_idx = jnp.arange(NFFT, dtype=jnp.int32)
    phase_int = freq_index[:, None] * times_idx[None, :] % NFFT
    angles = 2.0 * math.pi / NFFT * phase_int.astype(jnp.float32)
    window = 0.5 - 0.5 * jnp.cos(2.0 * math.pi / NFFT * times_idx.astype(jnp.float32))
    scaling = 1.0 / jnp.sqrt(jnp.sum(window * window))
    cosine = window[None, :] * jnp.cos(angles) * scaling
    sine_rows = -window[None, :] * jnp.sin(angles) * scaling
    return jnp.stack([cosine, sine_rows], 1).reshape(2 * NF, NFFT).astype(jnp.bfloat16)


def block_rows(block_starts):
    return block_starts[:, None] + jnp.arange(NFFT, dtype=jnp.int32)[None, :]


def matmul_batch(left, right):
    return jnp.einsum("fij,fjk->fik", left, right, precision=lax.Precision.HIGHEST)


def whiten(summed, points):
    gram_re = summed[:, 0]
    gram_im = summed[:, 1]
    top_rows = jnp.concatenate([gram_re, -gram_im], 2)
    low_rows = jnp.concatenate([gram_im, gram_re], 2)
    hermit = jnp.concatenate([top_rows, low_rows], 1)
    frob = jnp.sqrt(jnp.sum(hermit * hermit, axis=(1, 2)) + 1e-06)
    identity = jnp.eye(2 * NB, dtype=jnp.float32)[None]
    iterate = hermit / frob[:, None, None]
    inverse = jnp.broadcast_to(identity, hermit.shape)
    for iteration in range(NSIT):
        factor = 1.5 * identity - 0.5 * matmul_batch(inverse, iterate)
        iterate = matmul_batch(iterate, factor)
        inverse = matmul_batch(factor, inverse)
    columns = inverse[:, :, :NB] * jnp.sqrt(6.0 * points / frob)[:, None, None]
    upper = columns[:, :NB]
    lower = columns[:, NB:]
    coefficients = jnp.stack([jnp.stack([upper, -lower], 1), jnp.stack([lower, upper], 1)], 1)
    energy = jnp.trace(gram_re, axis1=1, axis2=2) / (3.0 * NB * points)
    return (coefficients, energy)


def local(snapshots, block_starts, freq_index):
    dft_table = dft_rows(freq_index)
    offsets = block_rows(block_starts)
    series = lax.all_to_all(snapshots, "tm", split_axis=2, concat_axis=0, tiled=True)
    count = series.shape[1]
    width = series.shape[2]
    columns_all = series.reshape(series.shape[0], count * width)
    windows = jnp.take(columns_all, offsets, axis=0)
    spectra_part = jnp.einsum(
        "rt,btn->rbn", dft_table, windows, preferred_element_type=jnp.float32
    ).astype(jnp.bfloat16)
    spectra = spectra_part.reshape(2 * NF, NB, count, width)
    width = spectra.shape[3]
    points = float(width * lax.axis_size("tm") * lax.axis_size("freq"))
    flat_spec = spectra.reshape(NF, 2, NB, 3 * width)
    real_part = flat_spec[:, 0]
    imag_part = flat_spec[:, 1]
    gram_re = jnp.einsum("fbn,fcn->fbc", real_part, real_part, preferred_element_type=jnp.float32)
    gram_re = gram_re + jnp.einsum(
        "fbn,fcn->fbc", imag_part, imag_part, preferred_element_type=jnp.float32
    )
    cross_terms = jnp.einsum(
        "fbn,fcn->fbc", real_part, imag_part, preferred_element_type=jnp.float32
    )
    partial_gram = jnp.stack([gram_re, cross_terms - jnp.swapaxes(cross_terms, 1, 2)], 1)
    shared = lax.psum_scatter(partial_gram, "freq", scatter_dimension=0, tiled=True)
    shared = lax.psum(shared, "tm")
    coef_part, energy_part = whiten(shared, points)
    coefficients, energy = (
        lax.all_gather(for_sending(coef_part), "freq", axis=0, tiled=True).astype(coef_part.dtype),
        lax.all_gather(for_sending(energy_part), "freq", axis=0, tiled=True).astype(
            energy_part.dtype
        ),
    )
    coef_bf = jnp.transpose(coefficients.astype(jnp.bfloat16), (0, 4, 1, 2, 3))
    modes = jnp.einsum(
        "fjorb,frbn->fjon", coef_bf, flat_spec, preferred_element_type=jnp.float32
    ).astype(jnp.bfloat16)
    return (modes.reshape(NF, NB, 2, 3, width), energy)


MESH = pl.DeviceIdType.MESH
ROWS = 2 * NF
HOP = 128
JIT = 64


def plan(n, rows, total, width):
    if n < 2 or n % 2 or NB % n or total % (2 * NF) or width != 128 or rows % 16:
        return None
    per = NB // n
    if per < 4 or per % 2:
        return None
    slots = per + 4
    whole = [[] for _ in range(slots)]
    shared = [[] for _ in range(slots)]
    holders = []
    for block in range(NB):
        touched = [
            dev for dev in range(n)
            if HOP * block < rows * (dev + 1) and HOP * block + JIT + NFFT > rows * dev
        ]
        holders.append(touched)
        if len(touched) > 2:
            return None
        for dev in touched:
            slot = block - per * dev + 2
            if not 0 <= slot < slots:
                return None
            if len(touched) == 2:
                if (slot < slots // 2) != (dev == touched[1]):
                    return None
                shared[slot].append(dev)
            else:
                whole[slot].append(dev)
    return per, whole, shared, holders


def base_table(freqs_ref):
    row = lax.broadcasted_iota(jnp.int32, (ROWS, NFFT), 0)
    times_idx = lax.broadcasted_iota(jnp.int32, (ROWS, NFFT), 1)
    freqs = jnp.zeros((ROWS, NFFT), jnp.int32)
    for f in range(NF):
        freqs = jnp.where((row >> 1) == f, freqs_ref[f], freqs)
    phase = (freqs * times_idx) & (NFFT - 1)
    angles = 2.0 * math.pi / NFFT * phase.astype(jnp.float32)
    window = 0.5 - 0.5 * jnp.cos(2.0 * math.pi / NFFT * times_idx.astype(jnp.float32))
    hann = 0.5 - 0.5 * np.cos(2.0 * math.pi / NFFT * np.arange(NFFT))
    scaling = np.float32(1.0 / np.sqrt(np.sum(hann * hann)))
    cosine = window * jnp.cos(angles) * scaling
    sine = -window * jnp.sin(angles) * scaling
    return jnp.where((row & 1) == 1, sine, cosine).astype(jnp.bfloat16)


def shifted(base, shift, rows):
    source = lax.broadcasted_iota(jnp.int32, (NFFT, rows), 0)
    target = lax.broadcasted_iota(jnp.int32, (NFFT, rows), 1)
    pick = jnp.where(source - target == shift, 1.0, 0.0).astype(jnp.bfloat16)
    return jnp.dot(base, pick, preferred_element_type=jnp.float32).astype(jnp.bfloat16)


def expanders(spread_ref, mask_ref):
    row = lax.broadcasted_iota(jnp.int32, (NB * 6, 2 * NB), 0)
    col = lax.broadcasted_iota(jnp.int32, (NB * 6, 2 * NB), 1)
    first = 6 * (col & (NB - 1))
    hit = (row >= first) & (row < first + 6) & ((row & 1) == jnp.where(col >= NB, 1, 0))
    spread_ref[...] = jnp.where(hit, 1.0, 0.0).astype(jnp.bfloat16)
    row = lax.broadcasted_iota(jnp.int32, (NB * 6, 6 * NB), 0)
    col = lax.broadcasted_iota(jnp.int32, (NB * 6, 6 * NB), 1)
    pair = row >> 1
    comp = pair - 3 * ((pair * 43691) >> 17)
    part = jnp.where(col >= 4 * NB, 2, jnp.where(col >= 2 * NB, 1, 0))
    mask_ref[...] = jnp.where(comp == part, 1.0, 0.0)


def member(index, devs):
    if not devs:
        return None
    if devs == list(range(devs[0], devs[-1] + 1)):
        return (index >= devs[0]) & (index <= devs[-1])
    hit = index == devs[0]
    for dev in devs[1:]:
        hit = hit | (index == dev)
    return hit


def kernel(n, nf_dev, per, whole, shared, holders, points, x_hbm, starts_hbm, freqs_hbm,
           modes_ref, energy_ref, starts_ref, freqs_ref, t_ref, spread_ref, mask_ref, xv, parts,
           others, sendb, recvb, spec32, spec, gpart, gath, msg, crecv, emsg, erecv, load_sem,
           psend, precv, asend, arecv, gsend, grecv, csend, crcv, esend, ercv):
    tm = lax.axis_index("tm")
    fr = lax.axis_index("freq")
    total = n * nf_dev
    lin = tm * nf_dev + fr
    step, lowest = total // (2 * NF), total // 4
    slots = per + 4
    mine = (lin - lowest) // step
    owns = (lin >= lowest) & (lin < lowest + NF * step) & ((lin - lowest) % step == 0)
    half_n = n // 2
    parity = tm % 2

    def owner(f):
        return lowest + f * step

    def where_is(index):
        return {"tm": index // nf_dev, "freq": index % nf_dev}

    small = pltpu.make_async_copy(freqs_hbm, freqs_ref, load_sem.at[3])
    small.start()
    starts = pltpu.make_async_copy(starts_hbm, starts_ref, load_sem.at[4])
    starts.start()
    for c in range(3):
        pltpu.make_async_copy(x_hbm.at[c], xv.at[c], load_sem.at[c]).start()
    barrier = pltpu.get_barrier_semaphore()

    @pl.loop(1, total)
    def _(k):
        pl.semaphore_signal(barrier, inc=1, device_id=where_is((lin + k) % total), device_id_type=MESH)

    small.wait()
    rows = xv.shape[1]
    base = base_table(freqs_ref)
    starts.wait()
    for slot in range(slots):
        block = per * tm + slot - 2
        start = starts_ref[jnp.clip(block, 0, NB - 1)]
        inside = (block >= 0) & (block < NB)
        shift = jnp.where(inside, rows * tm - start, 4 * (rows + NFFT))
        t_ref[slot * ROWS : (slot + 1) * ROWS, :] = shifted(base, shift, rows)
    expanders(spread_ref, mask_ref)
    width = xv.shape[2]
    pw = width // n
    def exchange(slot):
        low = slot < slots // 2
        there = slot + per if low else slot - per
        return pltpu.make_async_remote_copy(
            src_ref=parts.at[slot, 1 - parity], dst_ref=others.at[there],
            send_sem=psend.at[slot], recv_sem=precv.at[there],
            device_id={"tm": (tm + n - 1) % n if low else (tm + 1) % n, "freq": fr},
            device_id_type=MESH)

    def arrival(slot):
        return pltpu.make_async_remote_copy(
            src_ref=parts.at[slot, 1 - parity], dst_ref=others.at[slot],
            send_sem=psend.at[slot], recv_sem=precv.at[slot],
            device_id={"tm": tm, "freq": fr}, device_id_type=MESH)

    outward = []
    for reach in range(slots // 2):
        outward += [slots // 2 + reach, slots // 2 - 1 - reach]
    inward = [slot + per if slot < slots // 2 else slot - per for slot in outward]

    def compute(first, last):
        for c in range(3):
            part = jnp.dot(t_ref[first * ROWS : last * ROWS, :], xv[c], preferred_element_type=jnp.float32)
            for slot in range(first, last):
                for dest in range(n):
                    at = dest // 2 * pw
                    parts[slot, dest % 2, c, :, at : at + pw] = part[
                        (slot - first) * ROWS : (slot - first + 1) * ROWS, dest * pw : (dest + 1) * pw]

    def send_parts(chosen):
        for slot in chosen:
            if shared[slot]:
                @pl.when(member(tm, shared[slot]))
                def _(slot=slot):
                    exchange(slot).start()

    for c in range(3):
        pltpu.make_async_copy(x_hbm.at[c], xv.at[c], load_sem.at[c]).wait()
    inner = [slot for slot in outward if 2 <= slot < slots - 2]
    compute(2, slots - 2)
    pl.semaphore_wait(barrier, total - 1)
    send_parts(inner)
    compute(0, 2)
    compute(slots - 2, slots)
    send_parts([slot for slot in outward if slot not in inner])

    def scatter(slot, dest):
        return pltpu.make_async_remote_copy(
            src_ref=sendb.at[slot, dest], dst_ref=recvb.at[per * tm + slot - 2],
            send_sem=asend.at[slot, dest], recv_sem=arecv.at[per * tm + slot - 2],
            device_id={"tm": dest, "freq": fr}, device_id_type=MESH)

    def same_side(k):
        return 2 * ((tm // 2 + k) % half_n) + parity

    def other_side(k):
        return 2 * ((tm // 2 + k) % half_n) + 1 - parity

    def finish(slot, side, add):
        for q in range(half_n):
            for c in range(3):
                at = q * pw
                value = parts[slot, side, c, :, at : at + pw]
                if add:
                    value = value + others[slot, c, :, at : at + pw]
                sendb[slot, 2 * q + side, :, c * pw : (c + 1) * pw] = value.astype(jnp.bfloat16)

    def keep(slot):
        recvb[per * tm + slot - 2] = sendb[slot, tm]

    for slot in range(slots):
        if whole[slot]:
            @pl.when(member(tm, whole[slot]))
            def _(slot=slot):
                finish(slot, parity, False)
                finish(slot, 1 - parity, False)

                @pl.loop(1, half_n)
                def _(k):
                    scatter(slot, same_side(k)).start()

                @pl.loop(0, half_n)
                def _(k):
                    scatter(slot, other_side(k)).start()

                keep(slot)

    for slot in inward:
        if shared[slot]:
            @pl.when(member(tm, shared[slot]))
            def _(slot=slot):
                arrival(slot).wait_recv()
                finish(slot, parity, True)

                @pl.loop(1, half_n)
                def _(k):
                    scatter(slot, same_side(k)).start()

                keep(slot)

    ordered = [b for b in range(NB) if len(holders[b]) == 1] + [b for b in range(NB) if len(holders[b]) == 2]
    for block in ordered:
        @pl.when(jnp.logical_not(member(tm, holders[block])))
        def _(block=block):
            pltpu.make_async_remote_copy(
                src_ref=sendb.at[0, 0], dst_ref=recvb.at[block], send_sem=asend.at[0, 0],
                recv_sem=arecv.at[block], device_id={"tm": tm, "freq": fr},
                device_id_type=MESH).wait_recv()

    for block in range(NB):
        values = recvb[block]
        for c in range(3):
            spec32[c, block * ROWS : (block + 1) * ROWS, :] = values[:, c * 128 : (c + 1) * 128].astype(jnp.float32)

    def to_owner(f):
        return pltpu.make_async_remote_copy(
            src_ref=gpart.at[f], dst_ref=gath.at[lin], send_sem=gsend.at[f],
            recv_sem=grecv.at[lin], device_id=where_is(owner(f)), device_id_type=MESH)

    upper = lax.broadcasted_iota(jnp.int32, (NB, NB), 1) >= lax.broadcasted_iota(jnp.int32, (NB, NB), 0)
    for f in range(NF):
        real = [spec32[c, pl.ds(2 * f, NB, stride=ROWS), :].astype(jnp.bfloat16) for c in range(3)]
        imag = [spec32[c, pl.ds(2 * f + 1, NB, stride=ROWS), :].astype(jnp.bfloat16) for c in range(3)]
        for c in range(3):
            spec[f, c * 2 * NB : c * 2 * NB + NB, :] = real[c]
            spec[f, c * 2 * NB + NB : (c + 1) * 2 * NB, :] = imag[c]
        lhs = jnp.concatenate(real + imag, axis=1)
        rhs = jnp.concatenate([lhs, jnp.concatenate(imag + [-v for v in real], axis=1)], axis=0)
        gram = lax.dot_general(lhs, rhs, (((1,), (1,)), ((), ())), preferred_element_type=jnp.float32)
        packed = jnp.where(upper, gram[:, :NB], gram[:, NB:])
        gpart[f] = jnp.concatenate([packed[8 * q : 8 * q + 8] for q in range(NB // 8)], axis=1)
        if f % 4 == 3:
            for sent in range(f - 3, f + 1):
                @pl.when(lin != owner(sent))
                def _(sent=sent):
                    to_owner(sent).start()

    def coef_to(index):
        return pltpu.make_async_remote_copy(
            src_ref=msg, dst_ref=crecv.at[mine], send_sem=csend.at[index],
            recv_sem=crcv.at[mine], device_id=where_is(index), device_id_type=MESH)

    def energy_to(index):
        return pltpu.make_async_remote_copy(
            src_ref=emsg, dst_ref=erecv.at[mine], send_sem=esend.at[index],
            recv_sem=ercv.at[mine], device_id=where_is(index), device_id_type=MESH)

    @pl.when(owns)
    def _():
        gath[lin] = gpart[mine]

        @pl.loop(1, total)
        def _(k):
            src = (lin + k) % total
            pltpu.make_async_remote_copy(
                src_ref=gpart.at[0], dst_ref=gath.at[src], send_sem=gsend.at[0],
                recv_sem=grecv.at[src], device_id=where_is(src), device_id_type=MESH).wait_recv()

        packed = jnp.sum(gath[...], axis=0)
        square = jnp.concatenate([packed[:, q * NB : (q + 1) * NB] for q in range(NB // 8)], axis=0)
        flipped = jnp.transpose(square)
        ri = lax.broadcasted_iota(jnp.int32, (NB, NB), 0)
        ci = lax.broadcasted_iota(jnp.int32, (NB, NB), 1)
        gram_re = jnp.where(ci >= ri, square, flipped)
        gram_im = jnp.where(ci < ri, square, jnp.where(ci > ri, -flipped, 0.0))
        energy = jnp.sum(jnp.where(ri == ci, gram_re, 0.0), axis=(0, 1), keepdims=True) / (3.0 * NB * points)
        emsg[...] = jnp.broadcast_to(energy, (1, 4 * NB))
        erecv[mine] = emsg[...]

        @pl.loop(1, total)
        def _(k):
            energy_to((lin + k) % total).start()

        hermit = jnp.concatenate([
            jnp.concatenate([gram_re, -gram_im, gram_re, -gram_im], axis=1),
            jnp.concatenate([gram_im, gram_re, gram_im, gram_re], axis=1)], axis=0)
        frob = jnp.sqrt(0.5 * jnp.sum(hermit * hermit, axis=(0, 1), keepdims=True) + 1e-06)
        ri = lax.broadcasted_iota(jnp.int32, (2 * NB, 4 * NB), 0)
        ci = lax.broadcasted_iota(jnp.int32, (2 * NB, 4 * NB), 1)
        left = ci < 2 * NB
        identity = jnp.where(ri == (ci & (2 * NB - 1)), 1.0, 0.0).astype(jnp.float32)

        def pieces(a):
            high = a.astype(jnp.bfloat16)
            rest = a - high.astype(jnp.float32)
            mid = rest.astype(jnp.bfloat16)
            return high, mid, (rest - mid.astype(jnp.float32)).astype(jnp.bfloat16)

        def mul(a, b):
            ah, am, al = a
            bh, bm, bl = b
            lhs = jnp.concatenate([ah, am, jnp.where(left[: ah.shape[0]], ah, al)], axis=1)
            rhs = jnp.concatenate([bh, bm, bh, bm, bl, bh], axis=0)
            return jnp.dot(lhs, rhs, preferred_element_type=jnp.float32)

        iterate = hermit / frob
        inverse = identity
        for step in range(NSIT):
            it = pieces(iterate)
            if step:
                inv = pieces(inverse)
            factor = 1.5 * identity - 0.5 * (mul(inv, it) if step else iterate)
            fac = pieces(factor)
            if step < NSIT - 1:
                iterate = mul(it, fac)
                inverse = mul(fac, inv) if step else factor
            else:
                inverse = mul(tuple(piece[:NB] for piece in fac), inv)
        scaled = inverse * jnp.sqrt(6.0 * points / frob)
        msg[...] = jnp.where(left[: NB // 2], scaled[: NB // 2], scaled[NB // 2 :]).astype(jnp.bfloat16)
        crecv[mine] = msg[...]

        @pl.loop(1, total)
        def _(k):
            coef_to((lin + k) % total).start()

    for slot in range(slots):
        if shared[slot]:
            @pl.when(member(tm, shared[slot]))
            def _(slot=slot):
                exchange(slot).wait_send()

                @pl.loop(1, half_n)
                def _(k):
                    scatter(slot, same_side(k)).wait_send()

        if whole[slot]:
            @pl.when(member(tm, whole[slot]))
            def _(slot=slot):
                @pl.loop(1, half_n)
                def _(k):
                    scatter(slot, same_side(k)).wait_send()

                @pl.loop(0, half_n)
                def _(k):
                    scatter(slot, other_side(k)).wait_send()

    for f in range(NF):
        @pl.when(lin != owner(f))
        def _(f=f):
            to_owner(f).wait_send()

    for f in range(NF):
        @pl.when(lin != owner(f))
        def _(f=f):
            pltpu.make_async_remote_copy(
                src_ref=msg, dst_ref=crecv.at[f], send_sem=csend.at[f], recv_sem=crcv.at[f],
                device_id=where_is(owner(f)), device_id_type=MESH).wait_recv()
            pltpu.make_async_remote_copy(
                src_ref=emsg, dst_ref=erecv.at[f], send_sem=esend.at[f], recv_sem=ercv.at[f],
                device_id=where_is(owner(f)), device_id_type=MESH).wait_recv()

    lanes = lax.broadcasted_iota(jnp.int32, (NB, 2 * NB), 1)
    signs = jnp.where(lanes < NB, 1.0, -1.0).astype(jnp.bfloat16)
    wide_lane = lax.broadcasted_iota(jnp.int32, (1, NF), 1)
    energies = jnp.zeros((1, NF), jnp.float32)
    for f in range(NF):
        pairs = crecv[f]
        straight = jnp.concatenate([pairs[:, : 2 * NB], pairs[:, 2 * NB :]], axis=0)
        crossed = jnp.concatenate([straight[:, NB:], straight[:, :NB]], axis=1)
        stacked = jnp.concatenate([straight * signs, crossed], axis=0)
        tiled = jnp.concatenate([stacked] * 3, axis=1)
        full = jnp.dot(spread_ref[...], tiled, preferred_element_type=jnp.float32)
        full = (full * mask_ref[...]).astype(jnp.bfloat16)
        modes_ref[f * 6 * NB : (f + 1) * 6 * NB, :] = jnp.dot(
            full, spec[f], preferred_element_type=jnp.float32).astype(jnp.bfloat16)
        energies = jnp.where(wide_lane == f, erecv[f, :, :NF], energies)
    energy_ref[...] = energies

    @pl.when(owns)
    def _():
        @pl.loop(1, total)
        def _(k):
            coef_to((lin + k) % total).wait_send()
            energy_to((lin + k) % total).wait_send()


def fused(n, nf_dev, chosen, snapshots, block_starts, freq_index):
    per, whole, shared, holders = chosen
    rows, count, wide = snapshots.shape
    total = n * nf_dev
    pw = wide // n
    slots = per + 4
    f32, bf16 = jnp.float32, jnp.bfloat16
    dma = pltpu.SemaphoreType.DMA
    vmem = pl.BlockSpec(memory_space=pltpu.VMEM)
    modes, energy = pl.pallas_call(
        functools.partial(kernel, n, nf_dev, per, whole, shared, holders, float(wide * nf_dev)),
        out_shape=(jax.ShapeDtypeStruct((NF * NB * 6, pw), bf16), jax.ShapeDtypeStruct((1, NF), f32)),
        in_specs=[pl.BlockSpec(memory_space=pltpu.HBM)] * 3,
        out_specs=(vmem, vmem),
        scratch_shapes=[
            pltpu.SMEM((NB,), jnp.int32),
            pltpu.SMEM((NF,), jnp.int32),
            pltpu.VMEM((slots * ROWS, rows), bf16),
            pltpu.VMEM((NB * 6, 2 * NB), bf16),
            pltpu.VMEM((NB * 6, 6 * NB), f32),
            pltpu.VMEM((3, rows, wide), bf16),
            pltpu.VMEM((slots, 2, 3, ROWS, wide // 2), f32),
            pltpu.VMEM((slots, 3, ROWS, wide // 2), f32),
            pltpu.VMEM((slots, n, ROWS, 3 * pw), bf16),
            pltpu.VMEM((NB, ROWS, 3 * pw), bf16),
            pltpu.VMEM((3, NB * ROWS, pw), f32),
            pltpu.VMEM((NF, 6 * NB, pw), bf16),
            pltpu.VMEM((NF, NB // 4, 4 * NB), f32),
            pltpu.VMEM((total, NB // 4, 4 * NB), f32),
            pltpu.VMEM((NB // 2, 4 * NB), bf16),
            pltpu.VMEM((NF, NB // 2, 4 * NB), bf16),
            pltpu.VMEM((1, 4 * NB), f32),
            pltpu.VMEM((NF, 1, 4 * NB), f32),
            dma((5,)), dma((slots,)), dma((slots,)), dma((slots, n)), dma((NB,)),
            dma((NF,)), dma((total,)), dma((total,)), dma((NF,)), dma((total,)), dma((NF,)),
        ],
        compiler_params=pltpu.CompilerParams(
            collective_id=0, has_side_effects=True, vmem_limit_bytes=54_000_000),
    )(jnp.transpose(snapshots, (1, 0, 2)), block_starts, freq_index)
    modes = modes.reshape(NF, NB, 3, 2, pw).transpose(0, 1, 3, 2, 4)
    return modes, energy.reshape(NF)


def solution(mesh):
    n, nf_dev = mesh.shape["tm"], mesh.shape["freq"]

    def body(snapshots, block_starts, freq_index):
        rows, _, wide = snapshots.shape
        chosen = plan(n, rows, n * nf_dev, wide // n)
        if chosen is None:
            return local(snapshots, block_starts, freq_index)
        return fused(n, nf_dev, chosen, snapshots, block_starts, freq_index)

    return jax.shard_map(
        body,
        mesh=mesh,
        in_specs=(P("tm", None, "freq"), P(), P()),
        out_specs=(P(None, None, None, None, ("freq", "tm")), P()),
        check_vma=False,
    )
```

```python
import functools
import math

import jax
import jax.numpy as jnp
import numpy as np
from jax import lax
from jax.experimental import pallas as pl
from jax.experimental.pallas import tpu as pltpu
from jax.sharding import PartitionSpec as P

NB = 32
NFFT = 256
NF = 16
NSIT = 6


def for_sending(shard):
    return jax.tree.map(lambda a: a.astype(jnp.bfloat16) if a.dtype == jnp.float32 else a, shard)


def dft_rows(freq_index):
    times_idx = jnp.arange(NFFT, dtype=jnp.int32)
    phase_int = freq_index[:, None] * times_idx[None, :] % NFFT
    angles = 2.0 * math.pi / NFFT * phase_int.astype(jnp.float32)
    window = 0.5 - 0.5 * jnp.cos(2.0 * math.pi / NFFT * times_idx.astype(jnp.float32))
    scaling = 1.0 / jnp.sqrt(jnp.sum(window * window))
    cosine = window[None, :] * jnp.cos(angles) * scaling
    sine_rows = -window[None, :] * jnp.sin(angles) * scaling
    return jnp.stack([cosine, sine_rows], 1).reshape(2 * NF, NFFT).astype(jnp.bfloat16)


def block_rows(block_starts):
    return block_starts[:, None] + jnp.arange(NFFT, dtype=jnp.int32)[None, :]


def matmul_batch(left, right):
    return jnp.einsum("fij,fjk->fik", left, right, precision=lax.Precision.HIGHEST)


def whiten(summed, points):
    gram_re = summed[:, 0]
    gram_im = summed[:, 1]
    top_rows = jnp.concatenate([gram_re, -gram_im], 2)
    low_rows = jnp.concatenate([gram_im, gram_re], 2)
    hermit = jnp.concatenate([top_rows, low_rows], 1)
    frob = jnp.sqrt(jnp.sum(hermit * hermit, axis=(1, 2)) + 1e-06)
    identity = jnp.eye(2 * NB, dtype=jnp.float32)[None]
    iterate = hermit / frob[:, None, None]
    inverse = jnp.broadcast_to(identity, hermit.shape)
    for iteration in range(NSIT):
        factor = 1.5 * identity - 0.5 * matmul_batch(inverse, iterate)
        iterate = matmul_batch(iterate, factor)
        inverse = matmul_batch(factor, inverse)
    columns = inverse[:, :, :NB] * jnp.sqrt(6.0 * points / frob)[:, None, None]
    upper = columns[:, :NB]
    lower = columns[:, NB:]
    coefficients = jnp.stack([jnp.stack([upper, -lower], 1), jnp.stack([lower, upper], 1)], 1)
    energy = jnp.trace(gram_re, axis1=1, axis2=2) / (3.0 * NB * points)
    return (coefficients, energy)


def local(snapshots, block_starts, freq_index):
    dft_table = dft_rows(freq_index)
    offsets = block_rows(block_starts)
    series = lax.all_to_all(snapshots, "tm", split_axis=2, concat_axis=0, tiled=True)
    count = series.shape[1]
    width = series.shape[2]
    columns_all = series.reshape(series.shape[0], count * width)
    windows = jnp.take(columns_all, offsets, axis=0)
    spectra_part = jnp.einsum(
        "rt,btn->rbn", dft_table, windows, preferred_element_type=jnp.float32
    ).astype(jnp.bfloat16)
    spectra = spectra_part.reshape(2 * NF, NB, count, width)
    width = spectra.shape[3]
    points = float(width * lax.axis_size("tm") * lax.axis_size("freq"))
    flat_spec = spectra.reshape(NF, 2, NB, 3 * width)
    real_part = flat_spec[:, 0]
    imag_part = flat_spec[:, 1]
    gram_re = jnp.einsum("fbn,fcn->fbc", real_part, real_part, preferred_element_type=jnp.float32)
    gram_re = gram_re + jnp.einsum(
        "fbn,fcn->fbc", imag_part, imag_part, preferred_element_type=jnp.float32
    )
    cross_terms = jnp.einsum(
        "fbn,fcn->fbc", real_part, imag_part, preferred_element_type=jnp.float32
    )
    partial_gram = jnp.stack([gram_re, cross_terms - jnp.swapaxes(cross_terms, 1, 2)], 1)
    shared = lax.psum_scatter(partial_gram, "freq", scatter_dimension=0, tiled=True)
    shared = lax.psum(shared, "tm")
    coef_part, energy_part = whiten(shared, points)
    coefficients, energy = (
        lax.all_gather(for_sending(coef_part), "freq", axis=0, tiled=True).astype(coef_part.dtype),
        lax.all_gather(for_sending(energy_part), "freq", axis=0, tiled=True).astype(
            energy_part.dtype
        ),
    )
    coef_bf = jnp.transpose(coefficients.astype(jnp.bfloat16), (0, 4, 1, 2, 3))
    modes = jnp.einsum(
        "fjorb,frbn->fjon", coef_bf, flat_spec, preferred_element_type=jnp.float32
    ).astype(jnp.bfloat16)
    return (modes.reshape(NF, NB, 2, 3, width), energy)


MESH = pl.DeviceIdType.MESH
ROWS = 2 * NF
HOP = 128
JIT = 64


def plan(n, rows, total, width):
    if n < 2 or n % 2 or NB % n or total % (2 * NF) or width != 128 or rows % 16:
        return None
    per = NB // n
    if per < 4 or per % 2:
        return None
    slots = per + 4
    whole = [[] for _ in range(slots)]
    shared = [[] for _ in range(slots)]
    holders = []
    for block in range(NB):
        touched = [
            dev for dev in range(n)
            if HOP * block < rows * (dev + 1) and HOP * block + JIT + NFFT > rows * dev
        ]
        holders.append(touched)
        if len(touched) > 2:
            return None
        for dev in touched:
            slot = block - per * dev + 2
            if not 0 <= slot < slots:
                return None
            if len(touched) == 2:
                if (slot < slots // 2) != (dev == touched[1]):
                    return None
                shared[slot].append(dev)
            else:
                whole[slot].append(dev)
    return per, whole, shared, holders


def base_table(freqs_ref):
    row = lax.broadcasted_iota(jnp.int32, (ROWS, NFFT), 0)
    times_idx = lax.broadcasted_iota(jnp.int32, (ROWS, NFFT), 1)
    freqs = jnp.zeros((ROWS, NFFT), jnp.int32)
    for f in range(NF):
        freqs = jnp.where((row >> 1) == f, freqs_ref[f], freqs)
    phase = (freqs * times_idx) & (NFFT - 1)
    angles = 2.0 * math.pi / NFFT * phase.astype(jnp.float32)
    window = 0.5 - 0.5 * jnp.cos(2.0 * math.pi / NFFT * times_idx.astype(jnp.float32))
    hann = 0.5 - 0.5 * np.cos(2.0 * math.pi / NFFT * np.arange(NFFT))
    scaling = np.float32(1.0 / np.sqrt(np.sum(hann * hann)))
    cosine = window * jnp.cos(angles) * scaling
    sine = -window * jnp.sin(angles) * scaling
    return jnp.where((row & 1) == 1, sine, cosine).astype(jnp.bfloat16)


def shifted(base, shift, rows):
    source = lax.broadcasted_iota(jnp.int32, (NFFT, rows), 0)
    target = lax.broadcasted_iota(jnp.int32, (NFFT, rows), 1)
    pick = jnp.where(source - target == shift, 1.0, 0.0).astype(jnp.bfloat16)
    return jnp.dot(base, pick, preferred_element_type=jnp.float32).astype(jnp.bfloat16)


def expanders(spread_ref, mask_ref):
    row = lax.broadcasted_iota(jnp.int32, (NB * 6, 2 * NB), 0)
    col = lax.broadcasted_iota(jnp.int32, (NB * 6, 2 * NB), 1)
    first = 6 * (col & (NB - 1))
    hit = (row >= first) & (row < first + 6) & ((row & 1) == jnp.where(col >= NB, 1, 0))
    spread_ref[...] = jnp.where(hit, 1.0, 0.0).astype(jnp.bfloat16)
    row = lax.broadcasted_iota(jnp.int32, (NB * 6, 6 * NB), 0)
    col = lax.broadcasted_iota(jnp.int32, (NB * 6, 6 * NB), 1)
    pair = row >> 1
    comp = pair - 3 * ((pair * 43691) >> 17)
    part = jnp.where(col >= 4 * NB, 2, jnp.where(col >= 2 * NB, 1, 0))
    mask_ref[...] = jnp.where(comp == part, 1.0, 0.0)


def member(index, devs):
    if not devs:
        return None
    if devs == list(range(devs[0], devs[-1] + 1)):
        return (index >= devs[0]) & (index <= devs[-1])
    hit = index == devs[0]
    for dev in devs[1:]:
        hit = hit | (index == dev)
    return hit


def kernel(n, nf_dev, per, whole, shared, holders, points, x_hbm, starts_hbm, freqs_hbm,
           modes_ref, energy_ref, starts_ref, freqs_ref, t_ref, spread_ref, mask_ref, xv, parts,
           sendp, others, scales, oscales, sendb, recvb, spec32, spec, gpart, gath, msg, crecv,
           load_sem, psend, precv, ssend, srecv, asend, arecv, gsend, grecv, csend, crcv):
    tm = lax.axis_index("tm")
    fr = lax.axis_index("freq")
    total = n * nf_dev
    lin = tm * nf_dev + fr
    step, lowest = total // (2 * NF), total // 4
    slots = per + 4
    half_slots = slots // 2
    mine = (lin - lowest) // step
    owns = (lin >= lowest) & (lin < lowest + NF * step) & ((lin - lowest) % step == 0)
    half_n = n // 2
    parity = tm % 2
    rows = xv.shape[2]
    pw = xv.shape[3] // 2

    def owner(f):
        return lowest + f * step

    def where_is(index):
        return {"tm": index // nf_dev, "freq": index % nf_dev}

    def group(k):
        return jnp.where(tm < half_n, half_n - 1 - k, k)

    def load(g, c):
        return pltpu.make_async_copy(
            x_hbm.at[c, :, pl.ds(pl.multiple_of(g * 2 * pw, 2 * pw), 2 * pw)], xv.at[g, c],
            load_sem.at[2 + 3 * g + c])

    small = pltpu.make_async_copy(freqs_hbm, freqs_ref, load_sem.at[0])
    small.start()
    starts = pltpu.make_async_copy(starts_hbm, starts_ref, load_sem.at[1])
    starts.start()
    for k in range(half_n):
        for c in range(3):
            load(group(k), c).start()
    barrier = pltpu.get_barrier_semaphore()

    @pl.loop(1, total)
    def _(k):
        pl.semaphore_signal(barrier, inc=1, device_id=where_is((lin + k) % total), device_id_type=MESH)

    small.wait()
    base = base_table(freqs_ref)
    starts.wait()
    for slot in range(slots):
        block = per * tm + slot - 2
        start = starts_ref[jnp.clip(block, 0, NB - 1)]
        inside = (block >= 0) & (block < NB)
        shift = jnp.where(inside, rows * tm - start, 4 * (rows + NFFT))
        t_ref[slot * ROWS : (slot + 1) * ROWS, :] = shifted(base, shift, rows)
    scales[...] = jnp.zeros_like(scales)
    expanders(spread_ref, mask_ref)

    def low(slot):
        return slot < half_slots

    def pick(flag, yes, no):
        return (yes if flag else no) if isinstance(flag, bool) else jnp.where(flag, yes, no)

    def partner(slot):
        return pick(low(slot), (tm + n - 1) % n, (tm + 1) % n)

    def across(slot):
        return pick(low(slot), slot + per, slot - per)

    def is_shared(slot):
        block = per * tm + slot - 2
        edge = rows * (tm + pick(low(slot), 0, 1))
        inside = (block >= 0) & (block < NB) & (edge > 0) & (edge < rows * n)
        return inside & (HOP * block < edge) & (HOP * block + JIT + NFFT > edge)

    def is_theirs(slot, dest):
        middle = tm + pick(low(slot), 0, 1) == half_n
        by_half = (dest < half_n) != (tm < half_n)
        return (middle & by_half) | (jnp.logical_not(middle) & (dest % 2 != parity))

    def exchange(slot, dest):
        return pltpu.make_async_remote_copy(
            src_ref=sendp.at[slot, dest], dst_ref=others.at[across(slot), dest],
            send_sem=psend.at[slot, dest], recv_sem=precv.at[across(slot), dest],
            device_id={"tm": partner(slot), "freq": fr}, device_id_type=MESH)

    def arrival(slot, dest):
        return pltpu.make_async_remote_copy(
            src_ref=sendp.at[slot, dest], dst_ref=others.at[slot, dest],
            send_sem=psend.at[slot, dest], recv_sem=precv.at[slot, dest],
            device_id={"tm": partner(slot), "freq": fr}, device_id_type=MESH)

    def scale_copy(side):
        return pltpu.make_async_remote_copy(
            src_ref=scales.at[side], dst_ref=oscales.at[1 - side],
            send_sem=ssend.at[side], recv_sem=srecv.at[1 - side],
            device_id={"tm": (tm + 1) % n if side else (tm + n - 1) % n, "freq": fr},
            device_id_type=MESH)

    def scatter(slot, dest):
        return pltpu.make_async_remote_copy(
            src_ref=sendb.at[slot, dest], dst_ref=recvb.at[per * tm + slot - 2],
            send_sem=asend.at[slot, dest], recv_sem=arecv.at[per * tm + slot - 2],
            device_id={"tm": dest, "freq": fr}, device_id_type=MESH)

    def deliver(slot, dest, value):
        value = value.astype(jnp.bfloat16)

        @pl.when(dest == tm)
        def _():
            recvb[per * tm + slot - 2] = value

        @pl.when(dest != tm)
        def _():
            sendb[slot, dest] = value
            scatter(slot, dest).start()

    diagonal = (lax.broadcasted_iota(jnp.int32, (ROWS, 128), 0)
                == lax.broadcasted_iota(jnp.int32, (ROWS, 128), 1))

    def encode(slot, dest):
        value = parts[dest, slot * ROWS : (slot + 1) * ROWS, :]
        peak = jnp.maximum(jnp.max(jnp.abs(value), axis=1, keepdims=True), 1e-30)
        whole_numbers = (value * (32767.0 / peak) + 12582912.0) - 12582912.0
        sendp[slot, dest] = whole_numbers.astype(jnp.int32).astype(jnp.int16)
        line = jnp.sum(jnp.where(diagonal, peak, 0.0), axis=0, keepdims=True)
        scales[slot // half_slots, pl.ds(slot % half_slots * n + dest, 1), :] = line
        exchange(slot, dest).start()

    @pl.loop(0, half_n)
    def _(k):
        g = group(k)
        for c in range(3):
            load(g, c).wait()
            part = jnp.dot(t_ref[...], xv[g, c], preferred_element_type=jnp.float32)
            for d in range(2):
                parts[2 * g + d, :, c * pw : (c + 1) * pw] = part[:, d * pw : (d + 1) * pw]

        @pl.when(k == 0)
        def _():
            pl.semaphore_wait(barrier, total - 1)

        for d in range(2):
            for slot in range(slots):
                if shared[slot]:
                    @pl.when(member(tm, shared[slot]) & is_theirs(slot, 2 * g + d))
                    def _(slot=slot, d=d):
                        encode(slot, 2 * g + d)

        for d in range(2):
            for slot in range(slots):
                if whole[slot]:
                    @pl.when(member(tm, whole[slot]))
                    def _(slot=slot, d=d):
                        deliver(slot, 2 * g + d, parts[2 * g + d, slot * ROWS : (slot + 1) * ROWS, :])

    @pl.when(tm > 0)
    def _():
        scale_copy(0).start()

    @pl.when(tm < n - 1)
    def _():
        scale_copy(1).start()

    @pl.when(tm > 0)
    def _():
        scale_copy(1).wait_recv()

    @pl.when(tm < n - 1)
    def _():
        scale_copy(0).wait_recv()

    @pl.loop(0, half_n)
    def _(k):
        g = group(k)

        @pl.loop(0, slots)
        def _(turn):
            slot = (turn + half_slots * (1 - parity)) % slots
            for d in range(2):
                @pl.when(is_shared(slot) & jnp.logical_not(is_theirs(slot, 2 * g + d)))
                def _(d=d):
                    dest = 2 * g + d
                    arrival(slot, dest).wait_recv()
                    line = oscales[slot // half_slots, pl.ds(slot % half_slots * n + dest, 1), :]
                    peak = jnp.sum(jnp.where(diagonal, line, 0.0), axis=1, keepdims=True)
                    other = others[slot, dest].astype(jnp.int32).astype(jnp.float32)
                    here = parts[dest, pl.ds(pl.multiple_of(slot * ROWS, ROWS), ROWS), :]
                    deliver(slot, dest, here + other * (peak * (1.0 / 32767.0)))

    ordered = [b for b in range(NB) if len(holders[b]) == 1] + [b for b in range(NB) if len(holders[b]) == 2]
    for block in ordered:
        @pl.when(jnp.logical_not(member(tm, holders[block])))
        def _(block=block):
            pltpu.make_async_remote_copy(
                src_ref=sendb.at[0, 0], dst_ref=recvb.at[block], send_sem=asend.at[0, 0],
                recv_sem=arecv.at[block], device_id={"tm": tm, "freq": fr},
                device_id_type=MESH).wait_recv()

    pitch = spec32.shape[1] // NB
    for block in range(NB):
        values = recvb[block]
        for c in range(3):
            spec32[c, block * pitch : block * pitch + ROWS, :] = values[:, c * 128 : (c + 1) * 128].astype(jnp.float32)

    def to_owner(f):
        return pltpu.make_async_remote_copy(
            src_ref=gpart.at[f], dst_ref=gath.at[lin], send_sem=gsend.at[f],
            recv_sem=grecv.at[lin], device_id=where_is(owner(f)), device_id_type=MESH)

    upper = lax.broadcasted_iota(jnp.int32, (NB, NB), 1) >= lax.broadcasted_iota(jnp.int32, (NB, NB), 0)
    for f in range(NF):
        real = [spec32[c, pl.ds(2 * f, NB, stride=pitch), :].astype(jnp.bfloat16) for c in range(3)]
        imag = [spec32[c, pl.ds(2 * f + 1, NB, stride=pitch), :].astype(jnp.bfloat16) for c in range(3)]
        for c in range(3):
            spec[f, c * 2 * NB : c * 2 * NB + NB, :] = real[c]
            spec[f, c * 2 * NB + NB : (c + 1) * 2 * NB, :] = imag[c]
        lhs = jnp.concatenate(real + imag, axis=1)
        rhs = jnp.concatenate([lhs, jnp.concatenate(imag + [-v for v in real], axis=1)], axis=0)
        gram = lax.dot_general(lhs, rhs, (((1,), (1,)), ((), ())), preferred_element_type=jnp.float32)
        packed = jnp.where(upper, gram[:, :NB], gram[:, NB:])
        gpart[f] = jnp.concatenate([packed[8 * q : 8 * q + 8] for q in range(NB // 8)], axis=1)
        if f % 4 == 3:
            for sent in range(f - 3, f + 1):
                @pl.when(lin != owner(sent))
                def _(sent=sent):
                    to_owner(sent).start()

    def coef_to(away):
        row, col = tm + away // nf_dev, fr + away % nf_dev
        where = {"tm": jnp.where(row >= n, row - n, row),
                 "freq": jnp.where(col >= nf_dev, col - nf_dev, col)}
        return pltpu.make_async_remote_copy(
            src_ref=msg, dst_ref=crecv.at[mine], send_sem=csend.at[away],
            recv_sem=crcv.at[mine], device_id=where, device_id_type=MESH)

    @pl.when(owns)
    def _():
        gath[lin] = gpart[mine]

        @pl.loop(1, total)
        def _(k):
            src = (lin + k) % total
            pltpu.make_async_remote_copy(
                src_ref=gpart.at[0], dst_ref=gath.at[src], send_sem=gsend.at[0],
                recv_sem=grecv.at[src], device_id=where_is(src), device_id_type=MESH).wait_recv()

        packed = jnp.sum(gath[...], axis=0)
        square = jnp.concatenate([packed[:, q * NB : (q + 1) * NB] for q in range(NB // 8)], axis=0)
        flipped = jnp.transpose(square)
        ri = lax.broadcasted_iota(jnp.int32, (NB, NB), 0)
        ci = lax.broadcasted_iota(jnp.int32, (NB, NB), 1)
        gram_re = jnp.where(ci >= ri, square, flipped)
        gram_im = jnp.where(ci < ri, square, jnp.where(ci > ri, -flipped, 0.0))
        energy = jnp.sum(jnp.where(ri == ci, gram_re, 0.0), axis=(0, 1), keepdims=True) / (3.0 * NB * points)
        hermit = jnp.concatenate([
            jnp.concatenate([gram_re, -gram_im, gram_re, -gram_im], axis=1),
            jnp.concatenate([gram_im, gram_re, gram_im, gram_re], axis=1)], axis=0)
        frob = jnp.sqrt(0.5 * jnp.sum(hermit * hermit, axis=(0, 1), keepdims=True) + 1e-06)
        ri = lax.broadcasted_iota(jnp.int32, (2 * NB, 4 * NB), 0)
        ci = lax.broadcasted_iota(jnp.int32, (2 * NB, 4 * NB), 1)
        left = ci < 2 * NB
        identity = jnp.where(ri == (ci & (2 * NB - 1)), 1.0, 0.0).astype(jnp.float32)

        def pieces(a):
            high = a.astype(jnp.bfloat16)
            rest = a - high.astype(jnp.float32)
            mid = rest.astype(jnp.bfloat16)
            return high, mid, (rest - mid.astype(jnp.float32)).astype(jnp.bfloat16)

        def mul(a, b):
            ah, am, al = a
            bh, bm, bl = b
            lhs = jnp.concatenate([ah, am, jnp.where(left[: ah.shape[0]], ah, al)], axis=1)
            rhs = jnp.concatenate([bh, bm, bh, bm, bl, bh], axis=0)
            return jnp.dot(lhs, rhs, preferred_element_type=jnp.float32)

        iterate = hermit / frob
        inverse = identity
        for step in range(NSIT):
            it = pieces(iterate)
            if step:
                inv = pieces(inverse)
            factor = 1.5 * identity - 0.5 * (mul(inv, it) if step else iterate)
            fac = pieces(factor)
            if step < NSIT - 1:
                iterate = mul(it, fac)
                inverse = mul(fac, inv) if step else factor
            else:
                inverse = mul(tuple(piece[:NB] for piece in fac), inv)
        scaled = inverse * jnp.sqrt(6.0 * points / frob)
        high, mid, rest = [piece.astype(jnp.float32) for piece in pieces(energy)]
        top = ri[:NB]
        extra = jnp.where(top == 0, high, jnp.where(top == 1, mid, jnp.where(top == 2, rest, 0.0)))
        scaled = jnp.where((ci[:NB] & (2 * NB - 1)) == NB + top, extra, scaled)
        msg[...] = jnp.where(left[: NB // 2], scaled[: NB // 2], scaled[NB // 2 :]).astype(jnp.bfloat16)
        crecv[mine] = msg[...]

        for away in range(total - 1, 0, -1):
            coef_to(away).start()

    @pl.loop(0, slots)
    def _(slot):
        sharing = is_shared(slot)
        block = per * tm + slot - 2
        inside = (block >= 0) & (block < NB)
        alone = inside & (HOP * block >= rows * tm) & (HOP * block + JIT + NFFT <= rows * (tm + 1))

        @pl.loop(0, n)
        def _(dest):
            theirs = is_theirs(slot, dest)

            @pl.when(sharing & theirs)
            def _():
                exchange(slot, dest).wait_send()

            @pl.when((alone | (sharing & jnp.logical_not(theirs))) & (dest != tm))
            def _():
                scatter(slot, dest).wait_send()

    @pl.when(tm > 0)
    def _():
        scale_copy(0).wait_send()

    @pl.when(tm < n - 1)
    def _():
        scale_copy(1).wait_send()

    for f in range(NF):
        @pl.when(lin != owner(f))
        def _(f=f):
            to_owner(f).wait_send()

    for f in range(NF):
        @pl.when(lin != owner(f))
        def _(f=f):
            pltpu.make_async_remote_copy(
                src_ref=msg, dst_ref=crecv.at[f], send_sem=csend.at[f], recv_sem=crcv.at[f],
                device_id=where_is(owner(f)), device_id_type=MESH).wait_recv()

    lanes = lax.broadcasted_iota(jnp.int32, (NB, 2 * NB), 1)
    signs = jnp.where(lanes < NB, 1.0, -1.0).astype(jnp.bfloat16)
    hidden = lanes == NB + lax.broadcasted_iota(jnp.int32, (NB, 2 * NB), 0)
    wide_lane = lax.broadcasted_iota(jnp.int32, (1, NF), 1)
    energies = jnp.zeros((1, NF), jnp.float32)
    for f in range(NF):
        pairs = crecv[f]
        straight = jnp.concatenate([pairs[:, : 2 * NB], pairs[:, 2 * NB :]], axis=0)
        found = jnp.sum(jnp.where(hidden, straight.astype(jnp.float32), 0.0), axis=(0, 1), keepdims=True)
        energies = jnp.where(wide_lane == f, found, energies)
        straight = jnp.where(hidden, jnp.zeros_like(straight), straight)
        crossed = jnp.concatenate([straight[:, NB:], straight[:, :NB]], axis=1)
        stacked = jnp.concatenate([straight * signs, crossed], axis=0)
        tiled = jnp.concatenate([stacked] * 3, axis=1)
        full = jnp.dot(spread_ref[...], tiled, preferred_element_type=jnp.float32)
        full = (full * mask_ref[...]).astype(jnp.bfloat16)
        modes_ref[f * 6 * NB : (f + 1) * 6 * NB, :] = jnp.dot(
            full, spec[f], preferred_element_type=jnp.float32).astype(jnp.bfloat16)
    energy_ref[...] = energies

    @pl.when(owns)
    def _():
        for away in range(total - 1, 0, -1):
            coef_to(away).wait_send()


def fused(n, nf_dev, chosen, snapshots, block_starts, freq_index):
    per, whole, shared, holders = chosen
    rows, count, wide = snapshots.shape
    total = n * nf_dev
    pw = wide // n
    slots = per + 4
    f32, bf16 = jnp.float32, jnp.bfloat16
    dma = pltpu.SemaphoreType.DMA
    vmem = pl.BlockSpec(memory_space=pltpu.VMEM)
    modes, energy = pl.pallas_call(
        functools.partial(kernel, n, nf_dev, per, whole, shared, holders, float(wide * nf_dev)),
        out_shape=(jax.ShapeDtypeStruct((NF * NB * 6, pw), bf16), jax.ShapeDtypeStruct((1, NF), f32)),
        in_specs=[pl.BlockSpec(memory_space=pltpu.HBM)] * 3,
        out_specs=(vmem, vmem),
        scratch_shapes=[
            pltpu.SMEM((NB,), jnp.int32),
            pltpu.SMEM((NF,), jnp.int32),
            pltpu.VMEM((slots * ROWS, rows), bf16),
            pltpu.VMEM((NB * 6, 2 * NB), bf16),
            pltpu.VMEM((NB * 6, 6 * NB), f32),
            pltpu.VMEM((n // 2, 3, rows, 2 * pw), bf16),
            pltpu.VMEM((n, slots * ROWS, 3 * pw), f32),
            pltpu.VMEM((slots, n, ROWS, 3 * pw), jnp.int16),
            pltpu.VMEM((slots, n, ROWS, 3 * pw), jnp.int16),
            pltpu.VMEM((2, slots // 2 * n, 128), f32),
            pltpu.VMEM((2, slots // 2 * n, 128), f32),
            pltpu.VMEM((slots, n, ROWS, 3 * pw), bf16),
            pltpu.VMEM((NB, ROWS, 3 * pw), bf16),
            pltpu.VMEM((3, NB * (ROWS + 8), pw), f32),
            pltpu.VMEM((NF, 6 * NB, pw), bf16),
            pltpu.VMEM((NF, NB // 4, 4 * NB), f32),
            pltpu.VMEM((total, NB // 4, 4 * NB), f32),
            pltpu.VMEM((NB // 2, 4 * NB), bf16),
            pltpu.VMEM((NF, NB // 2, 4 * NB), bf16),
            dma((2 + 3 * n // 2,)), dma((slots, n)), dma((slots, n)), dma((2,)), dma((2,)),
            dma((slots, n)), dma((NB,)), dma((NF,)), dma((total,)), dma((total,)), dma((NF,)),
        ],
        compiler_params=pltpu.CompilerParams(
            collective_id=0, has_side_effects=True, vmem_limit_bytes=54_000_000),
    )(jnp.transpose(snapshots, (1, 0, 2)), block_starts, freq_index)
    modes = modes.reshape(NF, NB, 3, 2, pw).transpose(0, 1, 3, 2, 4)
    return modes, energy.reshape(NF)


def solution(mesh):
    n, nf_dev = mesh.shape["tm"], mesh.shape["freq"]

    def body(snapshots, block_starts, freq_index):
        rows, _, wide = snapshots.shape
        chosen = plan(n, rows, n * nf_dev, wide // n)
        if chosen is None:
            return local(snapshots, block_starts, freq_index)
        return fused(n, nf_dev, chosen, snapshots, block_starts, freq_index)

    return jax.shard_map(
        body,
        mesh=mesh,
        in_specs=(P("tm", None, "freq"), P(), P()),
        out_specs=(P(None, None, None, None, ("freq", "tm")), P()),
        check_vma=False,
    )
```

```python
import functools
import math

import jax
import jax.numpy as jnp
import numpy as np
from jax import lax
from jax.experimental import pallas as pl
from jax.experimental.pallas import tpu as pltpu
from jax.sharding import PartitionSpec as P

NB = 32
NFFT = 256
NF = 16
NSIT = 6


def for_sending(shard):
    return jax.tree.map(lambda a: a.astype(jnp.bfloat16) if a.dtype == jnp.float32 else a, shard)


def dft_rows(freq_index):
    times_idx = jnp.arange(NFFT, dtype=jnp.int32)
    phase_int = freq_index[:, None] * times_idx[None, :] % NFFT
    angles = 2.0 * math.pi / NFFT * phase_int.astype(jnp.float32)
    window = 0.5 - 0.5 * jnp.cos(2.0 * math.pi / NFFT * times_idx.astype(jnp.float32))
    scaling = 1.0 / jnp.sqrt(jnp.sum(window * window))
    cosine = window[None, :] * jnp.cos(angles) * scaling
    sine_rows = -window[None, :] * jnp.sin(angles) * scaling
    return jnp.stack([cosine, sine_rows], 1).reshape(2 * NF, NFFT).astype(jnp.bfloat16)


def block_rows(block_starts):
    return block_starts[:, None] + jnp.arange(NFFT, dtype=jnp.int32)[None, :]


def matmul_batch(left, right):
    return jnp.einsum("fij,fjk->fik", left, right, precision=lax.Precision.HIGHEST)


def whiten(summed, points):
    gram_re = summed[:, 0]
    gram_im = summed[:, 1]
    top_rows = jnp.concatenate([gram_re, -gram_im], 2)
    low_rows = jnp.concatenate([gram_im, gram_re], 2)
    hermit = jnp.concatenate([top_rows, low_rows], 1)
    frob = jnp.sqrt(jnp.sum(hermit * hermit, axis=(1, 2)) + 1e-06)
    identity = jnp.eye(2 * NB, dtype=jnp.float32)[None]
    iterate = hermit / frob[:, None, None]
    inverse = jnp.broadcast_to(identity, hermit.shape)
    for iteration in range(NSIT):
        factor = 1.5 * identity - 0.5 * matmul_batch(inverse, iterate)
        iterate = matmul_batch(iterate, factor)
        inverse = matmul_batch(factor, inverse)
    columns = inverse[:, :, :NB] * jnp.sqrt(6.0 * points / frob)[:, None, None]
    upper = columns[:, :NB]
    lower = columns[:, NB:]
    coefficients = jnp.stack([jnp.stack([upper, -lower], 1), jnp.stack([lower, upper], 1)], 1)
    energy = jnp.trace(gram_re, axis1=1, axis2=2) / (3.0 * NB * points)
    return (coefficients, energy)


def local(snapshots, block_starts, freq_index):
    dft_table = dft_rows(freq_index)
    offsets = block_rows(block_starts)
    series = lax.all_to_all(snapshots, "tm", split_axis=2, concat_axis=0, tiled=True)
    count = series.shape[1]
    width = series.shape[2]
    columns_all = series.reshape(series.shape[0], count * width)
    windows = jnp.take(columns_all, offsets, axis=0)
    spectra_part = jnp.einsum(
        "rt,btn->rbn", dft_table, windows, preferred_element_type=jnp.float32
    ).astype(jnp.bfloat16)
    spectra = spectra_part.reshape(2 * NF, NB, count, width)
    width = spectra.shape[3]
    points = float(width * lax.axis_size("tm") * lax.axis_size("freq"))
    flat_spec = spectra.reshape(NF, 2, NB, 3 * width)
    real_part = flat_spec[:, 0]
    imag_part = flat_spec[:, 1]
    gram_re = jnp.einsum("fbn,fcn->fbc", real_part, real_part, preferred_element_type=jnp.float32)
    gram_re = gram_re + jnp.einsum(
        "fbn,fcn->fbc", imag_part, imag_part, preferred_element_type=jnp.float32
    )
    cross_terms = jnp.einsum(
        "fbn,fcn->fbc", real_part, imag_part, preferred_element_type=jnp.float32
    )
    partial_gram = jnp.stack([gram_re, cross_terms - jnp.swapaxes(cross_terms, 1, 2)], 1)
    shared = lax.psum_scatter(partial_gram, "freq", scatter_dimension=0, tiled=True)
    shared = lax.psum(shared, "tm")
    coef_part, energy_part = whiten(shared, points)
    coefficients, energy = (
        lax.all_gather(for_sending(coef_part), "freq", axis=0, tiled=True).astype(coef_part.dtype),
        lax.all_gather(for_sending(energy_part), "freq", axis=0, tiled=True).astype(
            energy_part.dtype
        ),
    )
    coef_bf = jnp.transpose(coefficients.astype(jnp.bfloat16), (0, 4, 1, 2, 3))
    modes = jnp.einsum(
        "fjorb,frbn->fjon", coef_bf, flat_spec, preferred_element_type=jnp.float32
    ).astype(jnp.bfloat16)
    return (modes.reshape(NF, NB, 2, 3, width), energy)


MESH = pl.DeviceIdType.MESH
ROWS = 2 * NF
HOP = 128
JIT = 64


def plan(n, rows, total, width):
    if n < 2 or n % 2 or NB % n or total % (2 * NF) or width != 128 or rows % 16:
        return None
    per = NB // n
    if per < 4 or per % 2:
        return None
    slots = per + 4
    whole = [[] for _ in range(slots)]
    shared = [[] for _ in range(slots)]
    holders = []
    for block in range(NB):
        touched = [
            dev for dev in range(n)
            if HOP * block < rows * (dev + 1) and HOP * block + JIT + NFFT > rows * dev
        ]
        holders.append(touched)
        if len(touched) > 2:
            return None
        for dev in touched:
            slot = block - per * dev + 2
            if not 0 <= slot < slots:
                return None
            if len(touched) == 2:
                if (slot < slots // 2) != (dev == touched[1]):
                    return None
                shared[slot].append(dev)
            else:
                whole[slot].append(dev)
    return per, whole, shared, holders


def base_table(freqs_ref):
    row = lax.broadcasted_iota(jnp.int32, (ROWS, NFFT), 0)
    times_idx = lax.broadcasted_iota(jnp.int32, (ROWS, NFFT), 1)
    freqs = jnp.zeros((ROWS, NFFT), jnp.int32)
    for f in range(NF):
        freqs = jnp.where((row >> 1) == f, freqs_ref[f], freqs)
    phase = (freqs * times_idx) & (NFFT - 1)
    angles = 2.0 * math.pi / NFFT * phase.astype(jnp.float32)
    window = 0.5 - 0.5 * jnp.cos(2.0 * math.pi / NFFT * times_idx.astype(jnp.float32))
    hann = 0.5 - 0.5 * np.cos(2.0 * math.pi / NFFT * np.arange(NFFT))
    scaling = np.float32(1.0 / np.sqrt(np.sum(hann * hann)))
    cosine = window * jnp.cos(angles) * scaling
    sine = -window * jnp.sin(angles) * scaling
    return jnp.where((row & 1) == 1, sine, cosine).astype(jnp.bfloat16)


def shifted(base, shift, rows):
    source = lax.broadcasted_iota(jnp.int32, (NFFT, rows), 0)
    target = lax.broadcasted_iota(jnp.int32, (NFFT, rows), 1)
    pick = jnp.where(source - target == shift, 1.0, 0.0).astype(jnp.bfloat16)
    return jnp.dot(base, pick, preferred_element_type=jnp.float32).astype(jnp.bfloat16)


def expanders(spread_ref, mask_ref):
    row = lax.broadcasted_iota(jnp.int32, (NB * 6, 2 * NB), 0)
    col = lax.broadcasted_iota(jnp.int32, (NB * 6, 2 * NB), 1)
    first = 6 * (col & (NB - 1))
    hit = (row >= first) & (row < first + 6) & ((row & 1) == jnp.where(col >= NB, 1, 0))
    spread_ref[...] = jnp.where(hit, 1.0, 0.0).astype(jnp.bfloat16)
    row = lax.broadcasted_iota(jnp.int32, (NB * 6, 6 * NB), 0)
    col = lax.broadcasted_iota(jnp.int32, (NB * 6, 6 * NB), 1)
    pair = row >> 1
    comp = pair - 3 * ((pair * 43691) >> 17)
    part = jnp.where(col >= 4 * NB, 2, jnp.where(col >= 2 * NB, 1, 0))
    mask_ref[...] = jnp.where(comp == part, 1.0, 0.0)


def member(index, devs):
    if not devs:
        return None
    if devs == list(range(devs[0], devs[-1] + 1)):
        return (index >= devs[0]) & (index <= devs[-1])
    hit = index == devs[0]
    for dev in devs[1:]:
        hit = hit | (index == dev)
    return hit


def kernel(n, nf_dev, per, whole, shared, holders, points, x_hbm, starts_hbm, freqs_hbm,
           modes_ref, energy_ref, starts_ref, freqs_ref, t_ref, spread_ref, mask_ref, xv, parts,
           sendp, others, scales, oscales, sendb, recvb, spec32, spec, gpart, gath, msg, crecv,
           load_sem, psend, precv, ssend, srecv, asend, arecv, gsend, grecv, csend, crcv):
    tm = lax.axis_index("tm")
    fr = lax.axis_index("freq")
    total = n * nf_dev
    lin = tm * nf_dev + fr
    step, lowest = total // (2 * NF), total // 4
    slots = per + 4
    half_slots = slots // 2
    mine = (lin - lowest) // step
    owns = (lin >= lowest) & (lin < lowest + NF * step) & ((lin - lowest) % step == 0)
    half_n = n // 2
    parity = tm % 2
    rows = xv.shape[2]
    pw = xv.shape[3] // 2

    def owner(f):
        return lowest + f * step

    def where_is(index):
        return {"tm": index // nf_dev, "freq": index % nf_dev}

    def group(k):
        return jnp.where(tm < half_n, half_n - 1 - k, k)

    def load(g, c):
        return pltpu.make_async_copy(
            x_hbm.at[c, :, pl.ds(pl.multiple_of(g * 2 * pw, 2 * pw), 2 * pw)], xv.at[g, c],
            load_sem.at[2 + g])

    small = pltpu.make_async_copy(freqs_hbm, freqs_ref, load_sem.at[0])
    small.start()
    starts = pltpu.make_async_copy(starts_hbm, starts_ref, load_sem.at[1])
    starts.start()
    for k in range(half_n):
        for c in range(3):
            load(group(k), c).start()
    barrier = pltpu.get_barrier_semaphore()

    @pl.loop(1, total)
    def _(k):
        pl.semaphore_signal(barrier, inc=1, device_id=where_is((lin + k) % total), device_id_type=MESH)

    small.wait()
    base = base_table(freqs_ref)
    starts.wait()
    for slot in range(slots):
        block = per * tm + slot - 2
        start = starts_ref[jnp.clip(block, 0, NB - 1)]
        inside = (block >= 0) & (block < NB)
        shift = jnp.where(inside, rows * tm - start, 4 * (rows + NFFT))
        t_ref[slot * ROWS : (slot + 1) * ROWS, :] = shifted(base, shift, rows)
    scales[...] = jnp.zeros_like(scales)
    expanders(spread_ref, mask_ref)

    def low(slot):
        return slot < half_slots

    def pick(flag, yes, no):
        return (yes if flag else no) if isinstance(flag, bool) else jnp.where(flag, yes, no)

    def partner(slot):
        return pick(low(slot), (tm + n - 1) % n, (tm + 1) % n)

    def across(slot):
        return pick(low(slot), slot + per, slot - per)

    def is_shared(slot):
        block = per * tm + slot - 2
        edge = rows * (tm + pick(low(slot), 0, 1))
        inside = (block >= 0) & (block < NB) & (edge > 0) & (edge < rows * n)
        return inside & (HOP * block < edge) & (HOP * block + JIT + NFFT > edge)

    def is_theirs(slot, dest):
        middle = tm + pick(low(slot), 0, 1) == half_n
        by_half = (dest < half_n) != (tm < half_n)
        return (middle & by_half) | (jnp.logical_not(middle) & (dest % 2 != parity))

    def exchange(slot, dest):
        return pltpu.make_async_remote_copy(
            src_ref=sendp.at[slot * n + dest], dst_ref=others.at[across(slot) * n + dest],
            send_sem=psend.at[0], recv_sem=precv.at[across(slot) // half_slots * half_n + dest // 2],
            device_id={"tm": partner(slot), "freq": fr}, device_id_type=MESH)

    def scale_copy(side, g):
        return pltpu.make_async_remote_copy(
            src_ref=scales.at[side * half_n + g], dst_ref=oscales.at[(1 - side) * half_n + g],
            send_sem=ssend.at[0], recv_sem=srecv.at[(1 - side) * half_n + g],
            device_id={"tm": partner(side * half_slots), "freq": fr}, device_id_type=MESH)

    def scatter(slot, dest):
        return pltpu.make_async_remote_copy(
            src_ref=sendb.at[slot * n + dest], dst_ref=recvb.at[per * tm + slot - 2],
            send_sem=asend.at[0], recv_sem=arecv.at[0],
            device_id={"tm": dest, "freq": fr}, device_id_type=MESH)

    def settle(ref, sem):
        pltpu.make_async_copy(ref, ref, sem).wait()

    def settle_count(ref, count, sem, options):
        for option in sorted(set(options)):
            @pl.when(count == option)
            def _(option=option):
                settle(ref.at[pl.ds(0, option)], sem)

    def edge_exists(side):
        return pick(side == 0, tm > 0, tm < n - 1)

    def at_middle(side):
        return tm + side == half_n

    def sharing(side):
        return sum(jnp.where(is_shared(side * half_slots + k), 1, 0) for k in range(half_slots))

    def deliver(slot, dest, value):
        value = value.astype(jnp.bfloat16)

        @pl.when(dest == tm)
        def _():
            recvb[per * tm + slot - 2] = value

        @pl.when(dest != tm)
        def _():
            sendb[slot * n + dest] = value
            scatter(slot, dest).start()

    diagonal = (lax.broadcasted_iota(jnp.int32, (ROWS, 128), 0)
                == lax.broadcasted_iota(jnp.int32, (ROWS, 128), 1))

    def encode(slot, g, d):
        value = parts[2 * g + d, slot * ROWS : (slot + 1) * ROWS, :]
        peak = jnp.maximum(jnp.max(jnp.abs(value), axis=1, keepdims=True), 1e-30)
        whole_numbers = (value * (32767.0 / peak) + 12582912.0) - 12582912.0
        sendp[slot * n + 2 * g + d] = whole_numbers.astype(jnp.int32).astype(jnp.int16)
        line = jnp.sum(jnp.where(diagonal, peak, 0.0), axis=0, keepdims=True)
        row = 2 * (slot % half_slots) + d
        scales[slot // half_slots * half_n + g, row : row + 1, :] = line

    @pl.loop(0, half_n)
    def _(k):
        g = group(k)
        settle(xv.at[g], load_sem.at[2 + g])
        for c in range(3):
            part = jnp.dot(t_ref[...], xv[g, c], preferred_element_type=jnp.float32)
            for d in range(2):
                parts[2 * g + d, :, c * pw : (c + 1) * pw] = part[:, d * pw : (d + 1) * pw]

        @pl.when(k == 0)
        def _():
            pl.semaphore_wait(barrier, total - 1)

        for d in range(2):
            for slot in range(slots):
                if shared[slot]:
                    @pl.when(member(tm, shared[slot]) & is_theirs(slot, 2 * g + d))
                    def _(slot=slot, d=d):
                        encode(slot, g, d)

        for side in range(2):
            @pl.when(edge_exists(side) & (jnp.logical_not(at_middle(side)) | is_theirs(side * half_slots, 2 * g)))
            def _(side=side):
                scale_copy(side, g).start()

        for d in range(2):
            for slot in range(slots):
                if shared[slot]:
                    @pl.when(member(tm, shared[slot]) & is_theirs(slot, 2 * g + d))
                    def _(slot=slot, d=d):
                        exchange(slot, 2 * g + d).start()

        for d in range(2):
            for slot in range(slots):
                if whole[slot]:
                    @pl.when(member(tm, whole[slot]))
                    def _(slot=slot, d=d):
                        deliver(slot, 2 * g + d, parts[2 * g + d, slot * ROWS : (slot + 1) * ROWS, :])

    counts = [sum(tm_at in devs for devs in shared) for tm_at in range(n)]

    @pl.loop(0, 2)
    def _(turn):
        side = jnp.where(turn == 0, 1 - parity, parity)

        @pl.loop(0, half_n)
        def _(k):
            g = group(k)
            middle = at_middle(side)

            @pl.when(edge_exists(side) & (jnp.logical_not(middle) | jnp.logical_not(is_theirs(side * half_slots, 2 * g))))
            def _():
                settle(oscales.at[side * half_n + g], srecv.at[side * half_n + g])
                settle_count(others, sharing(side) * jnp.where(middle, 2, 1), precv.at[side * half_n + g],
                             [count * twice for count in range(1, half_slots + 1) for twice in (1, 2)])
                for d in range(2):
                    dest = 2 * g + d
                    for index in range(half_slots):
                        slot = side * half_slots + index

                        @pl.when(is_shared(slot) & jnp.logical_not(is_theirs(slot, dest)))
                        def _(slot=slot, dest=dest, row=2 * index + d):
                            line = oscales[side * half_n + g, row : row + 1, :]
                            peak = jnp.sum(jnp.where(diagonal, line, 0.0), axis=1, keepdims=True)
                            other = others[slot * n + dest].astype(jnp.int32).astype(jnp.float32)
                            here = parts[dest, pl.ds(pl.multiple_of(slot * ROWS, ROWS), ROWS), :]
                            deliver(slot, dest, here + other * (peak * (1.0 / 32767.0)))


    alone = [sum(tm_at in devs for devs in whole) for tm_at in range(n)]
    for tm_at in range(n):
        @pl.when(tm == tm_at)
        def _(tm_at=tm_at):
            settle(recvb.at[pl.ds(0, NB - alone[tm_at] - counts[tm_at])], arecv.at[0])

    pitch = spec32.shape[1] // NB
    for block in range(NB):
        values = recvb[block]
        for c in range(3):
            spec32[c, block * pitch : block * pitch + ROWS, :] = values[:, c * 128 : (c + 1) * 128].astype(jnp.float32)

    def to_owner(f):
        return pltpu.make_async_remote_copy(
            src_ref=gpart.at[f], dst_ref=gath.at[lin], send_sem=gsend.at[0],
            recv_sem=grecv.at[0], device_id=where_is(owner(f)), device_id_type=MESH)

    upper = lax.broadcasted_iota(jnp.int32, (NB, NB), 1) >= lax.broadcasted_iota(jnp.int32, (NB, NB), 0)
    for f in range(NF):
        real = [spec32[c, pl.ds(2 * f, NB, stride=pitch), :].astype(jnp.bfloat16) for c in range(3)]
        imag = [spec32[c, pl.ds(2 * f + 1, NB, stride=pitch), :].astype(jnp.bfloat16) for c in range(3)]
        for c in range(3):
            spec[f, c * 2 * NB : c * 2 * NB + NB, :] = real[c]
            spec[f, c * 2 * NB + NB : (c + 1) * 2 * NB, :] = imag[c]
        lhs = jnp.concatenate(real + imag, axis=1)
        rhs = jnp.concatenate([lhs, jnp.concatenate(imag + [-v for v in real], axis=1)], axis=0)
        gram = lax.dot_general(lhs, rhs, (((1,), (1,)), ((), ())), preferred_element_type=jnp.float32)
        packed = jnp.where(upper, gram[:, :NB], gram[:, NB:])
        gpart[f] = jnp.concatenate([packed[8 * q : 8 * q + 8] for q in range(NB // 8)], axis=1)
        if f % 4 == 3:
            for sent in range(f - 3, f + 1):
                @pl.when(lin != owner(sent))
                def _(sent=sent):
                    to_owner(sent).start()

    def coef_to(away):
        row, col = tm + away // nf_dev, fr + away % nf_dev
        where = {"tm": jnp.where(row >= n, row - n, row),
                 "freq": jnp.where(col >= nf_dev, col - nf_dev, col)}
        return pltpu.make_async_remote_copy(
            src_ref=msg, dst_ref=crecv.at[mine], send_sem=csend.at[0],
            recv_sem=crcv.at[0], device_id=where, device_id_type=MESH)

    @pl.when(owns)
    def _():
        gath[lin] = gpart[mine]

        settle(gath.at[pl.ds(0, total - 1)], grecv.at[0])
        packed = jnp.sum(gath[...], axis=0)
        square = jnp.concatenate([packed[:, q * NB : (q + 1) * NB] for q in range(NB // 8)], axis=0)
        flipped = jnp.transpose(square)
        ri = lax.broadcasted_iota(jnp.int32, (NB, NB), 0)
        ci = lax.broadcasted_iota(jnp.int32, (NB, NB), 1)
        gram_re = jnp.where(ci >= ri, square, flipped)
        gram_im = jnp.where(ci < ri, square, jnp.where(ci > ri, -flipped, 0.0))
        energy = jnp.sum(jnp.where(ri == ci, gram_re, 0.0), axis=(0, 1), keepdims=True) / (3.0 * NB * points)
        hermit = jnp.concatenate([
            jnp.concatenate([gram_re, -gram_im, gram_re, -gram_im], axis=1),
            jnp.concatenate([gram_im, gram_re, gram_im, gram_re], axis=1)], axis=0)
        frob = jnp.sqrt(0.5 * jnp.sum(hermit * hermit, axis=(0, 1), keepdims=True) + 1e-06)
        ri = lax.broadcasted_iota(jnp.int32, (2 * NB, 4 * NB), 0)
        ci = lax.broadcasted_iota(jnp.int32, (2 * NB, 4 * NB), 1)
        left = ci < 2 * NB
        identity = jnp.where(ri == (ci & (2 * NB - 1)), 1.0, 0.0).astype(jnp.float32)

        def pieces(a):
            high = a.astype(jnp.bfloat16)
            rest = a - high.astype(jnp.float32)
            mid = rest.astype(jnp.bfloat16)
            return high, mid, (rest - mid.astype(jnp.float32)).astype(jnp.bfloat16)

        def mul(a, b):
            ah, am, al = a
            bh, bm, bl = b
            lhs = jnp.concatenate([ah, am, jnp.where(left[: ah.shape[0]], ah, al)], axis=1)
            rhs = jnp.concatenate([bh, bm, bh, bm, bl, bh], axis=0)
            return jnp.dot(lhs, rhs, preferred_element_type=jnp.float32)

        iterate = hermit / frob
        inverse = identity
        for step in range(NSIT):
            it = pieces(iterate)
            if step:
                inv = pieces(inverse)
            factor = 1.5 * identity - 0.5 * (mul(inv, it) if step else iterate)
            fac = pieces(factor)
            if step < NSIT - 1:
                iterate = mul(it, fac)
                inverse = mul(fac, inv) if step else factor
            else:
                inverse = mul(tuple(piece[:NB] for piece in fac), inv)
        scaled = inverse * jnp.sqrt(6.0 * points / frob)
        high, mid, rest = [piece.astype(jnp.float32) for piece in pieces(energy)]
        top = ri[:NB]
        extra = jnp.where(top == 0, high, jnp.where(top == 1, mid, jnp.where(top == 2, rest, 0.0)))
        scaled = jnp.where((ci[:NB] & (2 * NB - 1)) == NB + top, extra, scaled)
        msg[...] = jnp.where(left[: NB // 2], scaled[: NB // 2], scaled[NB // 2 :]).astype(jnp.bfloat16)
        crecv[mine] = msg[...]

        for away in range(total - 1, 0, -1):
            coef_to(away).start()

    for tm_at in range(n):
        @pl.when(tm == tm_at)
        def _(tm_at=tm_at):
            settle(sendp.at[pl.ds(0, half_n * counts[tm_at])], psend.at[0])
            settle(sendb.at[pl.ds(0, (n - 1) * alone[tm_at] + (half_n - 1) * counts[tm_at])], asend.at[0])
            groups = sum(half_n // 2 if tm_at + side == half_n else half_n
                         for side in range(2) if 0 < tm_at + side < n)
            settle(scales.at[pl.ds(0, groups)], ssend.at[0])

    sent = jnp.where(owns, NF - 1, NF)
    settle_count(gpart, sent, gsend.at[0], [NF - 1, NF])
    settle_count(crecv, sent, crcv.at[0], [NF - 1, NF])

    lanes = lax.broadcasted_iota(jnp.int32, (NB, 2 * NB), 1)
    signs = jnp.where(lanes < NB, 1.0, -1.0).astype(jnp.bfloat16)
    hidden = lanes == NB + lax.broadcasted_iota(jnp.int32, (NB, 2 * NB), 0)
    wide_lane = lax.broadcasted_iota(jnp.int32, (1, NF), 1)
    energies = jnp.zeros((1, NF), jnp.float32)
    for f in range(NF):
        pairs = crecv[f]
        straight = jnp.concatenate([pairs[:, : 2 * NB], pairs[:, 2 * NB :]], axis=0)
        found = jnp.sum(jnp.where(hidden, straight.astype(jnp.float32), 0.0), axis=(0, 1), keepdims=True)
        energies = jnp.where(wide_lane == f, found, energies)
        straight = jnp.where(hidden, jnp.zeros_like(straight), straight)
        crossed = jnp.concatenate([straight[:, NB:], straight[:, :NB]], axis=1)
        stacked = jnp.concatenate([straight * signs, crossed], axis=0)
        tiled = jnp.concatenate([stacked] * 3, axis=1)
        full = jnp.dot(spread_ref[...], tiled, preferred_element_type=jnp.float32)
        full = (full * mask_ref[...]).astype(jnp.bfloat16)
        modes_ref[f * 6 * NB : (f + 1) * 6 * NB, :] = jnp.dot(
            full, spec[f], preferred_element_type=jnp.float32).astype(jnp.bfloat16)
    energy_ref[...] = energies

    @pl.when(owns)
    def _():
        settle(gath.at[pl.ds(0, total - 1)], csend.at[0])


def fused(n, nf_dev, chosen, snapshots, block_starts, freq_index):
    per, whole, shared, holders = chosen
    rows, count, wide = snapshots.shape
    total = n * nf_dev
    pw = wide // n
    slots = per + 4
    f32, bf16 = jnp.float32, jnp.bfloat16
    dma = pltpu.SemaphoreType.DMA
    vmem = pl.BlockSpec(memory_space=pltpu.VMEM)
    modes, energy = pl.pallas_call(
        functools.partial(kernel, n, nf_dev, per, whole, shared, holders, float(wide * nf_dev)),
        out_shape=(jax.ShapeDtypeStruct((NF * NB * 6, pw), bf16), jax.ShapeDtypeStruct((1, NF), f32)),
        in_specs=[pl.BlockSpec(memory_space=pltpu.HBM)] * 3,
        out_specs=(vmem, vmem),
        scratch_shapes=[
            pltpu.SMEM((NB,), jnp.int32),
            pltpu.SMEM((NF,), jnp.int32),
            pltpu.VMEM((slots * ROWS, rows), bf16),
            pltpu.VMEM((NB * 6, 2 * NB), bf16),
            pltpu.VMEM((NB * 6, 6 * NB), f32),
            pltpu.VMEM((n // 2, 3, rows, 2 * pw), bf16),
            pltpu.VMEM((n, slots * ROWS, 3 * pw), f32),
            pltpu.VMEM((slots * n, ROWS, 3 * pw), jnp.int16),
            pltpu.VMEM((slots * n, ROWS, 3 * pw), jnp.int16),
            pltpu.VMEM((n, slots, 128), f32),
            pltpu.VMEM((n, slots, 128), f32),
            pltpu.VMEM((slots * n, ROWS, 3 * pw), bf16),
            pltpu.VMEM((NB, ROWS, 3 * pw), bf16),
            pltpu.VMEM((3, NB * (ROWS + 8), pw), f32),
            pltpu.VMEM((NF, 6 * NB, pw), bf16),
            pltpu.VMEM((NF, NB // 4, 4 * NB), f32),
            pltpu.VMEM((total, NB // 4, 4 * NB), f32),
            pltpu.VMEM((NB // 2, 4 * NB), bf16),
            pltpu.VMEM((NF, NB // 2, 4 * NB), bf16),
            dma((2 + n // 2,)), dma((1,)), dma((n,)), dma((1,)), dma((n,)),
            dma((1,)), dma((1,)), dma((1,)), dma((1,)), dma((1,)), dma((1,)),
        ],
        compiler_params=pltpu.CompilerParams(
            collective_id=0, has_side_effects=True, vmem_limit_bytes=54_000_000),
    )(jnp.transpose(snapshots, (1, 0, 2)), block_starts, freq_index)
    modes = modes.reshape(NF, NB, 3, 2, pw).transpose(0, 1, 3, 2, 4)
    return modes, energy.reshape(NF)


def solution(mesh):
    n, nf_dev = mesh.shape["tm"], mesh.shape["freq"]

    def body(snapshots, block_starts, freq_index):
        rows, _, wide = snapshots.shape
        chosen = plan(n, rows, n * nf_dev, wide // n)
        if chosen is None:
            return local(snapshots, block_starts, freq_index)
        return fused(n, nf_dev, chosen, snapshots, block_starts, freq_index)

    return jax.shard_map(
        body,
        mesh=mesh,
        in_specs=(P("tm", None, "freq"), P(), P()),
        out_specs=(P(None, None, None, None, ("freq", "tm")), P()),
        check_vma=False,
    )
```

```python
import functools
import math

import jax
import jax.numpy as jnp
import numpy as np
from jax import lax
from jax.experimental import pallas as pl
from jax.experimental.pallas import tpu as pltpu
from jax.sharding import PartitionSpec as P

NB = 32
NFFT = 256
NF = 16
NSIT = 6


def for_sending(shard):
    return jax.tree.map(lambda a: a.astype(jnp.bfloat16) if a.dtype == jnp.float32 else a, shard)


def dft_rows(freq_index):
    times_idx = jnp.arange(NFFT, dtype=jnp.int32)
    phase_int = freq_index[:, None] * times_idx[None, :] % NFFT
    angles = 2.0 * math.pi / NFFT * phase_int.astype(jnp.float32)
    window = 0.5 - 0.5 * jnp.cos(2.0 * math.pi / NFFT * times_idx.astype(jnp.float32))
    scaling = 1.0 / jnp.sqrt(jnp.sum(window * window))
    cosine = window[None, :] * jnp.cos(angles) * scaling
    sine_rows = -window[None, :] * jnp.sin(angles) * scaling
    return jnp.stack([cosine, sine_rows], 1).reshape(2 * NF, NFFT).astype(jnp.bfloat16)


def block_rows(block_starts):
    return block_starts[:, None] + jnp.arange(NFFT, dtype=jnp.int32)[None, :]


def matmul_batch(left, right):
    return jnp.einsum("fij,fjk->fik", left, right, precision=lax.Precision.HIGHEST)


def whiten(summed, points):
    gram_re = summed[:, 0]
    gram_im = summed[:, 1]
    top_rows = jnp.concatenate([gram_re, -gram_im], 2)
    low_rows = jnp.concatenate([gram_im, gram_re], 2)
    hermit = jnp.concatenate([top_rows, low_rows], 1)
    frob = jnp.sqrt(jnp.sum(hermit * hermit, axis=(1, 2)) + 1e-06)
    identity = jnp.eye(2 * NB, dtype=jnp.float32)[None]
    iterate = hermit / frob[:, None, None]
    inverse = jnp.broadcast_to(identity, hermit.shape)
    for iteration in range(NSIT):
        factor = 1.5 * identity - 0.5 * matmul_batch(inverse, iterate)
        iterate = matmul_batch(iterate, factor)
        inverse = matmul_batch(factor, inverse)
    columns = inverse[:, :, :NB] * jnp.sqrt(6.0 * points / frob)[:, None, None]
    upper = columns[:, :NB]
    lower = columns[:, NB:]
    coefficients = jnp.stack([jnp.stack([upper, -lower], 1), jnp.stack([lower, upper], 1)], 1)
    energy = jnp.trace(gram_re, axis1=1, axis2=2) / (3.0 * NB * points)
    return (coefficients, energy)


def local(snapshots, block_starts, freq_index):
    dft_table = dft_rows(freq_index)
    offsets = block_rows(block_starts)
    series = lax.all_to_all(snapshots, "tm", split_axis=2, concat_axis=0, tiled=True)
    count = series.shape[1]
    width = series.shape[2]
    columns_all = series.reshape(series.shape[0], count * width)
    windows = jnp.take(columns_all, offsets, axis=0)
    spectra_part = jnp.einsum(
        "rt,btn->rbn", dft_table, windows, preferred_element_type=jnp.float32
    ).astype(jnp.bfloat16)
    spectra = spectra_part.reshape(2 * NF, NB, count, width)
    width = spectra.shape[3]
    points = float(width * lax.axis_size("tm") * lax.axis_size("freq"))
    flat_spec = spectra.reshape(NF, 2, NB, 3 * width)
    real_part = flat_spec[:, 0]
    imag_part = flat_spec[:, 1]
    gram_re = jnp.einsum("fbn,fcn->fbc", real_part, real_part, preferred_element_type=jnp.float32)
    gram_re = gram_re + jnp.einsum(
        "fbn,fcn->fbc", imag_part, imag_part, preferred_element_type=jnp.float32
    )
    cross_terms = jnp.einsum(
        "fbn,fcn->fbc", real_part, imag_part, preferred_element_type=jnp.float32
    )
    partial_gram = jnp.stack([gram_re, cross_terms - jnp.swapaxes(cross_terms, 1, 2)], 1)
    shared = lax.psum_scatter(partial_gram, "freq", scatter_dimension=0, tiled=True)
    shared = lax.psum(shared, "tm")
    coef_part, energy_part = whiten(shared, points)
    coefficients, energy = (
        lax.all_gather(for_sending(coef_part), "freq", axis=0, tiled=True).astype(coef_part.dtype),
        lax.all_gather(for_sending(energy_part), "freq", axis=0, tiled=True).astype(
            energy_part.dtype
        ),
    )
    coef_bf = jnp.transpose(coefficients.astype(jnp.bfloat16), (0, 4, 1, 2, 3))
    modes = jnp.einsum(
        "fjorb,frbn->fjon", coef_bf, flat_spec, preferred_element_type=jnp.float32
    ).astype(jnp.bfloat16)
    return (modes.reshape(NF, NB, 2, 3, width), energy)


MESH = pl.DeviceIdType.MESH
ROWS = 2 * NF
HOP = 128
JIT = 64


def plan(n, rows, total, width):
    if n < 2 or n % 2 or NB % n or total % (2 * NF) or width != 128 or rows % 16:
        return None
    per = NB // n
    if per < 4 or per % 2:
        return None
    slots = per + 4
    whole = [[] for _ in range(slots)]
    shared = [[] for _ in range(slots)]
    holders = []
    for block in range(NB):
        touched = [
            dev for dev in range(n)
            if HOP * block < rows * (dev + 1) and HOP * block + JIT + NFFT > rows * dev
        ]
        holders.append(touched)
        if len(touched) > 2:
            return None
        for dev in touched:
            slot = block - per * dev + 2
            if not 0 <= slot < slots:
                return None
            if len(touched) == 2:
                if (slot < slots // 2) != (dev == touched[1]):
                    return None
                shared[slot].append(dev)
            else:
                whole[slot].append(dev)
    return per, whole, shared, holders


def base_table(freqs_ref):
    row = lax.broadcasted_iota(jnp.int32, (ROWS, NFFT), 0)
    times_idx = lax.broadcasted_iota(jnp.int32, (ROWS, NFFT), 1)
    freqs = jnp.zeros((ROWS, NFFT), jnp.int32)
    for f in range(NF):
        freqs = jnp.where((row >> 1) == f, freqs_ref[f], freqs)
    phase = (freqs * times_idx) & (NFFT - 1)
    angles = 2.0 * math.pi / NFFT * phase.astype(jnp.float32)
    window = 0.5 - 0.5 * jnp.cos(2.0 * math.pi / NFFT * times_idx.astype(jnp.float32))
    hann = 0.5 - 0.5 * np.cos(2.0 * math.pi / NFFT * np.arange(NFFT))
    scaling = np.float32(1.0 / np.sqrt(np.sum(hann * hann)))
    cosine = window * jnp.cos(angles) * scaling
    sine = -window * jnp.sin(angles) * scaling
    return jnp.where((row & 1) == 1, sine, cosine).astype(jnp.bfloat16)


def shifted(base, shift, rows):
    source = lax.broadcasted_iota(jnp.int32, (NFFT, rows), 0)
    target = lax.broadcasted_iota(jnp.int32, (NFFT, rows), 1)
    pick = jnp.where(source - target == shift, 1.0, 0.0).astype(jnp.bfloat16)
    return jnp.dot(base, pick, preferred_element_type=jnp.float32).astype(jnp.bfloat16)


def member(index, devs):
    if not devs:
        return None
    if devs == list(range(devs[0], devs[-1] + 1)):
        return (index >= devs[0]) & (index <= devs[-1])
    hit = index == devs[0]
    for dev in devs[1:]:
        hit = hit | (index == dev)
    return hit


def division(n, tm, side, dest):
    edge, half = tm + side, n // 2
    middle = edge == half
    left = dest < half
    all_mine = middle & (left == (tm < half))
    theirs = (middle & (all_mine ^ True)) | ((middle ^ True) & (dest % 2 != tm % 2))
    return theirs, middle, all_mine


def kernel(n, nf_dev, per, whole, shared, holders, points, x_hbm, starts_hbm, freqs_hbm,
           modes_ref, energy_ref, starts_ref, freqs_ref, t_ref, stage, xv, parts,
           sendp, others, scales, oscales, sendb, recvb, spec32, spec, gpart, gath, msg, crecv,
           load_sem, psend, precv, ssend, srecv, asend, arecv, gsend, grecv, csend, crcv):
    tm = lax.axis_index("tm")
    fr = lax.axis_index("freq")
    total = n * nf_dev
    lin = tm * nf_dev + fr
    step, lowest = total // (2 * NF), total // 4
    slots = per + 4
    half_slots = slots // 2
    mine = (lin - lowest) // step
    owns = (lin >= lowest) & (lin < lowest + NF * step) & ((lin - lowest) % step == 0)
    half_n = n // 2
    parity = tm % 2
    rows = xv.shape[2]
    pw = xv.shape[3] // 2

    def owner(f):
        return lowest + f * step

    def where_is(index):
        return {"tm": index // nf_dev, "freq": index % nf_dev}

    def displaced(away):
        row, col = tm + away // nf_dev, fr + away % nf_dev
        return {"tm": jnp.where(row >= n, row - n, row),
                "freq": jnp.where(col >= nf_dev, col - nf_dev, col)}

    def group(k):
        return jnp.where(tm < half_n, half_n - 1 - k, k)

    def load(g, c):
        return pltpu.make_async_copy(
            x_hbm.at[c, :, pl.ds(pl.multiple_of(g * 2 * pw, 2 * pw), 2 * pw)], xv.at[g, c],
            load_sem.at[2 + g])

    small = pltpu.make_async_copy(freqs_hbm, freqs_ref, load_sem.at[0])
    small.start()
    starts = pltpu.make_async_copy(starts_hbm, starts_ref, load_sem.at[1])
    starts.start()
    for k in range(half_n):
        for c in range(3):
            load(group(k), c).start()
    barrier = pltpu.get_barrier_semaphore()

    for away in range(total - 1, 0, -1):
        pl.semaphore_signal(barrier, inc=1, device_id=displaced(away), device_id_type=MESH)

    small.wait()
    base = base_table(freqs_ref)
    starts.wait()
    for slot in range(slots):
        block = per * tm + slot - 2
        start = starts_ref[jnp.clip(block, 0, NB - 1)]
        inside = (block >= 0) & (block < NB)
        shift = jnp.where(inside, rows * tm - start, 4 * (rows + NFFT))
        t_ref[slot * ROWS : (slot + 1) * ROWS, :] = shifted(base, shift, rows)
    scales[...] = jnp.zeros_like(scales)

    def low(slot):
        return slot < half_slots

    def pick(flag, yes, no):
        return (yes if flag else no) if isinstance(flag, bool) else jnp.where(flag, yes, no)

    def partner(slot):
        return pick(low(slot), (tm + n - 1) % n, (tm + 1) % n)

    def across(slot):
        return pick(low(slot), slot + per, slot - per)

    def is_shared(slot):
        block = per * tm + slot - 2
        edge = rows * (tm + pick(low(slot), 0, 1))
        inside = (block >= 0) & (block < NB) & (edge > 0) & (edge < rows * n)
        return inside & (HOP * block < edge) & (HOP * block + JIT + NFFT > edge)

    def is_theirs(slot, dest):
        return division(n, tm, slot // half_slots, dest)[0]

    def exchange(slot, dest):
        return pltpu.make_async_remote_copy(
            src_ref=sendp.at[slot * n + dest], dst_ref=others.at[across(slot) * n + dest],
            send_sem=psend.at[0], recv_sem=precv.at[across(slot) // half_slots * half_n + dest // 2],
            device_id={"tm": partner(slot), "freq": fr}, device_id_type=MESH)

    def scale_copy(side, g):
        return pltpu.make_async_remote_copy(
            src_ref=scales.at[side * half_n + g], dst_ref=oscales.at[(1 - side) * half_n + g],
            send_sem=ssend.at[0], recv_sem=srecv.at[(1 - side) * half_n + g],
            device_id={"tm": partner(side * half_slots), "freq": fr}, device_id_type=MESH)

    def scatter(slot, dest):
        return pltpu.make_async_remote_copy(
            src_ref=sendb.at[slot * n + dest], dst_ref=recvb.at[per * tm + slot - 2],
            send_sem=asend.at[0], recv_sem=arecv.at[0],
            device_id={"tm": dest, "freq": fr}, device_id_type=MESH)

    def settle(ref, sem):
        pltpu.make_async_copy(ref, ref, sem).wait()

    def settle_count(ref, count, sem, options):
        for option in sorted(set(options)):
            @pl.when(count == option)
            def _(option=option):
                settle(ref.at[pl.ds(0, option)], sem)

    def edge_exists(side):
        return pick(side == 0, tm > 0, tm < n - 1)

    def sharing(side):
        return sum(jnp.where(is_shared(side * half_slots + k), 1, 0) for k in range(half_slots))

    def deliver(slot, dest, value):
        value = value.astype(jnp.bfloat16)

        @pl.when(dest == tm)
        def _():
            recvb[per * tm + slot - 2] = value

        @pl.when(dest != tm)
        def _():
            sendb[slot * n + dest] = value
            scatter(slot, dest).start()

    diagonal = (lax.broadcasted_iota(jnp.int32, (ROWS, 128), 0)
                == lax.broadcasted_iota(jnp.int32, (ROWS, 128), 1))

    def encode(slot, g, d):
        value = parts[2 * g + d, slot * ROWS : (slot + 1) * ROWS, :]
        peak = jnp.maximum(jnp.max(jnp.abs(value), axis=1, keepdims=True), 1e-30)
        whole_numbers = (value * (32767.0 / peak) + 12582912.0) - 12582912.0
        sendp[slot * n + 2 * g + d] = whole_numbers.astype(jnp.int32).astype(jnp.int16)
        line = jnp.sum(jnp.where(diagonal, peak, 0.0), axis=0, keepdims=True)
        row = 2 * (slot % half_slots) + d
        scales[slot // half_slots * half_n + g, row : row + 1, :] = line

    @pl.loop(0, half_n)
    def _(k):
        g = group(k)
        settle(xv.at[g], load_sem.at[2 + g])
        for c in range(3):
            part = jnp.dot(t_ref[...], xv[g, c], preferred_element_type=jnp.float32)
            for d in range(2):
                parts[2 * g + d, :, c * pw : (c + 1) * pw] = part[:, d * pw : (d + 1) * pw]

        @pl.when(k == 0)
        def _():
            pl.semaphore_wait(barrier, total - 1)

        for d in range(2):
            for slot in range(slots):
                if shared[slot]:
                    @pl.when(member(tm, shared[slot]) & is_theirs(slot, 2 * g + d))
                    def _(slot=slot, d=d):
                        encode(slot, g, d)

        for side in range(2):
            _, whole_group, all_mine = division(n, tm, side, 2 * g)

            @pl.when(edge_exists(side) & jnp.logical_not(whole_group & all_mine))
            def _(side=side):
                scale_copy(side, g).start()

        for d in range(2):
            for slot in range(slots):
                if shared[slot]:
                    @pl.when(member(tm, shared[slot]) & is_theirs(slot, 2 * g + d) & (parity == (0 if slot >= half_slots else 1)))
                    def _(slot=slot, d=d):
                        exchange(slot, 2 * g + d).start()

        for d in range(2):
            for slot in range(slots):
                if whole[slot]:
                    @pl.when(member(tm, whole[slot]) & (parity == d))
                    def _(slot=slot, d=d):
                        deliver(slot, 2 * g + d, parts[2 * g + d, slot * ROWS : (slot + 1) * ROWS, :])

        for d in range(2):
            for slot in range(slots):
                if shared[slot]:
                    @pl.when(member(tm, shared[slot]) & is_theirs(slot, 2 * g + d) & (parity == (1 if slot >= half_slots else 0)))
                    def _(slot=slot, d=d):
                        exchange(slot, 2 * g + d).start()

    def send_crossing():
        @pl.loop(0, half_n)
        def _(k):
            dest = 2 * group(k) + 1 - parity
            for slot in range(slots):
                if whole[slot]:
                    @pl.when(member(tm, whole[slot]))
                    def _(slot=slot):
                        deliver(slot, dest, parts[dest, slot * ROWS : (slot + 1) * ROWS, :])

    counts = [sum(tm_at in devs for devs in shared) for tm_at in range(n)]

    @pl.loop(0, 2)
    def _(turn):
        side = jnp.where(turn == 0, 1 - parity, parity)

        @pl.loop(0, half_n)
        def _(k):
            g = group(k)
            _, whole_group, all_mine = division(n, tm, side, 2 * g)

            @pl.when(edge_exists(side) & (jnp.logical_not(whole_group) | all_mine))
            def _():
                settle(oscales.at[side * half_n + g], srecv.at[side * half_n + g])
                settle_count(others, sharing(side) * jnp.where(whole_group, 2, 1), precv.at[side * half_n + g],
                             [count * twice for count in range(1, half_slots + 1) for twice in (1, 2)])
                for d in range(2):
                    dest = 2 * g + d
                    for index in range(half_slots):
                        slot = side * half_slots + index

                        @pl.when(is_shared(slot) & jnp.logical_not(is_theirs(slot, dest)))
                        def _(slot=slot, dest=dest, row=2 * index + d):
                            line = oscales[side * half_n + g, row : row + 1, :]
                            peak = jnp.sum(jnp.where(diagonal, line, 0.0), axis=1, keepdims=True)
                            other = others[slot * n + dest].astype(jnp.int32).astype(jnp.float32)
                            here = parts[dest, pl.ds(pl.multiple_of(slot * ROWS, ROWS), ROWS), :]
                            deliver(slot, dest, here + other * (peak * (1.0 / 32767.0)))


            @pl.when((turn == 0) & (k == half_n - 1))
            def _():
                send_crossing()

    alone = [sum(tm_at in devs for devs in whole) for tm_at in range(n)]
    for tm_at in range(n):
        @pl.when(tm == tm_at)
        def _(tm_at=tm_at):
            settle(recvb.at[pl.ds(0, NB - alone[tm_at] - counts[tm_at])], arecv.at[0])

    pitch = spec32.shape[1] // NB
    for block in range(NB):
        values = recvb[block]
        for c in range(3):
            spec32[c, block * pitch : block * pitch + ROWS, :] = values[:, c * 128 : (c + 1) * 128].astype(jnp.float32)

    def to_owner(f):
        return pltpu.make_async_remote_copy(
            src_ref=gpart.at[f], dst_ref=gath.at[lin], send_sem=gsend.at[0],
            recv_sem=grecv.at[0], device_id=where_is(owner(f)), device_id_type=MESH)

    upper = lax.broadcasted_iota(jnp.int32, (NB, NB), 1) >= lax.broadcasted_iota(jnp.int32, (NB, NB), 0)
    for f in range(NF):
        real, imag = [jnp.concatenate([
            spec32[c, pl.ds(2 * f + r, NB, stride=pitch), :].astype(jnp.bfloat16)
            for c in range(3)], axis=1) for r in range(2)]
        spec[f, :NB, :] = real
        spec[f, NB:, :] = imag
        lhs = jnp.concatenate([real, imag], axis=1)
        rhs = jnp.concatenate([lhs, jnp.concatenate([imag, -real], axis=1)], axis=0)
        gram = lax.dot_general(lhs, rhs, (((1,), (1,)), ((), ())), preferred_element_type=jnp.float32)
        packed = jnp.where(upper, gram[:, :NB], gram[:, NB:])
        gpart[f] = jnp.concatenate([packed[8 * q : 8 * q + 8] for q in range(NB // 8)], axis=1)
        if f % 4 == 3:
            for sent in range(f - 3, f + 1):
                @pl.when(lin != owner(sent))
                def _(sent=sent):
                    to_owner(sent).start()

    def coef_to(away):
        return pltpu.make_async_remote_copy(
            src_ref=msg, dst_ref=crecv.at[mine], send_sem=csend.at[0],
            recv_sem=crcv.at[0], device_id=displaced(away), device_id_type=MESH)

    @pl.when(owns)
    def _():
        gath[lin] = gpart[mine]

        settle(gath.at[pl.ds(0, total - 1)], grecv.at[0])
        packed = jnp.sum(gath[...], axis=0)
        square = jnp.concatenate([packed[:, q * NB : (q + 1) * NB] for q in range(NB // 8)], axis=0)
        flipped = jnp.transpose(square)
        ri = lax.broadcasted_iota(jnp.int32, (NB, NB), 0)
        ci = lax.broadcasted_iota(jnp.int32, (NB, NB), 1)
        gram_re = jnp.where(ci >= ri, square, flipped)
        gram_im = jnp.where(ci < ri, square, jnp.where(ci > ri, -flipped, 0.0))
        energy = jnp.sum(jnp.where(ri == ci, gram_re, 0.0), axis=(0, 1), keepdims=True) / (3.0 * NB * points)
        hermit = jnp.concatenate([
            jnp.concatenate([gram_re, -gram_im, gram_re, -gram_im], axis=1),
            jnp.concatenate([gram_im, gram_re, gram_im, gram_re], axis=1)], axis=0)
        frob = jnp.sqrt(0.5 * jnp.sum(hermit * hermit, axis=(0, 1), keepdims=True) + 1e-06)
        ri = lax.broadcasted_iota(jnp.int32, (2 * NB, 4 * NB), 0)
        ci = lax.broadcasted_iota(jnp.int32, (2 * NB, 4 * NB), 1)
        left = ci < 2 * NB
        identity = jnp.where(ri == (ci & (2 * NB - 1)), 1.0, 0.0).astype(jnp.float32)

        def pieces(a):
            high = a.astype(jnp.bfloat16)
            rest = a - high.astype(jnp.float32)
            mid = rest.astype(jnp.bfloat16)
            return high, mid, (rest - mid.astype(jnp.float32)).astype(jnp.bfloat16)

        def mul(a, b):
            ah, am, al = a
            bh, bm, bl = b
            lhs = jnp.concatenate([ah, am, jnp.where(left[: ah.shape[0]], ah, al)], axis=1)
            rhs = jnp.concatenate([bh, bm, bh, bm, bl, bh], axis=0)
            return jnp.dot(lhs, rhs, preferred_element_type=jnp.float32)

        iterate = hermit / frob
        inverse = identity
        for step in range(NSIT):
            it = pieces(iterate)
            if step:
                inv = pieces(inverse)
            factor = 1.5 * identity - 0.5 * (mul(inv, it) if step else iterate)
            fac = pieces(factor)
            if step < NSIT - 1:
                iterate = mul(it, fac)
                inverse = mul(fac, inv) if step else factor
            else:
                inverse = mul(tuple(piece[:NB] for piece in fac), inv)
        scaled = inverse * jnp.sqrt(6.0 * points / frob)
        high, mid, rest = [piece.astype(jnp.float32) for piece in pieces(energy)]
        top = ri[:NB]
        extra = jnp.where(top == 0, high, jnp.where(top == 1, mid, jnp.where(top == 2, rest, 0.0)))
        scaled = jnp.where((ci[:NB] & (2 * NB - 1)) == NB + top, extra, scaled)
        msg[...] = jnp.where(left[: NB // 2], scaled[: NB // 2], scaled[NB // 2 :]).astype(jnp.bfloat16)
        crecv[mine] = msg[...]

        for away in range(total - 1, 0, -1):
            coef_to(away).start()

    for tm_at in range(n):
        handed, groups = 0, 0
        for slot in range(slots):
            if tm_at in shared[slot]:
                handed += sum(division(n, tm_at, slot // half_slots, dest)[0] for dest in range(n))
        for side in range(2):
            if 0 < tm_at + side < n:
                for g in range(half_n):
                    _, whole_group, all_mine = division(n, tm_at, side, 2 * g)
                    groups += not (whole_group and all_mine)

        @pl.when(tm == tm_at)
        def _(tm_at=tm_at, handed=handed, groups=groups):
            settle(sendp.at[pl.ds(0, handed)], psend.at[0])
            own = n * (alone[tm_at] + counts[tm_at]) - handed
            settle(sendb.at[pl.ds(0, own - alone[tm_at] - counts[tm_at])], asend.at[0])
            settle(scales.at[pl.ds(0, groups)], ssend.at[0])

    sent = jnp.where(owns, NF - 1, NF)
    settle_count(gpart, sent, gsend.at[0], [NF - 1, NF])
    settle_count(crecv, sent, crcv.at[0], [NF - 1, NF])

    lanes = lax.broadcasted_iota(jnp.int32, (NB, 2 * NB), 1)
    signs = jnp.where(lanes < NB, 1.0, -1.0).astype(jnp.bfloat16)
    hidden = lanes == NB + lax.broadcasted_iota(jnp.int32, (NB, 2 * NB), 0)
    wide_lane = lax.broadcasted_iota(jnp.int32, (1, NF), 1)
    energies = jnp.zeros((1, NF), jnp.float32)
    for f in range(NF):
        pairs = crecv[f]
        straight = jnp.concatenate([pairs[:, : 2 * NB], pairs[:, 2 * NB :]], axis=0)
        found = jnp.sum(jnp.where(hidden, straight.astype(jnp.float32), 0.0), axis=(0, 1), keepdims=True)
        energies = jnp.where(wide_lane == f, found, energies)
        straight = jnp.where(hidden, jnp.zeros_like(straight), straight)
        crossed = jnp.concatenate([straight[:, NB:], straight[:, :NB]], axis=1)
        stacked = jnp.concatenate([straight * signs, crossed], axis=0)
        out = jnp.dot(stacked, spec[f], preferred_element_type=jnp.float32)
        for c in range(3):
            for o in range(2):
                stage[f % 4, pl.ds(2 * c + o, NB, stride=6), :] = out[o * NB : (o + 1) * NB, c * pw : (c + 1) * pw]
        modes_ref[f * 6 * NB : (f + 1) * 6 * NB, :] = stage[f % 4].astype(jnp.bfloat16)
    energy_ref[...] = energies

    @pl.when(owns)
    def _():
        settle(gath.at[pl.ds(0, total - 1)], csend.at[0])


def fused(n, nf_dev, chosen, snapshots, block_starts, freq_index):
    per, whole, shared, holders = chosen
    rows, count, wide = snapshots.shape
    total = n * nf_dev
    pw = wide // n
    slots = per + 4
    f32, bf16 = jnp.float32, jnp.bfloat16
    dma = pltpu.SemaphoreType.DMA
    vmem = pl.BlockSpec(memory_space=pltpu.VMEM)
    modes, energy = pl.pallas_call(
        functools.partial(kernel, n, nf_dev, per, whole, shared, holders, float(wide * nf_dev)),
        out_shape=(jax.ShapeDtypeStruct((NF * NB * 6, pw), bf16), jax.ShapeDtypeStruct((1, NF), f32)),
        in_specs=[pl.BlockSpec(memory_space=pltpu.HBM)] * 3,
        out_specs=(vmem, vmem),
        scratch_shapes=[
            pltpu.SMEM((NB,), jnp.int32),
            pltpu.SMEM((NF,), jnp.int32),
            pltpu.VMEM((slots * ROWS, rows), bf16),
            pltpu.VMEM((4, 6 * NB, pw), f32),
            pltpu.VMEM((n // 2, 3, rows, 2 * pw), bf16),
            pltpu.VMEM((n, slots * ROWS, 3 * pw), f32),
            pltpu.VMEM((slots * n, ROWS, 3 * pw), jnp.int16),
            pltpu.VMEM((slots * n, ROWS, 3 * pw), jnp.int16),
            pltpu.VMEM((n, slots, 128), f32),
            pltpu.VMEM((n, slots, 128), f32),
            pltpu.VMEM((slots * n, ROWS, 3 * pw), bf16),
            pltpu.VMEM((NB, ROWS, 3 * pw), bf16),
            pltpu.VMEM((3, NB * (ROWS + 8), pw), f32),
            pltpu.VMEM((NF, 2 * NB, 3 * pw), bf16),
            pltpu.VMEM((NF, NB // 4, 4 * NB), f32),
            pltpu.VMEM((total, NB // 4, 4 * NB), f32),
            pltpu.VMEM((NB // 2, 4 * NB), bf16),
            pltpu.VMEM((NF, NB // 2, 4 * NB), bf16),
            dma((2 + n // 2,)), dma((1,)), dma((n,)), dma((1,)), dma((n,)),
            dma((1,)), dma((1,)), dma((1,)), dma((1,)), dma((1,)), dma((1,)),
        ],
        compiler_params=pltpu.CompilerParams(
            collective_id=0, has_side_effects=True, vmem_limit_bytes=54_000_000),
    )(jnp.transpose(snapshots, (1, 0, 2)), block_starts, freq_index)
    modes = modes.reshape(NF, NB, 3, 2, pw).transpose(0, 1, 3, 2, 4)
    return modes, energy.reshape(NF)


def solution(mesh):
    n, nf_dev = mesh.shape["tm"], mesh.shape["freq"]

    def body(snapshots, block_starts, freq_index):
        rows, _, wide = snapshots.shape
        chosen = plan(n, rows, n * nf_dev, wide // n)
        if chosen is None:
            return local(snapshots, block_starts, freq_index)
        return fused(n, nf_dev, chosen, snapshots, block_starts, freq_index)

    return jax.shard_map(
        body,
        mesh=mesh,
        in_specs=(P("tm", None, "freq"), P(), P()),
        out_specs=(P(None, None, None, None, ("freq", "tm")), P()),
        check_vma=False,
    )
```

```python
import functools
import math

import jax
import jax.numpy as jnp
import numpy as np
from jax import lax
from jax.experimental import pallas as pl
from jax.experimental.pallas import tpu as pltpu
from jax.sharding import PartitionSpec as P

NB = 32
NFFT = 256
NF = 16
NSIT = 6


def for_sending(shard):
    return jax.tree.map(lambda a: a.astype(jnp.bfloat16) if a.dtype == jnp.float32 else a, shard)


def dft_rows(freq_index):
    times_idx = jnp.arange(NFFT, dtype=jnp.int32)
    phase_int = freq_index[:, None] * times_idx[None, :] % NFFT
    angles = 2.0 * math.pi / NFFT * phase_int.astype(jnp.float32)
    window = 0.5 - 0.5 * jnp.cos(2.0 * math.pi / NFFT * times_idx.astype(jnp.float32))
    scaling = 1.0 / jnp.sqrt(jnp.sum(window * window))
    cosine = window[None, :] * jnp.cos(angles) * scaling
    sine_rows = -window[None, :] * jnp.sin(angles) * scaling
    return jnp.stack([cosine, sine_rows], 1).reshape(2 * NF, NFFT).astype(jnp.bfloat16)


def block_rows(block_starts):
    return block_starts[:, None] + jnp.arange(NFFT, dtype=jnp.int32)[None, :]


def matmul_batch(left, right):
    return jnp.einsum("fij,fjk->fik", left, right, precision=lax.Precision.HIGHEST)


def whiten(summed, points):
    gram_re = summed[:, 0]
    gram_im = summed[:, 1]
    top_rows = jnp.concatenate([gram_re, -gram_im], 2)
    low_rows = jnp.concatenate([gram_im, gram_re], 2)
    hermit = jnp.concatenate([top_rows, low_rows], 1)
    frob = jnp.sqrt(jnp.sum(hermit * hermit, axis=(1, 2)) + 1e-06)
    identity = jnp.eye(2 * NB, dtype=jnp.float32)[None]
    iterate = hermit / frob[:, None, None]
    inverse = jnp.broadcast_to(identity, hermit.shape)
    for iteration in range(NSIT):
        factor = 1.5 * identity - 0.5 * matmul_batch(inverse, iterate)
        iterate = matmul_batch(iterate, factor)
        inverse = matmul_batch(factor, inverse)
    columns = inverse[:, :, :NB] * jnp.sqrt(6.0 * points / frob)[:, None, None]
    upper = columns[:, :NB]
    lower = columns[:, NB:]
    coefficients = jnp.stack([jnp.stack([upper, -lower], 1), jnp.stack([lower, upper], 1)], 1)
    energy = jnp.trace(gram_re, axis1=1, axis2=2) / (3.0 * NB * points)
    return (coefficients, energy)


def local(snapshots, block_starts, freq_index):
    dft_table = dft_rows(freq_index)
    offsets = block_rows(block_starts)
    series = lax.all_to_all(snapshots, "tm", split_axis=2, concat_axis=0, tiled=True)
    count = series.shape[1]
    width = series.shape[2]
    columns_all = series.reshape(series.shape[0], count * width)
    windows = jnp.take(columns_all, offsets, axis=0)
    spectra_part = jnp.einsum(
        "rt,btn->rbn", dft_table, windows, preferred_element_type=jnp.float32
    ).astype(jnp.bfloat16)
    spectra = spectra_part.reshape(2 * NF, NB, count, width)
    width = spectra.shape[3]
    points = float(width * lax.axis_size("tm") * lax.axis_size("freq"))
    flat_spec = spectra.reshape(NF, 2, NB, 3 * width)
    real_part = flat_spec[:, 0]
    imag_part = flat_spec[:, 1]
    gram_re = jnp.einsum("fbn,fcn->fbc", real_part, real_part, preferred_element_type=jnp.float32)
    gram_re = gram_re + jnp.einsum(
        "fbn,fcn->fbc", imag_part, imag_part, preferred_element_type=jnp.float32
    )
    cross_terms = jnp.einsum(
        "fbn,fcn->fbc", real_part, imag_part, preferred_element_type=jnp.float32
    )
    partial_gram = jnp.stack([gram_re, cross_terms - jnp.swapaxes(cross_terms, 1, 2)], 1)
    shared = lax.psum_scatter(partial_gram, "freq", scatter_dimension=0, tiled=True)
    shared = lax.psum(shared, "tm")
    coef_part, energy_part = whiten(shared, points)
    coefficients, energy = (
        lax.all_gather(for_sending(coef_part), "freq", axis=0, tiled=True).astype(coef_part.dtype),
        lax.all_gather(for_sending(energy_part), "freq", axis=0, tiled=True).astype(
            energy_part.dtype
        ),
    )
    coef_bf = jnp.transpose(coefficients.astype(jnp.bfloat16), (0, 4, 1, 2, 3))
    modes = jnp.einsum(
        "fjorb,frbn->fjon", coef_bf, flat_spec, preferred_element_type=jnp.float32
    ).astype(jnp.bfloat16)
    return (modes.reshape(NF, NB, 2, 3, width), energy)


MESH = pl.DeviceIdType.MESH
ROWS = 2 * NF
HOP = 128
JIT = 64


def plan(n, rows, total, width):
    if n < 2 or n % 2 or NB % n or total % (2 * NF) or width != 128 or rows % 16:
        return None
    per = NB // n
    if per < 4 or per % 2:
        return None
    slots = per + 4
    whole = [[] for _ in range(slots)]
    shared = [[] for _ in range(slots)]
    holders = []
    for block in range(NB):
        touched = [
            dev for dev in range(n)
            if HOP * block < rows * (dev + 1) and HOP * block + JIT + NFFT > rows * dev
        ]
        holders.append(touched)
        if len(touched) > 2:
            return None
        for dev in touched:
            slot = block - per * dev + 2
            if not 0 <= slot < slots:
                return None
            if len(touched) == 2:
                if (slot < slots // 2) != (dev == touched[1]):
                    return None
                shared[slot].append(dev)
            else:
                whole[slot].append(dev)
    return per, whole, shared, holders


def base_table(ints_ref):
    row = lax.broadcasted_iota(jnp.int32, (ROWS, NFFT), 0)
    times_idx = lax.broadcasted_iota(jnp.int32, (ROWS, NFFT), 1)
    freqs = jnp.zeros((ROWS, NFFT), jnp.int32)
    for f in range(NF):
        freqs = jnp.where((row >> 1) == f, ints_ref[NB + f], freqs)
    phase = (freqs * times_idx) & (NFFT - 1)
    angles = 2.0 * math.pi / NFFT * phase.astype(jnp.float32)
    window = 0.5 - 0.5 * jnp.cos(2.0 * math.pi / NFFT * times_idx.astype(jnp.float32))
    hann = 0.5 - 0.5 * np.cos(2.0 * math.pi / NFFT * np.arange(NFFT))
    scaling = np.float32(1.0 / np.sqrt(np.sum(hann * hann)))
    cosine = window * jnp.cos(angles) * scaling
    sine = -window * jnp.sin(angles) * scaling
    return jnp.where((row & 1) == 1, sine, cosine).astype(jnp.bfloat16)


def shifted(base, shift, rows):
    source = lax.broadcasted_iota(jnp.int32, (NFFT, rows), 0)
    target = lax.broadcasted_iota(jnp.int32, (NFFT, rows), 1)
    pick = jnp.where(source - target == shift, 1.0, 0.0).astype(jnp.bfloat16)
    return jnp.dot(base, pick, preferred_element_type=jnp.float32).astype(jnp.bfloat16)


def member(index, devs):
    if not devs:
        return None
    if devs == list(range(devs[0], devs[-1] + 1)):
        return (index >= devs[0]) & (index <= devs[-1])
    hit = index == devs[0]
    for dev in devs[1:]:
        hit = hit | (index == dev)
    return hit


def division(n, tm, side, dest):
    edge, half = tm + side, n // 2
    middle = edge == half
    left = dest < half
    all_mine = middle & (left == (tm < half))
    theirs = (middle & (all_mine ^ True)) | ((middle ^ True) & (dest % 2 != tm % 2))
    return theirs, middle, all_mine


def kernel(n, nf_dev, per, whole, shared, holders, points, x_hbm, ints_hbm,
           spec, coefs_ref, ints_ref, t_ref, xv, parts,
           sendp, others, scales, oscales, sendb, recvb, spec32, gpart, gath, msg, crecv,
           load_sem, psend, precv, ssend, srecv, asend, arecv, gsend, grecv, csend, crcv):
    tm = lax.axis_index("tm")
    fr = lax.axis_index("freq")
    total = n * nf_dev
    lin = tm * nf_dev + fr
    step, lowest = total // (2 * NF), total // 4
    slots = per + 4
    half_slots = slots // 2
    mine = (lin - lowest) // step
    owns = (lin >= lowest) & (lin < lowest + NF * step) & ((lin - lowest) % step == 0)
    half_n = n // 2
    parity = tm % 2
    rows = xv.shape[2]
    pw = xv.shape[3] // 2

    def owner(f):
        return lowest + f * step

    def where_is(index):
        return {"tm": index // nf_dev, "freq": index % nf_dev}

    def displaced(away):
        row, col = tm + away // nf_dev, fr + away % nf_dev
        return {"tm": jnp.where(row >= n, row - n, row),
                "freq": jnp.where(col >= nf_dev, col - nf_dev, col)}

    def group(k):
        return jnp.where(tm < half_n, half_n - 1 - k, k)

    def load(g, c):
        return pltpu.make_async_copy(
            x_hbm.at[c, :, pl.ds(pl.multiple_of(g * 2 * pw, 2 * pw), 2 * pw)], xv.at[g, c],
            load_sem.at[1 + g])

    small = pltpu.make_async_copy(ints_hbm, ints_ref, load_sem.at[0])
    small.start()
    for k in range(half_n):
        for c in range(3):
            load(group(k), c).start()
    barrier = pltpu.get_barrier_semaphore()

    for away in range(total - 1, 0, -1):
        pl.semaphore_signal(barrier, inc=1, device_id=displaced(away), device_id_type=MESH)

    small.wait()
    base = base_table(ints_ref)
    for slot in range(slots):
        block = per * tm + slot - 2
        start = ints_ref[jnp.clip(block, 0, NB - 1)]
        inside = (block >= 0) & (block < NB)
        shift = jnp.where(inside, rows * tm - start, 4 * (rows + NFFT))
        t_ref[slot * ROWS : (slot + 1) * ROWS, :] = shifted(base, shift, rows)
    scales[...] = jnp.zeros_like(scales)

    def low(slot):
        return slot < half_slots

    def pick(flag, yes, no):
        return (yes if flag else no) if isinstance(flag, bool) else jnp.where(flag, yes, no)

    def partner(slot):
        return pick(low(slot), (tm + n - 1) % n, (tm + 1) % n)

    def across(slot):
        return pick(low(slot), slot + per, slot - per)

    def is_shared(slot):
        block = per * tm + slot - 2
        edge = rows * (tm + pick(low(slot), 0, 1))
        inside = (block >= 0) & (block < NB) & (edge > 0) & (edge < rows * n)
        return inside & (HOP * block < edge) & (HOP * block + JIT + NFFT > edge)

    def is_theirs(slot, dest):
        return division(n, tm, slot // half_slots, dest)[0]

    def exchange(slot, dest):
        return pltpu.make_async_remote_copy(
            src_ref=sendp.at[slot * n + dest], dst_ref=others.at[across(slot) * n + dest],
            send_sem=psend.at[0], recv_sem=precv.at[across(slot) // half_slots * half_n + dest // 2],
            device_id={"tm": partner(slot), "freq": fr}, device_id_type=MESH)

    def scale_copy(side, g):
        return pltpu.make_async_remote_copy(
            src_ref=scales.at[side * half_n + g], dst_ref=oscales.at[(1 - side) * half_n + g],
            send_sem=ssend.at[0], recv_sem=srecv.at[(1 - side) * half_n + g],
            device_id={"tm": partner(side * half_slots), "freq": fr}, device_id_type=MESH)

    def scatter(slot, dest):
        return pltpu.make_async_remote_copy(
            src_ref=sendb.at[slot * n + dest], dst_ref=recvb.at[per * tm + slot - 2],
            send_sem=asend.at[0], recv_sem=arecv.at[0],
            device_id={"tm": dest, "freq": fr}, device_id_type=MESH)

    def settle(ref, sem):
        pltpu.make_async_copy(ref, ref, sem).wait()

    def settle_count(ref, count, sem, options):
        for option in sorted(set(options)):
            @pl.when(count == option)
            def _(option=option):
                settle(ref.at[pl.ds(0, option)], sem)

    def edge_exists(side):
        return pick(side == 0, tm > 0, tm < n - 1)

    def sharing(side):
        return sum(jnp.where(is_shared(side * half_slots + k), 1, 0) for k in range(half_slots))

    def deliver(slot, dest, value):
        value = value.astype(jnp.bfloat16)

        @pl.when(dest == tm)
        def _():
            recvb[per * tm + slot - 2] = value

        @pl.when(dest != tm)
        def _():
            sendb[slot * n + dest] = value
            scatter(slot, dest).start()

    diagonal = (lax.broadcasted_iota(jnp.int32, (ROWS, 128), 0)
                == lax.broadcasted_iota(jnp.int32, (ROWS, 128), 1))

    def encode(slot, g, d):
        value = parts[2 * g + d, slot * ROWS : (slot + 1) * ROWS, :]
        peak = jnp.maximum(jnp.max(jnp.abs(value), axis=1, keepdims=True), 1e-30)
        whole_numbers = (value * (32767.0 / peak) + 12582912.0) - 12582912.0
        sendp[slot * n + 2 * g + d] = whole_numbers.astype(jnp.int32).astype(jnp.int16)
        line = jnp.sum(jnp.where(diagonal, peak, 0.0), axis=0, keepdims=True)
        row = 2 * (slot % half_slots) + d
        scales[slot // half_slots * half_n + g, row : row + 1, :] = line

    @pl.loop(0, half_n)
    def _(k):
        g = group(k)
        settle(xv.at[g], load_sem.at[1 + g])
        for c in range(3):
            part = jnp.dot(t_ref[...], xv[g, c], preferred_element_type=jnp.float32)
            for d in range(2):
                parts[2 * g + d, :, c * pw : (c + 1) * pw] = part[:, d * pw : (d + 1) * pw]

        @pl.when(k == 0)
        def _():
            pl.semaphore_wait(barrier, total - 1)

        for d in range(2):
            for slot in range(slots):
                if shared[slot]:
                    @pl.when(member(tm, shared[slot]) & is_theirs(slot, 2 * g + d))
                    def _(slot=slot, d=d):
                        encode(slot, g, d)

        for side in range(2):
            _, whole_group, all_mine = division(n, tm, side, 2 * g)

            @pl.when(edge_exists(side) & jnp.logical_not(whole_group & all_mine))
            def _(side=side):
                scale_copy(side, g).start()

        for d in range(2):
            for slot in range(slots):
                if shared[slot]:
                    @pl.when(member(tm, shared[slot]) & is_theirs(slot, 2 * g + d) & (parity == (0 if slot >= half_slots else 1)))
                    def _(slot=slot, d=d):
                        exchange(slot, 2 * g + d).start()

        for d in range(2):
            for slot in range(slots):
                if whole[slot]:
                    @pl.when(member(tm, whole[slot]) & (parity == d))
                    def _(slot=slot, d=d):
                        deliver(slot, 2 * g + d, parts[2 * g + d, slot * ROWS : (slot + 1) * ROWS, :])

        for d in range(2):
            for slot in range(slots):
                if shared[slot]:
                    @pl.when(member(tm, shared[slot]) & is_theirs(slot, 2 * g + d) & (parity == (1 if slot >= half_slots else 0)))
                    def _(slot=slot, d=d):
                        exchange(slot, 2 * g + d).start()

    def send_crossing():
        @pl.loop(0, half_n)
        def _(k):
            dest = 2 * group(k) + 1 - parity
            for slot in range(slots):
                if whole[slot]:
                    @pl.when(member(tm, whole[slot]))
                    def _(slot=slot):
                        deliver(slot, dest, parts[dest, slot * ROWS : (slot + 1) * ROWS, :])

    counts = [sum(tm_at in devs for devs in shared) for tm_at in range(n)]

    @pl.loop(0, 2)
    def _(turn):
        side = jnp.where(turn == 0, 1 - parity, parity)

        @pl.loop(0, half_n)
        def _(k):
            g = group(k)
            _, whole_group, all_mine = division(n, tm, side, 2 * g)

            @pl.when(edge_exists(side) & (jnp.logical_not(whole_group) | all_mine))
            def _():
                settle(oscales.at[side * half_n + g], srecv.at[side * half_n + g])
                settle_count(others, sharing(side) * jnp.where(whole_group, 2, 1), precv.at[side * half_n + g],
                             [count * twice for count in range(1, half_slots + 1) for twice in (1, 2)])
                for d in range(2):
                    dest = 2 * g + d
                    for index in range(half_slots):
                        slot = side * half_slots + index

                        @pl.when(is_shared(slot) & jnp.logical_not(is_theirs(slot, dest)))
                        def _(slot=slot, dest=dest, row=2 * index + d):
                            line = oscales[side * half_n + g, row : row + 1, :]
                            peak = jnp.sum(jnp.where(diagonal, line, 0.0), axis=1, keepdims=True)
                            other = others[slot * n + dest].astype(jnp.int32).astype(jnp.float32)
                            here = parts[dest, pl.ds(pl.multiple_of(slot * ROWS, ROWS), ROWS), :]
                            deliver(slot, dest, here + other * (peak * (1.0 / 32767.0)))


            @pl.when((turn == 0) & (k == half_n - 1))
            def _():
                send_crossing()

    alone = [sum(tm_at in devs for devs in whole) for tm_at in range(n)]
    for tm_at in range(n):
        @pl.when(tm == tm_at)
        def _(tm_at=tm_at):
            settle(recvb.at[pl.ds(0, NB - alone[tm_at] - counts[tm_at])], arecv.at[0])

    pitch = spec32.shape[1] // NB
    for block in range(NB):
        values = recvb[block]
        for c in range(3):
            spec32[c, block * pitch : block * pitch + ROWS, :] = values[:, c * 128 : (c + 1) * 128].astype(jnp.float32)

    def to_owner(f):
        return pltpu.make_async_remote_copy(
            src_ref=gpart.at[f], dst_ref=gath.at[lin], send_sem=gsend.at[0],
            recv_sem=grecv.at[0], device_id=where_is(owner(f)), device_id_type=MESH)

    upper = lax.broadcasted_iota(jnp.int32, (NB, NB), 1) >= lax.broadcasted_iota(jnp.int32, (NB, NB), 0)
    for f in range(NF):
        real, imag = [jnp.concatenate([
            spec32[c, pl.ds(2 * f + r, NB, stride=pitch), :].astype(jnp.bfloat16)
            for c in range(3)], axis=1) for r in range(2)]
        spec[f, :NB, :] = real
        spec[f, NB:, :] = imag
        lhs = jnp.concatenate([real, imag], axis=1)
        rhs = jnp.concatenate([lhs, jnp.concatenate([imag, -real], axis=1)], axis=0)
        gram = lax.dot_general(lhs, rhs, (((1,), (1,)), ((), ())), preferred_element_type=jnp.float32)
        packed = jnp.where(upper, gram[:, :NB], gram[:, NB:])
        gpart[f] = jnp.concatenate([packed[8 * q : 8 * q + 8] for q in range(NB // 8)], axis=1)
        if f % 4 == 3:
            for sent in range(f - 3, f + 1):
                @pl.when(lin != owner(sent))
                def _(sent=sent):
                    to_owner(sent).start()

    def coef_to(away):
        return pltpu.make_async_remote_copy(
            src_ref=msg, dst_ref=crecv.at[mine], send_sem=csend.at[0],
            recv_sem=crcv.at[0], device_id=displaced(away), device_id_type=MESH)

    @pl.when(owns)
    def _():
        gath[lin] = gpart[mine]

        settle(gath.at[pl.ds(0, total - 1)], grecv.at[0])
        packed = jnp.sum(gath[...], axis=0)
        square = jnp.concatenate([packed[:, q * NB : (q + 1) * NB] for q in range(NB // 8)], axis=0)
        flipped = jnp.transpose(square)
        ri = lax.broadcasted_iota(jnp.int32, (NB, NB), 0)
        ci = lax.broadcasted_iota(jnp.int32, (NB, NB), 1)
        gram_re = jnp.where(ci >= ri, square, flipped)
        gram_im = jnp.where(ci < ri, square, jnp.where(ci > ri, -flipped, 0.0))
        energy = jnp.sum(jnp.where(ri == ci, gram_re, 0.0), axis=(0, 1), keepdims=True) / (3.0 * NB * points)
        hermit = jnp.concatenate([
            jnp.concatenate([gram_re, -gram_im, gram_re, -gram_im], axis=1),
            jnp.concatenate([gram_im, gram_re, gram_im, gram_re], axis=1)], axis=0)
        frob = jnp.sqrt(0.5 * jnp.sum(hermit * hermit, axis=(0, 1), keepdims=True) + 1e-06)
        ri = lax.broadcasted_iota(jnp.int32, (2 * NB, 4 * NB), 0)
        ci = lax.broadcasted_iota(jnp.int32, (2 * NB, 4 * NB), 1)
        left = ci < 2 * NB
        identity = jnp.where(ri == (ci & (2 * NB - 1)), 1.0, 0.0).astype(jnp.float32)

        def pieces(a):
            high = a.astype(jnp.bfloat16)
            rest = a - high.astype(jnp.float32)
            mid = rest.astype(jnp.bfloat16)
            return high, mid, (rest - mid.astype(jnp.float32)).astype(jnp.bfloat16)

        def mul(a, b):
            ah, am, al = a
            bh, bm, bl = b
            lhs = jnp.concatenate([ah, am, jnp.where(left[: ah.shape[0]], ah, al)], axis=1)
            rhs = jnp.concatenate([bh, bm, bh, bm, bl, bh], axis=0)
            return jnp.dot(lhs, rhs, preferred_element_type=jnp.float32)

        iterate = hermit / frob
        inverse = identity
        for step in range(NSIT):
            it = pieces(iterate)
            if step:
                inv = pieces(inverse)
            factor = 1.5 * identity - 0.5 * (mul(inv, it) if step else iterate)
            fac = pieces(factor)
            if step < NSIT - 1:
                iterate = mul(it, fac)
                inverse = mul(fac, inv) if step else factor
            else:
                inverse = mul(tuple(piece[:NB] for piece in fac), inv)
        scaled = inverse * jnp.sqrt(6.0 * points / frob)
        high, mid, rest = [piece.astype(jnp.float32) for piece in pieces(energy)]
        top = ri[:NB]
        extra = jnp.where(top == 0, high, jnp.where(top == 1, mid, jnp.where(top == 2, rest, 0.0)))
        scaled = jnp.where((ci[:NB] & (2 * NB - 1)) == NB + top, extra, scaled)
        msg[...] = jnp.where(left[: NB // 2], scaled[: NB // 2], scaled[NB // 2 :]).astype(jnp.bfloat16)
        crecv[mine] = msg[...]

        for away in range(total - 1, 0, -1):
            coef_to(away).start()

    for tm_at in range(n):
        handed, groups = 0, 0
        for slot in range(slots):
            if tm_at in shared[slot]:
                handed += sum(division(n, tm_at, slot // half_slots, dest)[0] for dest in range(n))
        for side in range(2):
            if 0 < tm_at + side < n:
                for g in range(half_n):
                    _, whole_group, all_mine = division(n, tm_at, side, 2 * g)
                    groups += not (whole_group and all_mine)

        @pl.when(tm == tm_at)
        def _(tm_at=tm_at, handed=handed, groups=groups):
            settle(sendp.at[pl.ds(0, handed)], psend.at[0])
            own = n * (alone[tm_at] + counts[tm_at]) - handed
            settle(sendb.at[pl.ds(0, own - alone[tm_at] - counts[tm_at])], asend.at[0])
            settle(scales.at[pl.ds(0, groups)], ssend.at[0])

    sent = jnp.where(owns, NF - 1, NF)
    settle_count(gpart, sent, gsend.at[0], [NF - 1, NF])
    settle_count(crecv, sent, crcv.at[0], [NF - 1, NF])
    coefs_ref[...] = crecv[...]

    @pl.when(owns)
    def _():
        settle(gath.at[pl.ds(0, total - 1)], csend.at[0])


def finish_kernel(spec, crecv, modes_hbm, energy_hbm, stage, modes_ref, energy_ref, sem):
    pw = modes_ref.shape[1]

    lanes = lax.broadcasted_iota(jnp.int32, (NB, 2 * NB), 1)
    signs = jnp.where(lanes < NB, 1.0, -1.0).astype(jnp.bfloat16)
    hidden = lanes == NB + lax.broadcasted_iota(jnp.int32, (NB, 2 * NB), 0)
    wide_lane = lax.broadcasted_iota(jnp.int32, (1, NF), 1)
    energies = jnp.zeros((1, NF), jnp.float32)
    for f in range(NF):
        pairs = crecv[f]
        straight = jnp.concatenate([pairs[:, : 2 * NB], pairs[:, 2 * NB :]], axis=0)
        found = jnp.sum(jnp.where(hidden, straight.astype(jnp.float32), 0.0), axis=(0, 1), keepdims=True)
        energies = jnp.where(wide_lane == f, found, energies)
        straight = jnp.where(hidden, jnp.zeros_like(straight), straight)
        crossed = jnp.concatenate([straight[:, NB:], straight[:, :NB]], axis=1)
        stacked = jnp.concatenate([straight * signs, crossed], axis=0)
        out = jnp.dot(stacked, spec[f], preferred_element_type=jnp.float32)
        for c in range(3):
            for o in range(2):
                stage[f % 4, pl.ds(2 * c + o, NB, stride=6), :] = out[o * NB : (o + 1) * NB, c * pw : (c + 1) * pw]
        modes_ref[f * 6 * NB : (f + 1) * 6 * NB, :] = stage[f % 4].astype(jnp.bfloat16)
        part = pl.ds(f * 6 * NB, 6 * NB)
        pltpu.make_async_copy(modes_ref.at[part], modes_hbm.at[part], sem.at[0]).start()
    energy_ref[...] = energies
    last = pltpu.make_async_copy(energy_ref, energy_hbm, sem.at[1])
    last.start()
    pltpu.make_async_copy(modes_ref, modes_hbm, sem.at[0]).wait()
    last.wait()


def fused(n, nf_dev, chosen, snapshots, block_starts, freq_index):
    per, whole, shared, holders = chosen
    rows, count, wide = snapshots.shape
    total = n * nf_dev
    pw = wide // n
    slots = per + 4
    f32, bf16 = jnp.float32, jnp.bfloat16
    dma = pltpu.SemaphoreType.DMA
    vmem = pl.BlockSpec(memory_space=pltpu.VMEM)
    spec, coefs = pl.pallas_call(
        functools.partial(kernel, n, nf_dev, per, whole, shared, holders, float(wide * nf_dev)),
        out_shape=(jax.ShapeDtypeStruct((NF, 2 * NB, 3 * pw), bf16),
                   jax.ShapeDtypeStruct((NF, NB // 2, 4 * NB), bf16)),
        in_specs=[pl.BlockSpec(memory_space=pltpu.HBM)] * 2,
        out_specs=(vmem, vmem),
        scratch_shapes=[
            pltpu.SMEM((NB + NF,), jnp.int32),
            pltpu.VMEM((slots * ROWS, rows), bf16),
            pltpu.VMEM((n // 2, 3, rows, 2 * pw), bf16),
            pltpu.VMEM((n, slots * ROWS, 3 * pw), f32),
            pltpu.VMEM((slots * n, ROWS, 3 * pw), jnp.int16),
            pltpu.VMEM((slots * n, ROWS, 3 * pw), jnp.int16),
            pltpu.VMEM((n, slots, 128), f32),
            pltpu.VMEM((n, slots, 128), f32),
            pltpu.VMEM((slots * n, ROWS, 3 * pw), bf16),
            pltpu.VMEM((NB, ROWS, 3 * pw), bf16),
            pltpu.VMEM((3, NB * (ROWS + 8), pw), f32),
            pltpu.VMEM((NF, NB // 4, 4 * NB), f32),
            pltpu.VMEM((total, NB // 4, 4 * NB), f32),
            pltpu.VMEM((NB // 2, 4 * NB), bf16),
            pltpu.VMEM((NF, NB // 2, 4 * NB), bf16),
            dma((1 + n // 2,)), dma((1,)), dma((n,)), dma((1,)), dma((n,)),
            dma((1,)), dma((1,)), dma((1,)), dma((1,)), dma((1,)), dma((1,)),
        ],
        compiler_params=pltpu.CompilerParams(
            collective_id=0, has_side_effects=True, vmem_limit_bytes=54_000_000),
    )(jnp.transpose(snapshots, (1, 0, 2)), jnp.concatenate([block_starts, freq_index]))
    modes, energy = pl.pallas_call(
        finish_kernel,
        out_shape=(jax.ShapeDtypeStruct((NF * NB * 6, pw), bf16), jax.ShapeDtypeStruct((1, NF), f32)),
        in_specs=[vmem, vmem],
        out_specs=[pl.BlockSpec(memory_space=pltpu.HBM)] * 2,
        scratch_shapes=[
            pltpu.VMEM((4, 6 * NB, pw), f32), pltpu.VMEM((NF * NB * 6, pw), bf16),
            pltpu.VMEM((1, NF), f32), dma((2,)),
        ],
        compiler_params=pltpu.CompilerParams(vmem_limit_bytes=8_000_000),
    )(spec, coefs)
    modes = modes.reshape(NF, NB, 3, 2, pw).transpose(0, 1, 3, 2, 4)
    return modes, energy.reshape(NF)


def solution(mesh):
    n, nf_dev = mesh.shape["tm"], mesh.shape["freq"]

    def body(snapshots, block_starts, freq_index):
        rows, _, wide = snapshots.shape
        chosen = plan(n, rows, n * nf_dev, wide // n)
        if chosen is None:
            return local(snapshots, block_starts, freq_index)
        return fused(n, nf_dev, chosen, snapshots, block_starts, freq_index)

    return jax.shard_map(
        body,
        mesh=mesh,
        in_specs=(P("tm", None, "freq"), P(), P()),
        out_specs=(P(None, None, None, None, ("freq", "tm")), P()),
        check_vma=False,
    )
```

```python
import functools
import math

import jax
import jax.numpy as jnp
import numpy as np
from jax import lax
from jax.experimental import pallas as pl
from jax.experimental.pallas import tpu as pltpu
from jax.sharding import PartitionSpec as P

NB = 32
NFFT = 256
NF = 16
NSIT = 6


def for_sending(shard):
    return jax.tree.map(lambda a: a.astype(jnp.bfloat16) if a.dtype == jnp.float32 else a, shard)


def dft_rows(freq_index):
    times_idx = jnp.arange(NFFT, dtype=jnp.int32)
    phase_int = freq_index[:, None] * times_idx[None, :] % NFFT
    angles = 2.0 * math.pi / NFFT * phase_int.astype(jnp.float32)
    window = 0.5 - 0.5 * jnp.cos(2.0 * math.pi / NFFT * times_idx.astype(jnp.float32))
    scaling = 1.0 / jnp.sqrt(jnp.sum(window * window))
    cosine = window[None, :] * jnp.cos(angles) * scaling
    sine_rows = -window[None, :] * jnp.sin(angles) * scaling
    return jnp.stack([cosine, sine_rows], 1).reshape(2 * NF, NFFT).astype(jnp.bfloat16)


def block_rows(block_starts):
    return block_starts[:, None] + jnp.arange(NFFT, dtype=jnp.int32)[None, :]


def matmul_batch(left, right):
    return jnp.einsum("fij,fjk->fik", left, right, precision=lax.Precision.HIGHEST)


def whiten(summed, points):
    gram_re = summed[:, 0]
    gram_im = summed[:, 1]
    top_rows = jnp.concatenate([gram_re, -gram_im], 2)
    low_rows = jnp.concatenate([gram_im, gram_re], 2)
    hermit = jnp.concatenate([top_rows, low_rows], 1)
    frob = jnp.sqrt(jnp.sum(hermit * hermit, axis=(1, 2)) + 1e-06)
    identity = jnp.eye(2 * NB, dtype=jnp.float32)[None]
    iterate = hermit / frob[:, None, None]
    inverse = jnp.broadcast_to(identity, hermit.shape)
    for iteration in range(NSIT):
        factor = 1.5 * identity - 0.5 * matmul_batch(inverse, iterate)
        iterate = matmul_batch(iterate, factor)
        inverse = matmul_batch(factor, inverse)
    columns = inverse[:, :, :NB] * jnp.sqrt(6.0 * points / frob)[:, None, None]
    upper = columns[:, :NB]
    lower = columns[:, NB:]
    coefficients = jnp.stack([jnp.stack([upper, -lower], 1), jnp.stack([lower, upper], 1)], 1)
    energy = jnp.trace(gram_re, axis1=1, axis2=2) / (3.0 * NB * points)
    return (coefficients, energy)


def local(snapshots, block_starts, freq_index):
    dft_table = dft_rows(freq_index)
    offsets = block_rows(block_starts)
    series = lax.all_to_all(snapshots, "tm", split_axis=2, concat_axis=0, tiled=True)
    count = series.shape[1]
    width = series.shape[2]
    columns_all = series.reshape(series.shape[0], count * width)
    windows = jnp.take(columns_all, offsets, axis=0)
    spectra_part = jnp.einsum(
        "rt,btn->rbn", dft_table, windows, preferred_element_type=jnp.float32
    ).astype(jnp.bfloat16)
    spectra = spectra_part.reshape(2 * NF, NB, count, width)
    width = spectra.shape[3]
    points = float(width * lax.axis_size("tm") * lax.axis_size("freq"))
    flat_spec = spectra.reshape(NF, 2, NB, 3 * width)
    real_part = flat_spec[:, 0]
    imag_part = flat_spec[:, 1]
    gram_re = jnp.einsum("fbn,fcn->fbc", real_part, real_part, preferred_element_type=jnp.float32)
    gram_re = gram_re + jnp.einsum(
        "fbn,fcn->fbc", imag_part, imag_part, preferred_element_type=jnp.float32
    )
    cross_terms = jnp.einsum(
        "fbn,fcn->fbc", real_part, imag_part, preferred_element_type=jnp.float32
    )
    partial_gram = jnp.stack([gram_re, cross_terms - jnp.swapaxes(cross_terms, 1, 2)], 1)
    shared = lax.psum_scatter(partial_gram, "freq", scatter_dimension=0, tiled=True)
    shared = lax.psum(shared, "tm")
    coef_part, energy_part = whiten(shared, points)
    coefficients, energy = (
        lax.all_gather(for_sending(coef_part), "freq", axis=0, tiled=True).astype(coef_part.dtype),
        lax.all_gather(for_sending(energy_part), "freq", axis=0, tiled=True).astype(
            energy_part.dtype
        ),
    )
    coef_bf = jnp.transpose(coefficients.astype(jnp.bfloat16), (0, 4, 1, 2, 3))
    modes = jnp.einsum(
        "fjorb,frbn->fjon", coef_bf, flat_spec, preferred_element_type=jnp.float32
    ).astype(jnp.bfloat16)
    return (modes.reshape(NF, NB, 2, 3, width), energy)


MESH = pl.DeviceIdType.MESH
ROWS = 2 * NF
HOP = 128
JIT = 64


def plan(n, rows, total, width):
    if n % 4 or NB % n or total % (2 * NF) or width != 128 or rows % 16:
        return None
    per = NB // n
    if per < 4 or per % 2:
        return None
    slots = per + 4
    whole = [[] for _ in range(slots)]
    shared = [[] for _ in range(slots)]
    holders = []
    for block in range(NB):
        touched = [
            dev for dev in range(n)
            if HOP * block < rows * (dev + 1) and HOP * block + JIT + NFFT > rows * dev
        ]
        holders.append(touched)
        if len(touched) > 2:
            return None
        for dev in touched:
            slot = block - per * dev + 2
            if not 0 <= slot < slots:
                return None
            if len(touched) == 2:
                if (slot < slots // 2) != (dev == touched[1]):
                    return None
                shared[slot].append(dev)
            else:
                whole[slot].append(dev)
    return per, whole, shared, holders


def base_table(ints_ref):
    row = lax.broadcasted_iota(jnp.int32, (ROWS, NFFT), 0)
    times_idx = lax.broadcasted_iota(jnp.int32, (ROWS, NFFT), 1)
    freqs = jnp.zeros((ROWS, NFFT), jnp.int32)
    for f in range(NF):
        freqs = jnp.where((row >> 1) == f, ints_ref[NB + f], freqs)
    phase = (freqs * times_idx) & (NFFT - 1)
    angles = 2.0 * math.pi / NFFT * phase.astype(jnp.float32)
    window = 0.5 - 0.5 * jnp.cos(2.0 * math.pi / NFFT * times_idx.astype(jnp.float32))
    hann = 0.5 - 0.5 * np.cos(2.0 * math.pi / NFFT * np.arange(NFFT))
    scaling = np.float32(1.0 / np.sqrt(np.sum(hann * hann)))
    cosine = window * jnp.cos(angles) * scaling
    sine = -window * jnp.sin(angles) * scaling
    return jnp.where((row & 1) == 1, sine, cosine).astype(jnp.bfloat16)


def shifted(base, shift, rows):
    source = lax.broadcasted_iota(jnp.int32, (NFFT, rows), 0)
    target = lax.broadcasted_iota(jnp.int32, (NFFT, rows), 1)
    pick = jnp.where(source - target == shift, 1.0, 0.0).astype(jnp.bfloat16)
    return jnp.dot(base, pick, preferred_element_type=jnp.float32).astype(jnp.bfloat16)


def member(index, devs):
    if not devs:
        return None
    if devs == list(range(devs[0], devs[-1] + 1)):
        return (index >= devs[0]) & (index <= devs[-1])
    hit = index == devs[0]
    for dev in devs[1:]:
        hit = hit | (index == dev)
    return hit


def division(n, tm, side, dest):
    edge, half = tm + side, n // 2
    middle = edge == half
    left = dest < half
    all_mine = middle & (left == (tm < half))
    theirs = (middle & (all_mine ^ True)) | ((middle ^ True) & (dest % 2 != tm % 2))
    return theirs, middle, all_mine


def kernel(n, nf_dev, per, whole, shared, holders, points, x_hbm, ints_hbm,
           spec, coefs_ref, ints_ref, t_ref, xv, parts,
           sendp, others, relayb, scales, oscales, sendb, recvb, spec32, gpart, gath, msg, crecv,
           load_sem, psend, precv, rrecv, fsend, ssend, srecv, asend, arecv, gsend, grecv, csend, crcv):
    tm = lax.axis_index("tm")
    fr = lax.axis_index("freq")
    total = n * nf_dev
    lin = tm * nf_dev + fr
    step, lowest = total // (2 * NF), total // 4
    slots = per + 4
    half_slots = slots // 2
    mine = (lin - lowest) // step
    owns = (lin >= lowest) & (lin < lowest + NF * step) & ((lin - lowest) % step == 0)
    half_n = n // 2
    parity = tm % 2
    rows = xv.shape[2]
    pw = xv.shape[3] // 2

    def owner(f):
        return lowest + f * step

    def where_is(index):
        return {"tm": index // nf_dev, "freq": index % nf_dev}

    def displaced(away):
        row, col = tm + away // nf_dev, fr + away % nf_dev
        return {"tm": jnp.where(row >= n, row - n, row),
                "freq": jnp.where(col >= nf_dev, col - nf_dev, col)}

    def group(k):
        return jnp.where(tm < half_n, half_n - 1 - k, k)

    def load(g, c):
        return pltpu.make_async_copy(
            x_hbm.at[c, :, pl.ds(pl.multiple_of(g * 2 * pw, 2 * pw), 2 * pw)], xv.at[g, c],
            load_sem.at[1 + g])

    small = pltpu.make_async_copy(ints_hbm, ints_ref, load_sem.at[0])
    small.start()
    for k in range(half_n):
        for c in range(3):
            load(group(k), c).start()
    barrier = pltpu.get_barrier_semaphore()

    for away in range(total - 1, 0, -1):
        pl.semaphore_signal(barrier, inc=1, device_id=displaced(away), device_id_type=MESH)

    small.wait()
    base = base_table(ints_ref)
    for slot in range(slots):
        block = per * tm + slot - 2
        start = ints_ref[jnp.clip(block, 0, NB - 1)]
        inside = (block >= 0) & (block < NB)
        shift = jnp.where(inside, rows * tm - start, 4 * (rows + NFFT))
        t_ref[slot * ROWS : (slot + 1) * ROWS, :] = shifted(base, shift, rows)
    scales[...] = jnp.zeros_like(scales)

    def low(slot):
        return slot < half_slots

    def pick(flag, yes, no):
        return (yes if flag else no) if isinstance(flag, bool) else jnp.where(flag, yes, no)

    def partner(slot):
        return pick(low(slot), (tm + n - 1) % n, (tm + 1) % n)

    def across(slot):
        return pick(low(slot), slot + per, slot - per)

    def is_shared(slot):
        block = per * tm + slot - 2
        edge = rows * (tm + pick(low(slot), 0, 1))
        inside = (block >= 0) & (block < NB) & (edge > 0) & (edge < rows * n)
        return inside & (HOP * block < edge) & (HOP * block + JIT + NFFT > edge)

    def is_theirs(slot, dest):
        return division(n, tm, slot // half_slots, dest)[0]

    def exchange(slot, length, dest):
        return pltpu.make_async_remote_copy(
            src_ref=sendp.at[pl.ds(dest * slots + slot, length)],
            dst_ref=others.at[pl.ds(dest * slots + across(slot), length)],
            send_sem=psend.at[0], recv_sem=precv.at[across(slot) // half_slots * half_n + dest // 2],
            device_id={"tm": partner(slot), "freq": fr}, device_id_type=MESH)

    def scale_copy(side, g):
        return pltpu.make_async_remote_copy(
            src_ref=scales.at[side * half_n + g], dst_ref=oscales.at[(1 - side) * half_n + g],
            send_sem=ssend.at[0], recv_sem=srecv.at[(1 - side) * half_n + g],
            device_id={"tm": partner(side * half_slots), "freq": fr}, device_id_type=MESH)

    def scatter(slot, length, dest):
        block = per * tm + slot - 2
        return pltpu.make_async_remote_copy(
            src_ref=sendb.at[pl.ds(dest * slots + slot, length)], dst_ref=recvb.at[pl.ds(block, length)],
            send_sem=asend.at[0], recv_sem=arecv.at[0],
            device_id={"tm": dest, "freq": fr}, device_id_type=MESH)

    def settle(ref, sem):
        pltpu.make_async_copy(ref, ref, sem).wait()

    def settle_count(ref, count, sem, options):
        for option in sorted(set(options)):
            @pl.when(count == option)
            def _(option=option):
                settle(ref.at[pl.ds(0, option)], sem)

    def edge_exists(side):
        return pick(side == 0, tm > 0, tm < n - 1)

    def sharing(side):
        return sum(jnp.where(is_shared(side * half_slots + k), 1, 0) for k in range(half_slots))

    def put(slot, dest, value):
        value = value.astype(jnp.bfloat16)

        @pl.when(dest == tm)
        def _():
            recvb[per * tm + slot - 2] = value

        @pl.when(dest != tm)
        def _():
            sendb[dest * slots + slot] = value

    def first_shared(side):
        flags = [is_shared(side * half_slots + k) for k in range(half_slots)]
        first = half_slots - 1
        for k in range(half_slots - 2, -1, -1):
            first = jnp.where(flags[k], k, first)
        return side * half_slots + first

    def runs(table):
        found = {}
        for tm_at in range(n):
            slot = 0
            while slot < slots:
                length = 0
                while slot + length < slots and tm_at in table[slot + length]:
                    length += 1
                if length:
                    found.setdefault((slot, length), []).append(tm_at)
                slot += length + 1
        return found

    def hops(dest):
        return ((tm == 1) & (dest >= half_n)) | ((tm == n - 2) & (dest < half_n))

    def relay_rank(dest):
        return dest // 2 % (half_n // 2)

    def to_relay(first, length, place, dest):
        return pltpu.make_async_remote_copy(
            src_ref=sendb.at[pl.ds(dest * slots + first, length)], dst_ref=relayb.at[pl.ds(place, length)],
            send_sem=asend.at[0], recv_sem=rrecv.at[0],
            device_id={"tm": tm + 1 - 2 * parity, "freq": fr}, device_id_type=MESH)

    def relay_runs(source):
        placed, place = [], 0
        for (first, length), devs in runs(whole).items():
            if source in devs:
                placed.append((first, length, place))
                place += length * (half_n // 2)
        return placed, place

    def send_to_relay(dest):
        for source in (1, n - 2):
            @pl.when((tm == source) & hops(dest))
            def _(source=source):
                for first, length, place in relay_runs(source)[0]:
                    for slot in range(first, first + length):
                        sendb[dest * slots + slot] = parts[dest, slot * ROWS : (slot + 1) * ROWS, :].astype(jnp.bfloat16)
                    to_relay(first, length, place + length * relay_rank(dest), dest).start()

    def relay():
        for me, source in ((0, 1), (n - 1, n - 2)):
            @pl.when(tm == me)
            def _(source=source):
                placed, amount = relay_runs(source)
                settle(relayb.at[pl.ds(0, amount)], rrecv.at[0])
                for first, length, place in placed:
                    for rank in range(half_n // 2):
                        dest = 2 * rank + (half_n if source == 1 else 0) + 1 - source % 2
                        spot = place + length * rank
                        pltpu.make_async_remote_copy(
                            src_ref=relayb.at[pl.ds(spot, length)],
                            dst_ref=recvb.at[pl.ds(per * source + first - 2, length)],
                            send_sem=fsend.at[0], recv_sem=arecv.at[0],
                            device_id={"tm": dest, "freq": fr}, device_id_type=MESH).start()

    def send_whole(dest, chosen):
        for (first, length), devs in runs(whole).items():
            @pl.when(member(tm, devs) & chosen)
            def _(first=first, length=length):
                for slot in range(first, first + length):
                    put(slot, dest, parts[dest, slot * ROWS : (slot + 1) * ROWS, :])

                @pl.when(dest != tm)
                def _():
                    scatter(first, length, dest).start()

    diagonal = (lax.broadcasted_iota(jnp.int32, (ROWS, 128), 0)
                == lax.broadcasted_iota(jnp.int32, (ROWS, 128), 1))

    def encode(slot, g, d):
        value = parts[2 * g + d, slot * ROWS : (slot + 1) * ROWS, :]
        peak = jnp.maximum(jnp.max(jnp.abs(value), axis=1, keepdims=True), 1e-30)
        whole_numbers = (value * (32767.0 / peak) + 12582912.0) - 12582912.0
        sendp[(2 * g + d) * slots + slot] = whole_numbers.astype(jnp.int32).astype(jnp.int16)
        line = jnp.sum(jnp.where(diagonal, peak, 0.0), axis=0, keepdims=True)
        row = 2 * (slot % half_slots) + d
        scales[slot // half_slots * half_n + g, row : row + 1, :] = line

    lengths = sorted({sum(tm_at in devs for devs in shared[side * half_slots : (side + 1) * half_slots])
                      for tm_at in range(n) for side in range(2)} - {0})

    @pl.loop(0, half_n)
    def _(k):
        g = group(k)
        settle(xv.at[g], load_sem.at[1 + g])
        for c in range(3):
            part = jnp.dot(t_ref[...], xv[g, c], preferred_element_type=jnp.float32)
            for d in range(2):
                parts[2 * g + d, :, c * pw : (c + 1) * pw] = part[:, d * pw : (d + 1) * pw]

        @pl.when(k == 0)
        def _():
            pl.semaphore_wait(barrier, total - 1)

        for d in range(2):
            for slot in range(slots):
                if shared[slot]:
                    @pl.when(member(tm, shared[slot]) & is_theirs(slot, 2 * g + d))
                    def _(slot=slot, d=d):
                        encode(slot, g, d)

        for side in range(2):
            _, whole_group, all_mine = division(n, tm, side, 2 * g)

            @pl.when(edge_exists(side) & jnp.logical_not(whole_group & all_mine))
            def _(side=side):
                scale_copy(side, g).start()

        def send_codes(want):
            for side in range(2):
                for d in range(2):
                    theirs = division(n, tm, side, 2 * g + d)[0]
                    for length in lengths:
                        @pl.when(edge_exists(side) & theirs & (parity == (want ^ side)) & (sharing(side) == length))
                        def _(side=side, d=d, length=length):
                            exchange(first_shared(side), length, 2 * g + d).start()

        send_codes(1)
        send_to_relay(2 * g + 1 - parity)
        for d in range(2):
            send_whole(2 * g + d, parity == d)
        send_codes(0)

    def send_crossing():
        @pl.loop(0, half_n)
        def _(k):
            dest = 2 * group(k) + 1 - parity
            send_whole(dest, jnp.logical_not(hops(dest)))

    counts = [sum(tm_at in devs for devs in shared) for tm_at in range(n)]

    @pl.loop(0, 2)
    def _(turn):
        side = jnp.where(turn == 0, 1 - parity, parity)

        @pl.loop(0, half_n)
        def _(k):
            g = group(k)
            _, whole_group, all_mine = division(n, tm, side, 2 * g)

            @pl.when(edge_exists(side) & (jnp.logical_not(whole_group) | all_mine))
            def _():
                settle(oscales.at[side * half_n + g], srecv.at[side * half_n + g])
                settle_count(others, sharing(side) * jnp.where(whole_group, 2, 1), precv.at[side * half_n + g],
                             [count * twice for count in range(1, half_slots + 1) for twice in (1, 2)])
                for d in range(2):
                    dest = 2 * g + d
                    for index in range(half_slots):
                        slot = side * half_slots + index

                        @pl.when(is_shared(slot) & jnp.logical_not(is_theirs(slot, dest)))
                        def _(slot=slot, dest=dest, row=2 * index + d):
                            line = oscales[side * half_n + g, row : row + 1, :]
                            peak = jnp.sum(jnp.where(diagonal, line, 0.0), axis=1, keepdims=True)
                            other = others[dest * slots + slot].astype(jnp.int32).astype(jnp.float32)
                            here = parts[dest, pl.ds(pl.multiple_of(slot * ROWS, ROWS), ROWS), :]
                            put(slot, dest, here + other * (peak * (1.0 / 32767.0)))

                    mine_here = jnp.logical_not(division(n, tm, side, dest)[0]) & (dest != tm)
                    for length in lengths:
                        @pl.when(mine_here & (sharing(side) == length))
                        def _(length=length, dest=dest):
                            scatter(first_shared(side), length, dest).start()


            @pl.when((turn == 0) & (k == 0))
            def _():
                relay()

            @pl.when((turn == 0) & (k == 0))
            def _():
                send_crossing()

    alone = [sum(tm_at in devs for devs in whole) for tm_at in range(n)]
    pitch = spec32.shape[1] // NB
    missing = [NB - alone[tm_at] - counts[tm_at] for tm_at in range(n)]
    settle_count(recvb, sum(jnp.where(tm == tm_at, missing[tm_at], 0) for tm_at in range(n)), arecv.at[0], missing)
    for block in range(NB):
        values = recvb[block]
        for c in range(3):
            spec32[c, block * pitch : block * pitch + ROWS, :] = values[:, c * 128 : (c + 1) * 128].astype(jnp.float32)
    for f in range(NF):
        for r in range(2):
            spec[f, r * NB : (r + 1) * NB, :] = jnp.concatenate([
                spec32[c, pl.ds(2 * f + r, NB, stride=pitch), :].astype(jnp.bfloat16)
                for c in range(3)], axis=1)

    def to_owner(k):
        first, last = owner(NF - 1 - k), owner(k)
        near_start = tm < half_n
        f = jnp.where(near_start, NF - 1 - k, k)
        place = {"tm": jnp.where(near_start, first // nf_dev, last // nf_dev),
                 "freq": jnp.where(near_start, first % nf_dev, last % nf_dev)}
        return f, pltpu.make_async_remote_copy(
            src_ref=gpart.at[f], dst_ref=gath.at[lin], send_sem=gsend.at[0],
            recv_sem=grecv.at[0], device_id=place, device_id_type=MESH)

    upper = lax.broadcasted_iota(jnp.int32, (NB, NB), 1) >= lax.broadcasted_iota(jnp.int32, (NB, NB), 0)
    for f in range(NF):
        real, imag = spec[f, :NB, :], spec[f, NB:, :]
        lhs = jnp.concatenate([real, imag], axis=1)
        rhs = jnp.concatenate([lhs, jnp.concatenate([imag, -real], axis=1)], axis=0)
        gram = lax.dot_general(lhs, rhs, (((1,), (1,)), ((), ())), preferred_element_type=jnp.float32)
        packed = jnp.where(upper, gram[:, :NB], gram[:, NB:])
        gpart[f] = jnp.concatenate([packed[8 * q : 8 * q + 8] for q in range(NB // 8)], axis=1)
        if f % 16 == 15:
            for sent in range(f - 15, f + 1):
                target, copy = to_owner(sent)

                @pl.when(lin != owner(target))
                def _(copy=copy):
                    copy.start()

    def coef_to(away):
        return pltpu.make_async_remote_copy(
            src_ref=msg, dst_ref=crecv.at[mine], send_sem=csend.at[0],
            recv_sem=crcv.at[0], device_id=displaced(away), device_id_type=MESH)

    @pl.when(owns)
    def _():
        gath[lin] = gpart[mine]

        settle(gath.at[pl.ds(0, total - 1)], grecv.at[0])
        packed = jnp.sum(gath[...], axis=0)
        square = jnp.concatenate([packed[:, q * NB : (q + 1) * NB] for q in range(NB // 8)], axis=0)
        flipped = jnp.transpose(square)
        ri = lax.broadcasted_iota(jnp.int32, (NB, NB), 0)
        ci = lax.broadcasted_iota(jnp.int32, (NB, NB), 1)
        gram_re = jnp.where(ci >= ri, square, flipped)
        gram_im = jnp.where(ci < ri, square, jnp.where(ci > ri, -flipped, 0.0))
        energy = jnp.sum(jnp.where(ri == ci, gram_re, 0.0), axis=(0, 1), keepdims=True) / (3.0 * NB * points)
        hermit = jnp.concatenate([
            jnp.concatenate([gram_re, -gram_im, gram_re, -gram_im], axis=1),
            jnp.concatenate([gram_im, gram_re, gram_im, gram_re], axis=1)], axis=0)
        frob = jnp.sqrt(0.5 * jnp.sum(hermit * hermit, axis=(0, 1), keepdims=True) + 1e-06)
        ri = lax.broadcasted_iota(jnp.int32, (2 * NB, 4 * NB), 0)
        ci = lax.broadcasted_iota(jnp.int32, (2 * NB, 4 * NB), 1)
        left = ci < 2 * NB
        identity = jnp.where(ri == (ci & (2 * NB - 1)), 1.0, 0.0).astype(jnp.float32)

        def pieces(a):
            high = a.astype(jnp.bfloat16)
            rest = a - high.astype(jnp.float32)
            mid = rest.astype(jnp.bfloat16)
            return high, mid, (rest - mid.astype(jnp.float32)).astype(jnp.bfloat16)

        def mul(a, b):
            ah, am, al = a
            bh, bm, bl = b
            lhs = jnp.concatenate([ah, am, jnp.where(left[: ah.shape[0]], ah, al)], axis=1)
            rhs = jnp.concatenate([bh, bm, bh, bm, bl, bh], axis=0)
            return jnp.dot(lhs, rhs, preferred_element_type=jnp.float32)

        iterate = hermit / frob
        inverse = identity
        for step in range(NSIT):
            it = pieces(iterate)
            if step:
                inv = pieces(inverse)
            factor = 1.5 * identity - 0.5 * (mul(inv, it) if step else iterate)
            fac = pieces(factor)
            if step < NSIT - 1:
                iterate = mul(it, fac)
                inverse = mul(fac, inv) if step else factor
            else:
                inverse = mul(tuple(piece[:NB] for piece in fac), inv)
        scaled = inverse * jnp.sqrt(6.0 * points / frob)
        high, mid, rest = [piece.astype(jnp.float32) for piece in pieces(energy)]
        top = ri[:NB]
        extra = jnp.where(top == 0, high, jnp.where(top == 1, mid, jnp.where(top == 2, rest, 0.0)))
        scaled = jnp.where((ci[:NB] & (2 * NB - 1)) == NB + top, extra, scaled)
        msg[...] = jnp.where(left[: NB // 2], scaled[: NB // 2], scaled[NB // 2 :]).astype(jnp.bfloat16)
        crecv[mine] = msg[...]

        for away in range(total - 1, 0, -1):
            coef_to(away).start()

    for tm_at in range(n):
        handed, groups = 0, 0
        for slot in range(slots):
            if tm_at in shared[slot]:
                handed += sum(division(n, tm_at, slot // half_slots, dest)[0] for dest in range(n))
        for side in range(2):
            if 0 < tm_at + side < n:
                for g in range(half_n):
                    _, whole_group, all_mine = division(n, tm_at, side, 2 * g)
                    groups += not (whole_group and all_mine)

        @pl.when(tm == tm_at)
        def _(tm_at=tm_at, handed=handed, groups=groups):
            settle(sendp.at[pl.ds(0, handed)], psend.at[0])
            own = n * (alone[tm_at] + counts[tm_at]) - handed
            settle(sendb.at[pl.ds(0, own - alone[tm_at] - counts[tm_at])], asend.at[0])
            settle(scales.at[pl.ds(0, groups)], ssend.at[0])
            if tm_at in (0, n - 1):
                settle(relayb.at[pl.ds(0, relay_runs(1 if tm_at == 0 else n - 2)[1])], fsend.at[0])

    sent = jnp.where(owns, NF - 1, NF)
    settle_count(gpart, sent, gsend.at[0], [NF - 1, NF])
    settle_count(crecv, sent, crcv.at[0], [NF - 1, NF])
    coefs_ref[...] = crecv[...]

    @pl.when(owns)
    def _():
        settle(gath.at[pl.ds(0, total - 1)], csend.at[0])


def finish_kernel(spec, crecv, modes_hbm, energy_hbm, stage, modes_ref, energy_ref, sem):
    pw = modes_ref.shape[1]

    lanes = lax.broadcasted_iota(jnp.int32, (NB, 2 * NB), 1)
    signs = jnp.where(lanes < NB, 1.0, -1.0).astype(jnp.bfloat16)
    hidden = lanes == NB + lax.broadcasted_iota(jnp.int32, (NB, 2 * NB), 0)
    wide_lane = lax.broadcasted_iota(jnp.int32, (1, NF), 1)
    energies = jnp.zeros((1, NF), jnp.float32)
    for f in range(NF):
        pairs = crecv[f]
        straight = jnp.concatenate([pairs[:, : 2 * NB], pairs[:, 2 * NB :]], axis=0)
        found = jnp.sum(jnp.where(hidden, straight.astype(jnp.float32), 0.0), axis=(0, 1), keepdims=True)
        energies = jnp.where(wide_lane == f, found, energies)
        straight = jnp.where(hidden, jnp.zeros_like(straight), straight)
        crossed = jnp.concatenate([straight[:, NB:], straight[:, :NB]], axis=1)
        stacked = jnp.concatenate([straight * signs, crossed], axis=0)
        out = jnp.dot(stacked, spec[f], preferred_element_type=jnp.float32)
        for c in range(3):
            for o in range(2):
                stage[f % 4, pl.ds(2 * c + o, NB, stride=6), :] = out[o * NB : (o + 1) * NB, c * pw : (c + 1) * pw]
        modes_ref[f * 6 * NB : (f + 1) * 6 * NB, :] = stage[f % 4].astype(jnp.bfloat16)
        part = pl.ds(f * 6 * NB, 6 * NB)
        pltpu.make_async_copy(modes_ref.at[part], modes_hbm.at[part], sem.at[0]).start()
    energy_ref[...] = energies
    last = pltpu.make_async_copy(energy_ref, energy_hbm, sem.at[1])
    last.start()
    pltpu.make_async_copy(modes_ref, modes_hbm, sem.at[0]).wait()
    last.wait()


def fused(n, nf_dev, chosen, snapshots, block_starts, freq_index):
    per, whole, shared, holders = chosen
    rows, count, wide = snapshots.shape
    total = n * nf_dev
    pw = wide // n
    slots = per + 4
    f32, bf16 = jnp.float32, jnp.bfloat16
    dma = pltpu.SemaphoreType.DMA
    vmem = pl.BlockSpec(memory_space=pltpu.VMEM)
    spec, coefs = pl.pallas_call(
        functools.partial(kernel, n, nf_dev, per, whole, shared, holders, float(wide * nf_dev)),
        out_shape=(jax.ShapeDtypeStruct((NF, 2 * NB, 3 * pw), bf16),
                   jax.ShapeDtypeStruct((NF, NB // 2, 4 * NB), bf16)),
        in_specs=[pl.BlockSpec(memory_space=pltpu.HBM)] * 2,
        out_specs=(vmem, vmem),
        scratch_shapes=[
            pltpu.SMEM((NB + NF,), jnp.int32),
            pltpu.VMEM((slots * ROWS, rows), bf16),
            pltpu.VMEM((n // 2, 3, rows, 2 * pw), bf16),
            pltpu.VMEM((n, slots * ROWS, 3 * pw), f32),
            pltpu.VMEM((slots * n, ROWS, 3 * pw), jnp.int16),
            pltpu.VMEM((slots * n, ROWS, 3 * pw), jnp.int16),
            pltpu.VMEM((slots * n // 2, ROWS, 3 * pw), bf16),
            pltpu.VMEM((n, slots, 128), f32),
            pltpu.VMEM((n, slots, 128), f32),
            pltpu.VMEM((slots * n, ROWS, 3 * pw), bf16),
            pltpu.VMEM((NB, ROWS, 3 * pw), bf16),
            pltpu.VMEM((3, NB * (ROWS + 8), pw), f32),
            pltpu.VMEM((NF, NB // 4, 4 * NB), f32),
            pltpu.VMEM((total, NB // 4, 4 * NB), f32),
            pltpu.VMEM((NB // 2, 4 * NB), bf16),
            pltpu.VMEM((NF, NB // 2, 4 * NB), bf16),
            dma((1 + n // 2,)), dma((1,)), dma((n,)), dma((1,)), dma((1,)), dma((1,)), dma((n,)),
            dma((1,)), dma((1,)), dma((1,)), dma((1,)), dma((1,)), dma((1,)),
        ],
        compiler_params=pltpu.CompilerParams(
            collective_id=0, has_side_effects=True, vmem_limit_bytes=54_000_000),
    )(jnp.transpose(snapshots, (1, 0, 2)), jnp.concatenate([block_starts, freq_index]))
    modes, energy = pl.pallas_call(
        finish_kernel,
        out_shape=(jax.ShapeDtypeStruct((NF * NB * 6, pw), bf16), jax.ShapeDtypeStruct((1, NF), f32)),
        in_specs=[vmem, vmem],
        out_specs=[pl.BlockSpec(memory_space=pltpu.HBM)] * 2,
        scratch_shapes=[
            pltpu.VMEM((4, 6 * NB, pw), f32), pltpu.VMEM((NF * NB * 6, pw), bf16),
            pltpu.VMEM((1, NF), f32), dma((2,)),
        ],
        compiler_params=pltpu.CompilerParams(vmem_limit_bytes=8_000_000),
    )(spec, coefs)
    modes = modes.reshape(NF, NB, 3, 2, pw).transpose(0, 1, 3, 2, 4)
    return modes, energy.reshape(NF)


def solution(mesh):
    n, nf_dev = mesh.shape["tm"], mesh.shape["freq"]

    def body(snapshots, block_starts, freq_index):
        rows, _, wide = snapshots.shape
        chosen = plan(n, rows, n * nf_dev, wide // n)
        if chosen is None:
            return local(snapshots, block_starts, freq_index)
        return fused(n, nf_dev, chosen, snapshots, block_starts, freq_index)

    return jax.shard_map(
        body,
        mesh=mesh,
        in_specs=(P("tm", None, "freq"), P(), P()),
        out_specs=(P(None, None, None, None, ("freq", "tm")), P()),
        check_vma=False,
    )
```

```python
import functools
import math

import jax
import jax.numpy as jnp
import numpy as np
from jax import lax
from jax.experimental import pallas as pl
from jax.experimental.pallas import tpu as pltpu
from jax.sharding import PartitionSpec as P

NB = 32
NFFT = 256
NF = 16
NSIT = 6


def for_sending(shard):
    return jax.tree.map(lambda a: a.astype(jnp.bfloat16) if a.dtype == jnp.float32 else a, shard)


def dft_rows(freq_index):
    times_idx = jnp.arange(NFFT, dtype=jnp.int32)
    phase_int = freq_index[:, None] * times_idx[None, :] % NFFT
    angles = 2.0 * math.pi / NFFT * phase_int.astype(jnp.float32)
    window = 0.5 - 0.5 * jnp.cos(2.0 * math.pi / NFFT * times_idx.astype(jnp.float32))
    scaling = 1.0 / jnp.sqrt(jnp.sum(window * window))
    cosine = window[None, :] * jnp.cos(angles) * scaling
    sine_rows = -window[None, :] * jnp.sin(angles) * scaling
    return jnp.stack([cosine, sine_rows], 1).reshape(2 * NF, NFFT).astype(jnp.bfloat16)


def block_rows(block_starts):
    return block_starts[:, None] + jnp.arange(NFFT, dtype=jnp.int32)[None, :]


def matmul_batch(left, right):
    return jnp.einsum("fij,fjk->fik", left, right, precision=lax.Precision.HIGHEST)


def whiten(summed, points):
    gram_re = summed[:, 0]
    gram_im = summed[:, 1]
    top_rows = jnp.concatenate([gram_re, -gram_im], 2)
    low_rows = jnp.concatenate([gram_im, gram_re], 2)
    hermit = jnp.concatenate([top_rows, low_rows], 1)
    frob = jnp.sqrt(jnp.sum(hermit * hermit, axis=(1, 2)) + 1e-06)
    identity = jnp.eye(2 * NB, dtype=jnp.float32)[None]
    iterate = hermit / frob[:, None, None]
    inverse = jnp.broadcast_to(identity, hermit.shape)
    for iteration in range(NSIT):
        factor = 1.5 * identity - 0.5 * matmul_batch(inverse, iterate)
        iterate = matmul_batch(iterate, factor)
        inverse = matmul_batch(factor, inverse)
    columns = inverse[:, :, :NB] * jnp.sqrt(6.0 * points / frob)[:, None, None]
    upper = columns[:, :NB]
    lower = columns[:, NB:]
    coefficients = jnp.stack([jnp.stack([upper, -lower], 1), jnp.stack([lower, upper], 1)], 1)
    energy = jnp.trace(gram_re, axis1=1, axis2=2) / (3.0 * NB * points)
    return (coefficients, energy)


def local(snapshots, block_starts, freq_index):
    dft_table = dft_rows(freq_index)
    offsets = block_rows(block_starts)
    series = lax.all_to_all(snapshots, "tm", split_axis=2, concat_axis=0, tiled=True)
    count = series.shape[1]
    width = series.shape[2]
    columns_all = series.reshape(series.shape[0], count * width)
    windows = jnp.take(columns_all, offsets, axis=0)
    spectra_part = jnp.einsum(
        "rt,btn->rbn", dft_table, windows, preferred_element_type=jnp.float32
    ).astype(jnp.bfloat16)
    spectra = spectra_part.reshape(2 * NF, NB, count, width)
    width = spectra.shape[3]
    points = float(width * lax.axis_size("tm") * lax.axis_size("freq"))
    flat_spec = spectra.reshape(NF, 2, NB, 3 * width)
    real_part = flat_spec[:, 0]
    imag_part = flat_spec[:, 1]
    gram_re = jnp.einsum("fbn,fcn->fbc", real_part, real_part, preferred_element_type=jnp.float32)
    gram_re = gram_re + jnp.einsum(
        "fbn,fcn->fbc", imag_part, imag_part, preferred_element_type=jnp.float32
    )
    cross_terms = jnp.einsum(
        "fbn,fcn->fbc", real_part, imag_part, preferred_element_type=jnp.float32
    )
    partial_gram = jnp.stack([gram_re, cross_terms - jnp.swapaxes(cross_terms, 1, 2)], 1)
    shared = lax.psum_scatter(partial_gram, "freq", scatter_dimension=0, tiled=True)
    shared = lax.psum(shared, "tm")
    coef_part, energy_part = whiten(shared, points)
    coefficients, energy = (
        lax.all_gather(for_sending(coef_part), "freq", axis=0, tiled=True).astype(coef_part.dtype),
        lax.all_gather(for_sending(energy_part), "freq", axis=0, tiled=True).astype(
            energy_part.dtype
        ),
    )
    coef_bf = jnp.transpose(coefficients.astype(jnp.bfloat16), (0, 4, 1, 2, 3))
    modes = jnp.einsum(
        "fjorb,frbn->fjon", coef_bf, flat_spec, preferred_element_type=jnp.float32
    ).astype(jnp.bfloat16)
    return (modes.reshape(NF, NB, 2, 3, width), energy)


MESH = pl.DeviceIdType.MESH
ROWS = 2 * NF
HOP = 128
JIT = 64


def plan(n, rows, total, width):
    if n % 4 or NB % n or total % (2 * NF) or width != 128 or rows % 16:
        return None
    per = NB // n
    if per < 4 or per % 2:
        return None
    slots = per + 4
    whole = [[] for _ in range(slots)]
    shared = [[] for _ in range(slots)]
    holders = []
    for block in range(NB):
        touched = [
            dev for dev in range(n)
            if HOP * block < rows * (dev + 1) and HOP * block + JIT + NFFT > rows * dev
        ]
        holders.append(touched)
        if len(touched) > 2:
            return None
        for dev in touched:
            slot = block - per * dev + 2
            if not 0 <= slot < slots:
                return None
            if len(touched) == 2:
                if (slot < slots // 2) != (dev == touched[1]):
                    return None
                shared[slot].append(dev)
            else:
                whole[slot].append(dev)
    return per, whole, shared, holders


def base_table(ints_ref):
    row = lax.broadcasted_iota(jnp.int32, (ROWS, NFFT), 0)
    times_idx = lax.broadcasted_iota(jnp.int32, (ROWS, NFFT), 1)
    freqs = jnp.zeros((ROWS, NFFT), jnp.int32)
    for f in range(NF):
        freqs = jnp.where((row >> 1) == f, ints_ref[NB + f], freqs)
    phase = (freqs * times_idx) & (NFFT - 1)
    angles = 2.0 * math.pi / NFFT * phase.astype(jnp.float32)
    window = 0.5 - 0.5 * jnp.cos(2.0 * math.pi / NFFT * times_idx.astype(jnp.float32))
    hann = 0.5 - 0.5 * np.cos(2.0 * math.pi / NFFT * np.arange(NFFT))
    scaling = np.float32(1.0 / np.sqrt(np.sum(hann * hann)))
    cosine = window * jnp.cos(angles) * scaling
    sine = -window * jnp.sin(angles) * scaling
    return jnp.where((row & 1) == 1, sine, cosine).astype(jnp.bfloat16)


def shifted(base, shift, rows):
    source = lax.broadcasted_iota(jnp.int32, (NFFT, rows), 0)
    target = lax.broadcasted_iota(jnp.int32, (NFFT, rows), 1)
    pick = jnp.where(source - target == shift, 1.0, 0.0).astype(jnp.bfloat16)
    return jnp.dot(base, pick, preferred_element_type=jnp.float32).astype(jnp.bfloat16)


def member(index, devs):
    if not devs:
        return None
    if devs == list(range(devs[0], devs[-1] + 1)):
        return (index >= devs[0]) & (index <= devs[-1])
    hit = index == devs[0]
    for dev in devs[1:]:
        hit = hit | (index == dev)
    return hit


def division(n, tm, side, dest):
    edge, half = tm + side, n // 2
    middle = edge == half
    left = dest < half
    all_mine = middle & (left == (tm < half))
    theirs = (middle & (all_mine ^ True)) | ((middle ^ True) & (dest % 2 != tm % 2))
    return theirs, middle, all_mine


def kernel(n, nf_dev, per, whole, shared, holders, points, x_hbm, ints_hbm,
           spec, coefs_ref, ints_ref, t_ref, xv, parts,
           sendp, others, relayb, scales, oscales, sendb, recvb, spec32, gpart, gath, msg, crecv,
           load_sem, psend, precv, rrecv, fsend, ssend, srecv, asend, arecv, gsend, grecv, csend, crcv):
    tm = lax.axis_index("tm")
    fr = lax.axis_index("freq")
    total = n * nf_dev
    lin = tm * nf_dev + fr
    step, lowest = total // (2 * NF), total // 4
    slots = per + 4
    half_slots = slots // 2
    mine = (lin - lowest) // step
    owns = (lin >= lowest) & (lin < lowest + NF * step) & ((lin - lowest) % step == 0)
    half_n = n // 2
    parity = tm % 2
    rows = xv.shape[2]
    pw = xv.shape[3] // 2

    def owner(f):
        return lowest + f * step

    def where_is(index):
        return {"tm": index // nf_dev, "freq": index % nf_dev}

    def displaced(away):
        row, col = tm + away // nf_dev, fr + away % nf_dev
        return {"tm": jnp.where(row >= n, row - n, row),
                "freq": jnp.where(col >= nf_dev, col - nf_dev, col)}

    def group(k):
        return jnp.where(tm < half_n, half_n - 1 - k, k)

    def load(g, c):
        return pltpu.make_async_copy(
            x_hbm.at[c, :, pl.ds(pl.multiple_of(g * 2 * pw, 2 * pw), 2 * pw)], xv.at[g, c],
            load_sem.at[1 + g])

    small = pltpu.make_async_copy(ints_hbm, ints_ref, load_sem.at[0])
    small.start()
    for k in range(half_n):
        for c in range(3):
            load(group(k), c).start()
    barrier = pltpu.get_barrier_semaphore()

    for away in range(total - 1, 0, -1):
        pl.semaphore_signal(barrier, inc=1, device_id=displaced(away), device_id_type=MESH)

    small.wait()
    base = base_table(ints_ref)
    for slot in range(slots):
        block = per * tm + slot - 2
        start = ints_ref[jnp.clip(block, 0, NB - 1)]
        inside = (block >= 0) & (block < NB)
        shift = jnp.where(inside, rows * tm - start, 4 * (rows + NFFT))
        t_ref[slot * ROWS : (slot + 1) * ROWS, :] = shifted(base, shift, rows)
    scales[...] = jnp.zeros_like(scales)

    def low(slot):
        return slot < half_slots

    def pick(flag, yes, no):
        return (yes if flag else no) if isinstance(flag, bool) else jnp.where(flag, yes, no)

    def partner(slot):
        return pick(low(slot), (tm + n - 1) % n, (tm + 1) % n)

    def across(slot):
        return pick(low(slot), slot + per, slot - per)

    def is_shared(slot):
        block = per * tm + slot - 2
        edge = rows * (tm + pick(low(slot), 0, 1))
        inside = (block >= 0) & (block < NB) & (edge > 0) & (edge < rows * n)
        return inside & (HOP * block < edge) & (HOP * block + JIT + NFFT > edge)

    def is_theirs(slot, dest):
        return division(n, tm, slot // half_slots, dest)[0]

    def exchange(slot, length, dest):
        return pltpu.make_async_remote_copy(
            src_ref=sendp.at[pl.ds(dest * slots + slot, length)],
            dst_ref=others.at[pl.ds(dest * slots + across(slot), length)],
            send_sem=psend.at[0], recv_sem=precv.at[across(slot) // half_slots * half_n + dest // 2],
            device_id={"tm": partner(slot), "freq": fr}, device_id_type=MESH)

    def scale_copy(side, g):
        return pltpu.make_async_remote_copy(
            src_ref=scales.at[side * half_n + g], dst_ref=oscales.at[(1 - side) * half_n + g],
            send_sem=ssend.at[0], recv_sem=srecv.at[(1 - side) * half_n + g],
            device_id={"tm": partner(side * half_slots), "freq": fr}, device_id_type=MESH)

    def scatter(slot, length, dest):
        block = per * tm + slot - 2
        return pltpu.make_async_remote_copy(
            src_ref=sendb.at[pl.ds(dest * slots + slot, length)], dst_ref=recvb.at[pl.ds(block, length)],
            send_sem=asend.at[0], recv_sem=arecv.at[0],
            device_id={"tm": dest, "freq": fr}, device_id_type=MESH)

    def settle(ref, sem):
        pltpu.make_async_copy(ref, ref, sem).wait()

    def settle_count(ref, count, sem, options):
        for option in sorted(set(options)):
            @pl.when(count == option)
            def _(option=option):
                settle(ref.at[pl.ds(0, option)], sem)

    def edge_exists(side):
        return pick(side == 0, tm > 0, tm < n - 1)

    def sharing(side):
        return sum(jnp.where(is_shared(side * half_slots + k), 1, 0) for k in range(half_slots))

    def put(slot, dest, value):
        value = value.astype(jnp.bfloat16)

        @pl.when(dest == tm)
        def _():
            recvb[per * tm + slot - 2] = value

        @pl.when(dest != tm)
        def _():
            sendb[dest * slots + slot] = value

    def first_shared(side):
        flags = [is_shared(side * half_slots + k) for k in range(half_slots)]
        first = half_slots - 1
        for k in range(half_slots - 2, -1, -1):
            first = jnp.where(flags[k], k, first)
        return side * half_slots + first

    def runs(table):
        found = {}
        for tm_at in range(n):
            slot = 0
            while slot < slots:
                length = 0
                while slot + length < slots and tm_at in table[slot + length]:
                    length += 1
                if length:
                    found.setdefault((slot, length), []).append(tm_at)
                slot += length + 1
        return found

    def hops(dest):
        return ((tm == 1) & (dest >= half_n)) | ((tm == n - 2) & (dest < half_n))

    def relay_rank(dest):
        return dest // 2 % (half_n // 2)

    def to_relay(first, length, place, dest):
        return pltpu.make_async_remote_copy(
            src_ref=sendb.at[pl.ds(dest * slots + first, length)], dst_ref=relayb.at[pl.ds(place, length)],
            send_sem=asend.at[0], recv_sem=rrecv.at[0],
            device_id={"tm": tm + 1 - 2 * parity, "freq": fr}, device_id_type=MESH)

    def relay_runs(source):
        placed, place = [], 0
        for (first, length), devs in runs(whole).items():
            if source in devs:
                placed.append((first, length, place))
                place += length * (half_n // 2)
        return placed, place

    def send_to_relay(dest):
        for source in (1, n - 2):
            @pl.when((tm == source) & hops(dest))
            def _(source=source):
                for first, length, place in relay_runs(source)[0]:
                    for slot in range(first, first + length):
                        sendb[dest * slots + slot] = parts[dest, slot * ROWS : (slot + 1) * ROWS, :].astype(jnp.bfloat16)
                    to_relay(first, length, place + length * relay_rank(dest), dest).start()

    def relay():
        for me, source in ((0, 1), (n - 1, n - 2)):
            @pl.when(tm == me)
            def _(source=source):
                placed, amount = relay_runs(source)
                settle(relayb.at[pl.ds(0, amount)], rrecv.at[0])
                for first, length, place in placed:
                    for rank in range(half_n // 2):
                        dest = 2 * rank + (half_n if source == 1 else 0) + 1 - source % 2
                        spot = place + length * rank
                        pltpu.make_async_remote_copy(
                            src_ref=relayb.at[pl.ds(spot, length)],
                            dst_ref=recvb.at[pl.ds(per * source + first - 2, length)],
                            send_sem=fsend.at[0], recv_sem=arecv.at[0],
                            device_id={"tm": dest, "freq": fr}, device_id_type=MESH).start()

    def send_whole(dest, chosen):
        for (first, length), devs in runs(whole).items():
            @pl.when(member(tm, devs) & chosen)
            def _(first=first, length=length):
                for slot in range(first, first + length):
                    put(slot, dest, parts[dest, slot * ROWS : (slot + 1) * ROWS, :])

                @pl.when(dest != tm)
                def _():
                    scatter(first, length, dest).start()

    diagonal = (lax.broadcasted_iota(jnp.int32, (ROWS, 128), 0)
                == lax.broadcasted_iota(jnp.int32, (ROWS, 128), 1))

    def encode(slot, g, d):
        value = parts[2 * g + d, slot * ROWS : (slot + 1) * ROWS, :]
        peak = jnp.maximum(jnp.max(jnp.abs(value), axis=1, keepdims=True), 1e-30)
        whole_numbers = (value * (32767.0 / peak) + 12582912.0) - 12582912.0
        sendp[(2 * g + d) * slots + slot] = whole_numbers.astype(jnp.int32).astype(jnp.int16)
        line = jnp.sum(jnp.where(diagonal, peak, 0.0), axis=0, keepdims=True)
        row = 2 * (slot % half_slots) + d
        scales[slot // half_slots * half_n + g, row : row + 1, :] = line

    lengths = sorted({sum(tm_at in devs for devs in shared[side * half_slots : (side + 1) * half_slots])
                      for tm_at in range(n) for side in range(2)} - {0})

    @pl.loop(0, half_n)
    def _(k):
        g = group(k)
        settle(xv.at[g], load_sem.at[1 + g])
        for c in range(3):
            part = jnp.dot(t_ref[...], xv[g, c], preferred_element_type=jnp.float32)
            for d in range(2):
                parts[2 * g + d, :, c * pw : (c + 1) * pw] = part[:, d * pw : (d + 1) * pw]

        for d in range(2):
            for slot in range(slots):
                if shared[slot]:
                    @pl.when(member(tm, shared[slot]) & is_theirs(slot, 2 * g + d))
                    def _(slot=slot, d=d):
                        encode(slot, g, d)

        @pl.when(k == 0)
        def _():
            pl.semaphore_wait(barrier, total - 1)

        for side in range(2):
            _, whole_group, all_mine = division(n, tm, side, 2 * g)

            @pl.when(edge_exists(side) & jnp.logical_not(whole_group & all_mine))
            def _(side=side):
                scale_copy(side, g).start()

        def send_codes(want):
            for side in range(2):
                for d in range(2):
                    theirs = division(n, tm, side, 2 * g + d)[0]
                    for length in lengths:
                        @pl.when(edge_exists(side) & theirs & (parity == (want ^ side)) & (sharing(side) == length))
                        def _(side=side, d=d, length=length):
                            exchange(first_shared(side), length, 2 * g + d).start()

        send_codes(1)
        send_to_relay(2 * g + 1 - parity)
        for d in range(2):
            send_whole(2 * g + d, parity == d)
        send_codes(0)

    def send_crossing():
        @pl.loop(0, half_n)
        def _(k):
            dest = 2 * group(k) + 1 - parity
            send_whole(dest, jnp.logical_not(hops(dest)))

    counts = [sum(tm_at in devs for devs in shared) for tm_at in range(n)]

    @pl.loop(0, 2)
    def _(turn):
        side = jnp.where(turn == 0, 1 - parity, parity)

        @pl.loop(0, half_n)
        def _(k):
            g = group(k)
            _, whole_group, all_mine = division(n, tm, side, 2 * g)

            @pl.when(edge_exists(side) & (jnp.logical_not(whole_group) | all_mine))
            def _():
                settle(oscales.at[side * half_n + g], srecv.at[side * half_n + g])
                settle_count(others, sharing(side) * jnp.where(whole_group, 2, 1), precv.at[side * half_n + g],
                             [count * twice for count in range(1, half_slots + 1) for twice in (1, 2)])
                for d in range(2):
                    dest = 2 * g + d
                    for index in range(half_slots):
                        slot = side * half_slots + index

                        @pl.when(is_shared(slot) & jnp.logical_not(is_theirs(slot, dest)))
                        def _(slot=slot, dest=dest, row=2 * index + d):
                            line = oscales[side * half_n + g, row : row + 1, :]
                            peak = jnp.sum(jnp.where(diagonal, line, 0.0), axis=1, keepdims=True)
                            other = others[dest * slots + slot].astype(jnp.int32).astype(jnp.float32)
                            here = parts[dest, pl.ds(pl.multiple_of(slot * ROWS, ROWS), ROWS), :]
                            put(slot, dest, here + other * (peak * (1.0 / 32767.0)))

                    mine_here = jnp.logical_not(division(n, tm, side, dest)[0]) & (dest != tm)
                    for length in lengths:
                        @pl.when(mine_here & (sharing(side) == length))
                        def _(length=length, dest=dest):
                            scatter(first_shared(side), length, dest).start()


            @pl.when((turn == 0) & (k == 0))
            def _():
                relay()

            @pl.when((turn == 0) & (k == 0))
            def _():
                send_crossing()

    alone = [sum(tm_at in devs for devs in whole) for tm_at in range(n)]
    pitch = spec32.shape[1] // NB
    missing = [NB - alone[tm_at] - counts[tm_at] for tm_at in range(n)]
    settle_count(recvb, sum(jnp.where(tm == tm_at, missing[tm_at], 0) for tm_at in range(n)), arecv.at[0], missing)
    for block in range(NB):
        values = recvb[block]
        for c in range(3):
            spec32[c, block * pitch : block * pitch + ROWS, :] = values[:, c * 128 : (c + 1) * 128].astype(jnp.float32)
    for f in range(NF):
        for r in range(2):
            spec[f, r * NB : (r + 1) * NB, :] = jnp.concatenate([
                spec32[c, pl.ds(2 * f + r, NB, stride=pitch), :].astype(jnp.bfloat16)
                for c in range(3)], axis=1)

    def to_owner(k):
        first, last = owner(NF - 1 - k), owner(k)
        near_start = tm < half_n
        f = jnp.where(near_start, NF - 1 - k, k)
        place = {"tm": jnp.where(near_start, first // nf_dev, last // nf_dev),
                 "freq": jnp.where(near_start, first % nf_dev, last % nf_dev)}
        return f, pltpu.make_async_remote_copy(
            src_ref=gpart.at[f], dst_ref=gath.at[lin], send_sem=gsend.at[0],
            recv_sem=grecv.at[0], device_id=place, device_id_type=MESH)

    upper = lax.broadcasted_iota(jnp.int32, (NB, NB), 1) >= lax.broadcasted_iota(jnp.int32, (NB, NB), 0)
    for f in range(NF):
        real, imag = spec[f, :NB, :], spec[f, NB:, :]
        lhs = jnp.concatenate([real, imag], axis=1)
        rhs = jnp.concatenate([lhs, jnp.concatenate([imag, -real], axis=1)], axis=0)
        gram = lax.dot_general(lhs, rhs, (((1,), (1,)), ((), ())), preferred_element_type=jnp.float32)
        packed = jnp.where(upper, gram[:, :NB], gram[:, NB:])
        gpart[f] = jnp.concatenate([packed[8 * q : 8 * q + 8] for q in range(NB // 8)], axis=1)
        if f % 16 == 15:
            for sent in range(f - 15, f + 1):
                target, copy = to_owner(sent)

                @pl.when(lin != owner(target))
                def _(copy=copy):
                    copy.start()

    def coef_to(away):
        return pltpu.make_async_remote_copy(
            src_ref=msg, dst_ref=crecv.at[mine], send_sem=csend.at[0],
            recv_sem=crcv.at[0], device_id=displaced(away), device_id_type=MESH)

    @pl.when(owns)
    def _():
        gath[lin] = gpart[mine]

        settle(gath.at[pl.ds(0, total - 1)], grecv.at[0])
        packed = jnp.sum(gath[...], axis=0)
        square = jnp.concatenate([packed[:, q * NB : (q + 1) * NB] for q in range(NB // 8)], axis=0)
        flipped = jnp.transpose(square)
        ri = lax.broadcasted_iota(jnp.int32, (NB, NB), 0)
        ci = lax.broadcasted_iota(jnp.int32, (NB, NB), 1)
        gram_re = jnp.where(ci >= ri, square, flipped)
        gram_im = jnp.where(ci < ri, square, jnp.where(ci > ri, -flipped, 0.0))
        energy = jnp.sum(jnp.where(ri == ci, gram_re, 0.0), axis=(0, 1), keepdims=True) / (3.0 * NB * points)
        hermit = jnp.concatenate([
            jnp.concatenate([gram_re, -gram_im, gram_re, -gram_im], axis=1),
            jnp.concatenate([gram_im, gram_re, gram_im, gram_re], axis=1)], axis=0)
        frob = jnp.sqrt(0.5 * jnp.sum(hermit * hermit, axis=(0, 1), keepdims=True) + 1e-06)
        ri = lax.broadcasted_iota(jnp.int32, (2 * NB, 4 * NB), 0)
        ci = lax.broadcasted_iota(jnp.int32, (2 * NB, 4 * NB), 1)
        left = ci < 2 * NB
        identity = jnp.where(ri == (ci & (2 * NB - 1)), 1.0, 0.0).astype(jnp.float32)

        def pieces(a):
            high = a.astype(jnp.bfloat16)
            rest = a - high.astype(jnp.float32)
            mid = rest.astype(jnp.bfloat16)
            return high, mid, (rest - mid.astype(jnp.float32)).astype(jnp.bfloat16)

        def mul(a, b):
            ah, am, al = a
            bh, bm, bl = b
            lhs = jnp.concatenate([ah, am, jnp.where(left[: ah.shape[0]], ah, al)], axis=1)
            rhs = jnp.concatenate([bh, bm, bh, bm, bl, bh], axis=0)
            return jnp.dot(lhs, rhs, preferred_element_type=jnp.float32)

        iterate = hermit / frob
        inverse = identity
        for step in range(NSIT):
            it = pieces(iterate)
            if step:
                inv = pieces(inverse)
            factor = 1.5 * identity - 0.5 * (mul(inv, it) if step else iterate)
            fac = pieces(factor)
            if step < NSIT - 1:
                iterate = mul(it, fac)
                inverse = mul(fac, inv) if step else factor
            else:
                inverse = mul(tuple(piece[:NB] for piece in fac), inv)
        scaled = inverse * jnp.sqrt(6.0 * points / frob)
        high, mid, rest = [piece.astype(jnp.float32) for piece in pieces(energy)]
        top = ri[:NB]
        extra = jnp.where(top == 0, high, jnp.where(top == 1, mid, jnp.where(top == 2, rest, 0.0)))
        scaled = jnp.where((ci[:NB] & (2 * NB - 1)) == NB + top, extra, scaled)
        msg[...] = jnp.where(left[: NB // 2], scaled[: NB // 2], scaled[NB // 2 :]).astype(jnp.bfloat16)
        crecv[mine] = msg[...]

        for away in range(total - 1, 0, -1):
            coef_to(away).start()

    for tm_at in range(n):
        handed, groups = 0, 0
        for slot in range(slots):
            if tm_at in shared[slot]:
                handed += sum(division(n, tm_at, slot // half_slots, dest)[0] for dest in range(n))
        for side in range(2):
            if 0 < tm_at + side < n:
                for g in range(half_n):
                    _, whole_group, all_mine = division(n, tm_at, side, 2 * g)
                    groups += not (whole_group and all_mine)

        @pl.when(tm == tm_at)
        def _(tm_at=tm_at, handed=handed, groups=groups):
            settle(sendp.at[pl.ds(0, handed)], psend.at[0])
            own = n * (alone[tm_at] + counts[tm_at]) - handed
            settle(sendb.at[pl.ds(0, own - alone[tm_at] - counts[tm_at])], asend.at[0])
            settle(scales.at[pl.ds(0, groups)], ssend.at[0])
            if tm_at in (0, n - 1):
                settle(relayb.at[pl.ds(0, relay_runs(1 if tm_at == 0 else n - 2)[1])], fsend.at[0])

    sent = jnp.where(owns, NF - 1, NF)
    settle_count(gpart, sent, gsend.at[0], [NF - 1, NF])
    settle_count(crecv, sent, crcv.at[0], [NF - 1, NF])
    coefs_ref[...] = crecv[...]

    @pl.when(owns)
    def _():
        settle(gath.at[pl.ds(0, total - 1)], csend.at[0])


def finish_kernel(spec, crecv, modes_hbm, energy_hbm, stage, modes_ref, energy_ref, sem):
    pw = modes_ref.shape[1]

    lanes = lax.broadcasted_iota(jnp.int32, (NB, 2 * NB), 1)
    signs = jnp.where(lanes < NB, 1.0, -1.0).astype(jnp.bfloat16)
    hidden = lanes == NB + lax.broadcasted_iota(jnp.int32, (NB, 2 * NB), 0)
    wide_lane = lax.broadcasted_iota(jnp.int32, (1, NF), 1)
    energies = jnp.zeros((1, NF), jnp.float32)
    for f in range(NF):
        pairs = crecv[f]
        straight = jnp.concatenate([pairs[:, : 2 * NB], pairs[:, 2 * NB :]], axis=0)
        found = jnp.sum(jnp.where(hidden, straight.astype(jnp.float32), 0.0), axis=(0, 1), keepdims=True)
        energies = jnp.where(wide_lane == f, found, energies)
        straight = jnp.where(hidden, jnp.zeros_like(straight), straight)
        crossed = jnp.concatenate([straight[:, NB:], straight[:, :NB]], axis=1)
        stacked = jnp.concatenate([straight * signs, crossed], axis=0)
        out = jnp.dot(stacked, spec[f], preferred_element_type=jnp.float32)
        for c in range(3):
            for o in range(2):
                stage[f % 4, pl.ds(2 * c + o, NB, stride=6), :] = out[o * NB : (o + 1) * NB, c * pw : (c + 1) * pw]
        modes_ref[f * 6 * NB : (f + 1) * 6 * NB, :] = stage[f % 4].astype(jnp.bfloat16)
        part = pl.ds(f * 6 * NB, 6 * NB)
        pltpu.make_async_copy(modes_ref.at[part], modes_hbm.at[part], sem.at[0]).start()
    energy_ref[...] = energies
    last = pltpu.make_async_copy(energy_ref, energy_hbm, sem.at[1])
    last.start()
    pltpu.make_async_copy(modes_ref, modes_hbm, sem.at[0]).wait()
    last.wait()


def fused(n, nf_dev, chosen, snapshots, block_starts, freq_index):
    per, whole, shared, holders = chosen
    rows, count, wide = snapshots.shape
    total = n * nf_dev
    pw = wide // n
    slots = per + 4
    f32, bf16 = jnp.float32, jnp.bfloat16
    dma = pltpu.SemaphoreType.DMA
    vmem = pl.BlockSpec(memory_space=pltpu.VMEM)
    spec, coefs = pl.pallas_call(
        functools.partial(kernel, n, nf_dev, per, whole, shared, holders, float(wide * nf_dev)),
        out_shape=(jax.ShapeDtypeStruct((NF, 2 * NB, 3 * pw), bf16),
                   jax.ShapeDtypeStruct((NF, NB // 2, 4 * NB), bf16)),
        in_specs=[pl.BlockSpec(memory_space=pltpu.HBM)] * 2,
        out_specs=(vmem, vmem),
        scratch_shapes=[
            pltpu.SMEM((NB + NF,), jnp.int32),
            pltpu.VMEM((slots * ROWS, rows), bf16),
            pltpu.VMEM((n // 2, 3, rows, 2 * pw), bf16),
            pltpu.VMEM((n, slots * ROWS, 3 * pw), f32),
            pltpu.VMEM((slots * n, ROWS, 3 * pw), jnp.int16),
            pltpu.VMEM((slots * n, ROWS, 3 * pw), jnp.int16),
            pltpu.VMEM((slots * n // 2, ROWS, 3 * pw), bf16),
            pltpu.VMEM((n, slots, 128), f32),
            pltpu.VMEM((n, slots, 128), f32),
            pltpu.VMEM((slots * n, ROWS, 3 * pw), bf16),
            pltpu.VMEM((NB, ROWS, 3 * pw), bf16),
            pltpu.VMEM((3, NB * (ROWS + 8), pw), f32),
            pltpu.VMEM((NF, NB // 4, 4 * NB), f32),
            pltpu.VMEM((total, NB // 4, 4 * NB), f32),
            pltpu.VMEM((NB // 2, 4 * NB), bf16),
            pltpu.VMEM((NF, NB // 2, 4 * NB), bf16),
            dma((1 + n // 2,)), dma((1,)), dma((n,)), dma((1,)), dma((1,)), dma((1,)), dma((n,)),
            dma((1,)), dma((1,)), dma((1,)), dma((1,)), dma((1,)), dma((1,)),
        ],
        compiler_params=pltpu.CompilerParams(
            collective_id=0, has_side_effects=True, vmem_limit_bytes=54_000_000),
    )(jnp.transpose(snapshots, (1, 0, 2)), jnp.concatenate([block_starts, freq_index]))
    modes, energy = pl.pallas_call(
        finish_kernel,
        out_shape=(jax.ShapeDtypeStruct((NF * NB * 6, pw), bf16), jax.ShapeDtypeStruct((1, NF), f32)),
        in_specs=[vmem, vmem],
        out_specs=[pl.BlockSpec(memory_space=pltpu.HBM)] * 2,
        scratch_shapes=[
            pltpu.VMEM((4, 6 * NB, pw), f32), pltpu.VMEM((NF * NB * 6, pw), bf16),
            pltpu.VMEM((1, NF), f32), dma((2,)),
        ],
        compiler_params=pltpu.CompilerParams(vmem_limit_bytes=8_000_000),
    )(spec, coefs)
    modes = modes.reshape(NF, NB, 3, 2, pw).transpose(0, 1, 3, 2, 4)
    return modes, energy.reshape(NF)


def solution(mesh):
    n, nf_dev = mesh.shape["tm"], mesh.shape["freq"]

    def body(snapshots, block_starts, freq_index):
        rows, _, wide = snapshots.shape
        chosen = plan(n, rows, n * nf_dev, wide // n)
        if chosen is None:
            return local(snapshots, block_starts, freq_index)
        return fused(n, nf_dev, chosen, snapshots, block_starts, freq_index)

    return jax.shard_map(
        body,
        mesh=mesh,
        in_specs=(P("tm", None, "freq"), P(), P()),
        out_specs=(P(None, None, None, None, ("freq", "tm")), P()),
        check_vma=False,
    )
```

```python
import functools
import math

import jax
import jax.numpy as jnp
import numpy as np
from jax import lax
from jax.experimental import pallas as pl
from jax.experimental.pallas import tpu as pltpu
from jax.sharding import PartitionSpec as P

NB = 32
NFFT = 256
NF = 16
NSIT = 6


def for_sending(shard):
    return jax.tree.map(lambda a: a.astype(jnp.bfloat16) if a.dtype == jnp.float32 else a, shard)


def dft_rows(freq_index):
    times_idx = jnp.arange(NFFT, dtype=jnp.int32)
    phase_int = freq_index[:, None] * times_idx[None, :] % NFFT
    angles = 2.0 * math.pi / NFFT * phase_int.astype(jnp.float32)
    window = 0.5 - 0.5 * jnp.cos(2.0 * math.pi / NFFT * times_idx.astype(jnp.float32))
    scaling = 1.0 / jnp.sqrt(jnp.sum(window * window))
    cosine = window[None, :] * jnp.cos(angles) * scaling
    sine_rows = -window[None, :] * jnp.sin(angles) * scaling
    return jnp.stack([cosine, sine_rows], 1).reshape(2 * NF, NFFT).astype(jnp.bfloat16)


def block_rows(block_starts):
    return block_starts[:, None] + jnp.arange(NFFT, dtype=jnp.int32)[None, :]


def matmul_batch(left, right):
    return jnp.einsum("fij,fjk->fik", left, right, precision=lax.Precision.HIGHEST)


def whiten(summed, points):
    gram_re = summed[:, 0]
    gram_im = summed[:, 1]
    top_rows = jnp.concatenate([gram_re, -gram_im], 2)
    low_rows = jnp.concatenate([gram_im, gram_re], 2)
    hermit = jnp.concatenate([top_rows, low_rows], 1)
    frob = jnp.sqrt(jnp.sum(hermit * hermit, axis=(1, 2)) + 1e-06)
    identity = jnp.eye(2 * NB, dtype=jnp.float32)[None]
    iterate = hermit / frob[:, None, None]
    inverse = jnp.broadcast_to(identity, hermit.shape)
    for iteration in range(NSIT):
        factor = 1.5 * identity - 0.5 * matmul_batch(inverse, iterate)
        iterate = matmul_batch(iterate, factor)
        inverse = matmul_batch(factor, inverse)
    columns = inverse[:, :, :NB] * jnp.sqrt(6.0 * points / frob)[:, None, None]
    upper = columns[:, :NB]
    lower = columns[:, NB:]
    coefficients = jnp.stack([jnp.stack([upper, -lower], 1), jnp.stack([lower, upper], 1)], 1)
    energy = jnp.trace(gram_re, axis1=1, axis2=2) / (3.0 * NB * points)
    return (coefficients, energy)


def local(snapshots, block_starts, freq_index):
    dft_table = dft_rows(freq_index)
    offsets = block_rows(block_starts)
    series = lax.all_to_all(snapshots, "tm", split_axis=2, concat_axis=0, tiled=True)
    count = series.shape[1]
    width = series.shape[2]
    columns_all = series.reshape(series.shape[0], count * width)
    windows = jnp.take(columns_all, offsets, axis=0)
    spectra_part = jnp.einsum(
        "rt,btn->rbn", dft_table, windows, preferred_element_type=jnp.float32
    ).astype(jnp.bfloat16)
    spectra = spectra_part.reshape(2 * NF, NB, count, width)
    width = spectra.shape[3]
    points = float(width * lax.axis_size("tm") * lax.axis_size("freq"))
    flat_spec = spectra.reshape(NF, 2, NB, 3 * width)
    real_part = flat_spec[:, 0]
    imag_part = flat_spec[:, 1]
    gram_re = jnp.einsum("fbn,fcn->fbc", real_part, real_part, preferred_element_type=jnp.float32)
    gram_re = gram_re + jnp.einsum(
        "fbn,fcn->fbc", imag_part, imag_part, preferred_element_type=jnp.float32
    )
    cross_terms = jnp.einsum(
        "fbn,fcn->fbc", real_part, imag_part, preferred_element_type=jnp.float32
    )
    partial_gram = jnp.stack([gram_re, cross_terms - jnp.swapaxes(cross_terms, 1, 2)], 1)
    shared = lax.psum_scatter(partial_gram, "freq", scatter_dimension=0, tiled=True)
    shared = lax.psum(shared, "tm")
    coef_part, energy_part = whiten(shared, points)
    coefficients, energy = (
        lax.all_gather(for_sending(coef_part), "freq", axis=0, tiled=True).astype(coef_part.dtype),
        lax.all_gather(for_sending(energy_part), "freq", axis=0, tiled=True).astype(
            energy_part.dtype
        ),
    )
    coef_bf = jnp.transpose(coefficients.astype(jnp.bfloat16), (0, 4, 1, 2, 3))
    modes = jnp.einsum(
        "fjorb,frbn->fjon", coef_bf, flat_spec, preferred_element_type=jnp.float32
    ).astype(jnp.bfloat16)
    return (modes.reshape(NF, NB, 2, 3, width), energy)


MESH = pl.DeviceIdType.MESH
ROWS = 2 * NF
HOP = 128
JIT = 64


def plan(n, rows, total, width):
    if n % 4 or NB % n or total % (2 * NF) or width != 128 or rows % 16:
        return None
    per = NB // n
    if per < 4 or per % 2:
        return None
    slots = per + 4
    whole = [[] for _ in range(slots)]
    shared = [[] for _ in range(slots)]
    holders = []
    for block in range(NB):
        touched = [
            dev for dev in range(n)
            if HOP * block < rows * (dev + 1) and HOP * block + JIT + NFFT > rows * dev
        ]
        holders.append(touched)
        if len(touched) > 2:
            return None
        for dev in touched:
            slot = block - per * dev + 2
            if not 0 <= slot < slots:
                return None
            if len(touched) == 2:
                if (slot < slots // 2) != (dev == touched[1]):
                    return None
                shared[slot].append(dev)
            else:
                whole[slot].append(dev)
    return per, whole, shared, holders


def base_table(ints_ref):
    row = lax.broadcasted_iota(jnp.int32, (ROWS, NFFT), 0)
    times_idx = lax.broadcasted_iota(jnp.int32, (ROWS, NFFT), 1)
    freqs = jnp.zeros((ROWS, NFFT), jnp.int32)
    for f in range(NF):
        freqs = jnp.where((row >> 1) == f, ints_ref[NB + f], freqs)
    phase = (freqs * times_idx) & (NFFT - 1)
    angles = 2.0 * math.pi / NFFT * phase.astype(jnp.float32)
    window = 0.5 - 0.5 * jnp.cos(2.0 * math.pi / NFFT * times_idx.astype(jnp.float32))
    hann = 0.5 - 0.5 * np.cos(2.0 * math.pi / NFFT * np.arange(NFFT))
    scaling = np.float32(1.0 / np.sqrt(np.sum(hann * hann)))
    cosine = window * jnp.cos(angles) * scaling
    sine = -window * jnp.sin(angles) * scaling
    return jnp.where((row & 1) == 1, sine, cosine).astype(jnp.bfloat16)


def shifted(base, shift, rows):
    source = lax.broadcasted_iota(jnp.int32, (NFFT, rows), 0)
    target = lax.broadcasted_iota(jnp.int32, (NFFT, rows), 1)
    pick = jnp.where(source - target == shift, 1.0, 0.0).astype(jnp.bfloat16)
    return jnp.dot(base, pick, preferred_element_type=jnp.float32).astype(jnp.bfloat16)


def member(index, devs):
    if not devs:
        return None
    if devs == list(range(devs[0], devs[-1] + 1)):
        return (index >= devs[0]) & (index <= devs[-1])
    hit = index == devs[0]
    for dev in devs[1:]:
        hit = hit | (index == dev)
    return hit


def division(n, tm, side, dest):
    edge, half = tm + side, n // 2
    middle = edge == half
    left = dest < half
    all_mine = middle & (left == (tm < half))
    theirs = (middle & (all_mine ^ True)) | ((middle ^ True) & (dest % 2 != tm % 2))
    return theirs, middle, all_mine


def kernel(n, nf_dev, per, whole, shared, holders, points, x_hbm, ints_hbm,
           spec, coefs_ref, ints_ref, t_ref, xv, parts,
           sendp, others, relayb, scales, oscales, sendb, recvb, spec32, gpart, gath, msg, crecv,
           load_sem, psend, precv, rrecv, fsend, ssend, srecv, asend, arecv, gsend, grecv, csend, crcv):
    tm = lax.axis_index("tm")
    fr = lax.axis_index("freq")
    total = n * nf_dev
    lin = tm * nf_dev + fr
    step, lowest = total // (2 * NF), total // 4
    slots = per + 4
    half_slots = slots // 2
    mine = (lin - lowest) // step
    owns = (lin >= lowest) & (lin < lowest + NF * step) & ((lin - lowest) % step == 0)
    half_n = n // 2
    parity = tm % 2
    rows = xv.shape[2]
    pw = xv.shape[3] // 2

    def owner(f):
        return lowest + f * step

    def where_is(index):
        return {"tm": index // nf_dev, "freq": index % nf_dev}

    def displaced(away):
        row, col = tm + away // nf_dev, fr + away % nf_dev
        return {"tm": jnp.where(row >= n, row - n, row),
                "freq": jnp.where(col >= nf_dev, col - nf_dev, col)}

    def group(k):
        inner = (tm // 2 > 0) & (tm // 2 < half_n - 1) & (k >= half_n - 2)
        k = jnp.where(inner, 2 * half_n - 3 - k, k)
        return jnp.where(tm < half_n, half_n - 1 - k, k)

    def load(g, c):
        return pltpu.make_async_copy(
            x_hbm.at[c, :, pl.ds(pl.multiple_of(g * 2 * pw, 2 * pw), 2 * pw)], xv.at[g, c],
            load_sem.at[1 + g])

    small = pltpu.make_async_copy(ints_hbm, ints_ref, load_sem.at[0])
    small.start()
    for k in range(half_n):
        for c in range(3):
            load(group(k), c).start()
    barrier = pltpu.get_barrier_semaphore()

    for away in range(total - 1, 0, -1):
        pl.semaphore_signal(barrier, inc=1, device_id=displaced(away), device_id_type=MESH)

    small.wait()
    base = base_table(ints_ref)
    for slot in range(slots):
        block = per * tm + slot - 2
        start = ints_ref[jnp.clip(block, 0, NB - 1)]
        inside = (block >= 0) & (block < NB)
        shift = jnp.where(inside, rows * tm - start, 4 * (rows + NFFT))
        t_ref[slot * ROWS : (slot + 1) * ROWS, :] = shifted(base, shift, rows)
    scales[...] = jnp.zeros_like(scales)

    def low(slot):
        return slot < half_slots

    def pick(flag, yes, no):
        return (yes if flag else no) if isinstance(flag, bool) else jnp.where(flag, yes, no)

    def partner(slot):
        return pick(low(slot), (tm + n - 1) % n, (tm + 1) % n)

    def across(slot):
        return pick(low(slot), slot + per, slot - per)

    def is_shared(slot):
        block = per * tm + slot - 2
        edge = rows * (tm + pick(low(slot), 0, 1))
        inside = (block >= 0) & (block < NB) & (edge > 0) & (edge < rows * n)
        return inside & (HOP * block < edge) & (HOP * block + JIT + NFFT > edge)

    def is_theirs(slot, dest):
        return division(n, tm, slot // half_slots, dest)[0]

    def exchange(slot, length, dest):
        return pltpu.make_async_remote_copy(
            src_ref=sendp.at[pl.ds(dest * slots + slot, length)],
            dst_ref=others.at[pl.ds(dest * slots + across(slot), length)],
            send_sem=psend.at[0], recv_sem=precv.at[across(slot) // half_slots * half_n + dest // 2],
            device_id={"tm": partner(slot), "freq": fr}, device_id_type=MESH)

    def scale_copy(side, g):
        return pltpu.make_async_remote_copy(
            src_ref=scales.at[side * half_n + g], dst_ref=oscales.at[(1 - side) * half_n + g],
            send_sem=ssend.at[0], recv_sem=srecv.at[(1 - side) * half_n + g],
            device_id={"tm": partner(side * half_slots), "freq": fr}, device_id_type=MESH)

    def scatter(slot, length, dest):
        block = per * tm + slot - 2
        return pltpu.make_async_remote_copy(
            src_ref=sendb.at[pl.ds(dest * slots + slot, length)], dst_ref=recvb.at[pl.ds(block, length)],
            send_sem=asend.at[0], recv_sem=arecv.at[jnp.where(block > NB // 2, 1, 0)],
            device_id={"tm": dest, "freq": fr}, device_id_type=MESH)

    def settle(ref, sem):
        pltpu.make_async_copy(ref, ref, sem).wait()

    def settle_count(ref, count, sem, options):
        for option in sorted(set(options)):
            @pl.when(count == option)
            def _(option=option):
                settle(ref.at[pl.ds(0, option)], sem)

    def edge_exists(side):
        return pick(side == 0, tm > 0, tm < n - 1)

    def sharing(side):
        return sum(jnp.where(is_shared(side * half_slots + k), 1, 0) for k in range(half_slots))

    def put(slot, dest, value):
        value = value.astype(jnp.bfloat16)

        @pl.when(dest == tm)
        def _():
            recvb[per * tm + slot - 2] = value

        @pl.when(dest != tm)
        def _():
            sendb[dest * slots + slot] = value

    def first_shared(side):
        flags = [is_shared(side * half_slots + k) for k in range(half_slots)]
        first = half_slots - 1
        for k in range(half_slots - 2, -1, -1):
            first = jnp.where(flags[k], k, first)
        return side * half_slots + first

    def runs(table):
        found = {}
        for tm_at in range(n):
            slot = 0
            while slot < slots:
                length = 0
                while slot + length < slots and tm_at in table[slot + length]:
                    length += 1
                if length:
                    found.setdefault((slot, length), []).append(tm_at)
                slot += length + 1
        return found

    def hops(dest):
        return ((tm == 1) & (dest >= half_n)) | ((tm == n - 2) & (dest < half_n))

    def relay_rank(dest):
        return dest // 2 % (half_n // 2)

    def to_relay(first, length, place, dest):
        return pltpu.make_async_remote_copy(
            src_ref=sendb.at[pl.ds(dest * slots + first, length)], dst_ref=relayb.at[pl.ds(place, length)],
            send_sem=asend.at[0], recv_sem=rrecv.at[0],
            device_id={"tm": tm + 1 - 2 * parity, "freq": fr}, device_id_type=MESH)

    def relay_runs(source):
        placed, place = [], 0
        for (first, length), devs in runs(whole).items():
            if source in devs:
                placed.append((first, length, place))
                place += length * (half_n // 2)
        return placed, place

    def send_to_relay(dest):
        for source in (1, n - 2):
            @pl.when((tm == source) & hops(dest))
            def _(source=source):
                for first, length, place in relay_runs(source)[0]:
                    for slot in range(first, first + length):
                        sendb[dest * slots + slot] = parts[dest, slot * ROWS : (slot + 1) * ROWS, :].astype(jnp.bfloat16)
                    to_relay(first, length, place + length * relay_rank(dest), dest).start()

    def relay():
        for me, source in ((0, 1), (n - 1, n - 2)):
            @pl.when(tm == me)
            def _(source=source):
                placed, amount = relay_runs(source)
                settle(relayb.at[pl.ds(0, amount)], rrecv.at[0])
                for first, length, place in placed:
                    for rank in range(half_n // 2):
                        dest = 2 * rank + (half_n if source == 1 else 0) + 1 - source % 2
                        spot = place + length * rank
                        pltpu.make_async_remote_copy(
                            src_ref=relayb.at[pl.ds(spot, length)],
                            dst_ref=recvb.at[pl.ds(per * source + first - 2, length)],
                            send_sem=fsend.at[0], recv_sem=arecv.at[int(per * source + first - 2 > NB // 2)],
                            device_id={"tm": dest, "freq": fr}, device_id_type=MESH).start()

    def send_whole(dest, chosen):
        for (first, length), devs in runs(whole).items():
            @pl.when(member(tm, devs) & chosen)
            def _(first=first, length=length):
                for slot in range(first, first + length):
                    put(slot, dest, parts[dest, slot * ROWS : (slot + 1) * ROWS, :])

                @pl.when(dest != tm)
                def _():
                    scatter(first, length, dest).start()

    diagonal = (lax.broadcasted_iota(jnp.int32, (ROWS, 128), 0)
                == lax.broadcasted_iota(jnp.int32, (ROWS, 128), 1))

    def encode(slot, g, d):
        value = parts[2 * g + d, slot * ROWS : (slot + 1) * ROWS, :]
        peak = jnp.maximum(jnp.max(jnp.abs(value), axis=1, keepdims=True), 1e-30)
        whole_numbers = (value * (32767.0 / peak) + 12582912.0) - 12582912.0
        sendp[(2 * g + d) * slots + slot] = whole_numbers.astype(jnp.int32).astype(jnp.int16)
        line = jnp.sum(jnp.where(diagonal, peak, 0.0), axis=0, keepdims=True)
        row = 2 * (slot % half_slots) + d
        scales[slot // half_slots * half_n + g, row : row + 1, :] = line

    lengths = sorted({sum(tm_at in devs for devs in shared[side * half_slots : (side + 1) * half_slots])
                      for tm_at in range(n) for side in range(2)} - {0})

    @pl.loop(0, half_n)
    def _(k):
        g = group(k)
        settle(xv.at[g], load_sem.at[1 + g])
        for c in range(3):
            part = jnp.dot(t_ref[...], xv[g, c], preferred_element_type=jnp.float32)
            for d in range(2):
                parts[2 * g + d, :, c * pw : (c + 1) * pw] = part[:, d * pw : (d + 1) * pw]

        for d in range(2):
            for slot in range(slots):
                if shared[slot]:
                    @pl.when(member(tm, shared[slot]) & is_theirs(slot, 2 * g + d))
                    def _(slot=slot, d=d):
                        encode(slot, g, d)

        @pl.when(k == 0)
        def _():
            pl.semaphore_wait(barrier, total - 1)

        for side in range(2):
            _, whole_group, all_mine = division(n, tm, side, 2 * g)

            @pl.when(edge_exists(side) & jnp.logical_not(whole_group & all_mine))
            def _(side=side):
                scale_copy(side, g).start()

        def send_codes(want):
            for side in range(2):
                for d in range(2):
                    theirs = division(n, tm, side, 2 * g + d)[0]
                    for length in lengths:
                        @pl.when(edge_exists(side) & theirs & (parity == (want ^ side)) & (sharing(side) == length))
                        def _(side=side, d=d, length=length):
                            exchange(first_shared(side), length, 2 * g + d).start()

        send_codes(1)
        send_to_relay(2 * g + 1 - parity)
        for d in range(2):
            send_whole(2 * g + d, parity == d)
        send_codes(0)

    def send_crossing():
        @pl.loop(0, half_n)
        def _(k):
            dest = 2 * group(k) + 1 - parity
            send_whole(dest, jnp.logical_not(hops(dest)))

    counts = [sum(tm_at in devs for devs in shared) for tm_at in range(n)]

    @pl.loop(0, 2)
    def _(turn):
        side = jnp.where(turn == 0, 1 - parity, parity)

        @pl.loop(0, half_n)
        def _(k):
            g = group(k)
            _, whole_group, all_mine = division(n, tm, side, 2 * g)

            @pl.when(edge_exists(side) & (jnp.logical_not(whole_group) | all_mine))
            def _():
                settle(oscales.at[side * half_n + g], srecv.at[side * half_n + g])
                settle_count(others, sharing(side) * jnp.where(whole_group, 2, 1), precv.at[side * half_n + g],
                             [count * twice for count in range(1, half_slots + 1) for twice in (1, 2)])
                for d in range(2):
                    dest = 2 * g + d
                    for index in range(half_slots):
                        slot = side * half_slots + index

                        @pl.when(is_shared(slot) & jnp.logical_not(is_theirs(slot, dest)))
                        def _(slot=slot, dest=dest, row=2 * index + d):
                            line = oscales[side * half_n + g, row : row + 1, :]
                            peak = jnp.sum(jnp.where(diagonal, line, 0.0), axis=1, keepdims=True)
                            other = others[dest * slots + slot].astype(jnp.int32).astype(jnp.float32)
                            here = parts[dest, pl.ds(pl.multiple_of(slot * ROWS, ROWS), ROWS), :]
                            put(slot, dest, here + other * (peak * (1.0 / 32767.0)))

                    mine_here = jnp.logical_not(division(n, tm, side, dest)[0]) & (dest != tm)
                    for length in lengths:
                        @pl.when(mine_here & (sharing(side) == length))
                        def _(length=length, dest=dest):
                            scatter(first_shared(side), length, dest).start()


            @pl.when((turn == 0) & (k == 0))
            def _():
                relay()

            @pl.when((turn == 0) & (k == 0))
            def _():
                send_crossing()

    alone = [sum(tm_at in devs for devs in whole) for tm_at in range(n)]
    pitch = spec32.shape[1] // NB
    late = []
    for block in range(NB):
        first = block
        while first and holders[first - 1] == holders[block]:
            first -= 1
        late.append(int(first > NB // 2))
    for h in range(2):
        group_of = [block for block in range(NB) if late[block] == h]
        missing = [sum(tm_at not in holders[block] for block in group_of) for tm_at in range(n)]
        settle_count(recvb, sum(jnp.where(tm == tm_at, missing[tm_at], 0) for tm_at in range(n)), arecv.at[h], missing)
        for block in group_of:
            values = recvb[block]
            for c in range(3):
                spec32[c, block * pitch : block * pitch + ROWS, :] = values[:, c * 128 : (c + 1) * 128].astype(jnp.float32)
        low_row = h * NB // 2
        for f in range(NF):
            for r in range(2):
                spec[f, r * NB + low_row : r * NB + low_row + NB // 2, :] = jnp.concatenate([
                    spec32[c, pl.ds(low_row * pitch + 2 * f + r, NB // 2, stride=pitch), :].astype(jnp.bfloat16)
                    for c in range(3)], axis=1)

    def to_owner(k):
        first, last = owner(NF - 1 - k), owner(k)
        near_start = tm < half_n
        f = jnp.where(near_start, NF - 1 - k, k)
        place = {"tm": jnp.where(near_start, first // nf_dev, last // nf_dev),
                 "freq": jnp.where(near_start, first % nf_dev, last % nf_dev)}
        return f, pltpu.make_async_remote_copy(
            src_ref=gpart.at[f], dst_ref=gath.at[lin], send_sem=gsend.at[0],
            recv_sem=grecv.at[0], device_id=place, device_id_type=MESH)

    upper = lax.broadcasted_iota(jnp.int32, (NB, NB), 1) >= lax.broadcasted_iota(jnp.int32, (NB, NB), 0)
    for f in range(NF):
        real, imag = spec[f, :NB, :], spec[f, NB:, :]
        lhs = jnp.concatenate([real, imag], axis=1)
        rhs = jnp.concatenate([lhs, jnp.concatenate([imag, -real], axis=1)], axis=0)
        gram = lax.dot_general(lhs, rhs, (((1,), (1,)), ((), ())), preferred_element_type=jnp.float32)
        packed = jnp.where(upper, gram[:, :NB], gram[:, NB:])
        gpart[f] = jnp.concatenate([packed[8 * q : 8 * q + 8] for q in range(NB // 8)], axis=1)
        if f % 16 == 15:
            for sent in range(f - 15, f + 1):
                target, copy = to_owner(sent)

                @pl.when(lin != owner(target))
                def _(copy=copy):
                    copy.start()

    def coef_to(away):
        return pltpu.make_async_remote_copy(
            src_ref=msg, dst_ref=crecv.at[mine], send_sem=csend.at[0],
            recv_sem=crcv.at[0], device_id=displaced(away), device_id_type=MESH)

    @pl.when(owns)
    def _():
        gath[lin] = gpart[mine]

        settle(gath.at[pl.ds(0, total - 1)], grecv.at[0])
        packed = jnp.sum(gath[...], axis=0)
        square = jnp.concatenate([packed[:, q * NB : (q + 1) * NB] for q in range(NB // 8)], axis=0)
        flipped = jnp.transpose(square)
        ri = lax.broadcasted_iota(jnp.int32, (NB, NB), 0)
        ci = lax.broadcasted_iota(jnp.int32, (NB, NB), 1)
        gram_re = jnp.where(ci >= ri, square, flipped)
        gram_im = jnp.where(ci < ri, square, jnp.where(ci > ri, -flipped, 0.0))
        energy = jnp.sum(jnp.where(ri == ci, gram_re, 0.0), axis=(0, 1), keepdims=True) / (3.0 * NB * points)
        hermit = jnp.concatenate([
            jnp.concatenate([gram_re, -gram_im, gram_re, -gram_im], axis=1),
            jnp.concatenate([gram_im, gram_re, gram_im, gram_re], axis=1)], axis=0)
        frob = jnp.sqrt(0.5 * jnp.sum(hermit * hermit, axis=(0, 1), keepdims=True) + 1e-06)
        ri = lax.broadcasted_iota(jnp.int32, (2 * NB, 4 * NB), 0)
        ci = lax.broadcasted_iota(jnp.int32, (2 * NB, 4 * NB), 1)
        left = ci < 2 * NB
        identity = jnp.where(ri == (ci & (2 * NB - 1)), 1.0, 0.0).astype(jnp.float32)

        def pieces(a):
            high = a.astype(jnp.bfloat16)
            rest = a - high.astype(jnp.float32)
            mid = rest.astype(jnp.bfloat16)
            return high, mid, (rest - mid.astype(jnp.float32)).astype(jnp.bfloat16)

        def mul(a, b):
            ah, am, al = a
            bh, bm, bl = b
            lhs = jnp.concatenate([ah, am, jnp.where(left[: ah.shape[0]], ah, al)], axis=1)
            rhs = jnp.concatenate([bh, bm, bh, bm, bl, bh], axis=0)
            return jnp.dot(lhs, rhs, preferred_element_type=jnp.float32)

        iterate = hermit / frob
        inverse = identity
        for step in range(NSIT):
            it = pieces(iterate)
            if step:
                inv = pieces(inverse)
            factor = 1.5 * identity - 0.5 * (mul(inv, it) if step else iterate)
            fac = pieces(factor)
            if step < NSIT - 1:
                iterate = mul(it, fac)
                inverse = mul(fac, inv) if step else factor
            else:
                inverse = mul(tuple(piece[:NB] for piece in fac), inv)
        scaled = inverse * jnp.sqrt(6.0 * points / frob)
        high, mid, rest = [piece.astype(jnp.float32) for piece in pieces(energy)]
        top = ri[:NB]
        extra = jnp.where(top == 0, high, jnp.where(top == 1, mid, jnp.where(top == 2, rest, 0.0)))
        scaled = jnp.where((ci[:NB] & (2 * NB - 1)) == NB + top, extra, scaled)
        msg[...] = jnp.where(left[: NB // 2], scaled[: NB // 2], scaled[NB // 2 :]).astype(jnp.bfloat16)
        crecv[mine] = msg[...]

        for away in range(total - 1, 0, -1):
            coef_to(away).start()

    for tm_at in range(n):
        handed, groups = 0, 0
        for slot in range(slots):
            if tm_at in shared[slot]:
                handed += sum(division(n, tm_at, slot // half_slots, dest)[0] for dest in range(n))
        for side in range(2):
            if 0 < tm_at + side < n:
                for g in range(half_n):
                    _, whole_group, all_mine = division(n, tm_at, side, 2 * g)
                    groups += not (whole_group and all_mine)

        @pl.when(tm == tm_at)
        def _(tm_at=tm_at, handed=handed, groups=groups):
            settle(sendp.at[pl.ds(0, handed)], psend.at[0])
            own = n * (alone[tm_at] + counts[tm_at]) - handed
            settle(sendb.at[pl.ds(0, own - alone[tm_at] - counts[tm_at])], asend.at[0])
            settle(scales.at[pl.ds(0, groups)], ssend.at[0])
            if tm_at in (0, n - 1):
                settle(relayb.at[pl.ds(0, relay_runs(1 if tm_at == 0 else n - 2)[1])], fsend.at[0])

    sent = jnp.where(owns, NF - 1, NF)
    settle_count(gpart, sent, gsend.at[0], [NF - 1, NF])
    settle_count(crecv, sent, crcv.at[0], [NF - 1, NF])
    coefs_ref[...] = crecv[...]

    @pl.when(owns)
    def _():
        settle(gath.at[pl.ds(0, total - 1)], csend.at[0])


def finish_kernel(spec, crecv, modes_hbm, energy_hbm, stage, modes_ref, energy_ref, sem):
    pw = modes_ref.shape[1]

    lanes = lax.broadcasted_iota(jnp.int32, (NB, 2 * NB), 1)
    signs = jnp.where(lanes < NB, 1.0, -1.0).astype(jnp.bfloat16)
    hidden = lanes == NB + lax.broadcasted_iota(jnp.int32, (NB, 2 * NB), 0)
    wide_lane = lax.broadcasted_iota(jnp.int32, (1, NF), 1)
    energies = jnp.zeros((1, NF), jnp.float32)
    for f in range(NF):
        pairs = crecv[f]
        straight = jnp.concatenate([pairs[:, : 2 * NB], pairs[:, 2 * NB :]], axis=0)
        found = jnp.sum(jnp.where(hidden, straight.astype(jnp.float32), 0.0), axis=(0, 1), keepdims=True)
        energies = jnp.where(wide_lane == f, found, energies)
        straight = jnp.where(hidden, jnp.zeros_like(straight), straight)
        crossed = jnp.concatenate([straight[:, NB:], straight[:, :NB]], axis=1)
        stacked = jnp.concatenate([straight * signs, crossed], axis=0)
        out = jnp.dot(stacked, spec[f], preferred_element_type=jnp.float32)
        for c in range(3):
            for o in range(2):
                stage[f % 4, pl.ds(2 * c + o, NB, stride=6), :] = out[o * NB : (o + 1) * NB, c * pw : (c + 1) * pw]
        modes_ref[f * 6 * NB : (f + 1) * 6 * NB, :] = stage[f % 4].astype(jnp.bfloat16)
        part = pl.ds(f * 6 * NB, 6 * NB)
        pltpu.make_async_copy(modes_ref.at[part], modes_hbm.at[part], sem.at[0]).start()
    energy_ref[...] = energies
    last = pltpu.make_async_copy(energy_ref, energy_hbm, sem.at[1])
    last.start()
    pltpu.make_async_copy(modes_ref, modes_hbm, sem.at[0]).wait()
    last.wait()


def fused(n, nf_dev, chosen, snapshots, block_starts, freq_index):
    per, whole, shared, holders = chosen
    rows, count, wide = snapshots.shape
    total = n * nf_dev
    pw = wide // n
    slots = per + 4
    f32, bf16 = jnp.float32, jnp.bfloat16
    dma = pltpu.SemaphoreType.DMA
    vmem = pl.BlockSpec(memory_space=pltpu.VMEM)
    spec, coefs = pl.pallas_call(
        functools.partial(kernel, n, nf_dev, per, whole, shared, holders, float(wide * nf_dev)),
        out_shape=(jax.ShapeDtypeStruct((NF, 2 * NB, 3 * pw), bf16),
                   jax.ShapeDtypeStruct((NF, NB // 2, 4 * NB), bf16)),
        in_specs=[pl.BlockSpec(memory_space=pltpu.HBM)] * 2,
        out_specs=(vmem, vmem),
        scratch_shapes=[
            pltpu.SMEM((NB + NF,), jnp.int32),
            pltpu.VMEM((slots * ROWS, rows), bf16),
            pltpu.VMEM((n // 2, 3, rows, 2 * pw), bf16),
            pltpu.VMEM((n, slots * ROWS, 3 * pw), f32),
            pltpu.VMEM((slots * n, ROWS, 3 * pw), jnp.int16),
            pltpu.VMEM((slots * n, ROWS, 3 * pw), jnp.int16),
            pltpu.VMEM((slots * n // 2, ROWS, 3 * pw), bf16),
            pltpu.VMEM((n, slots, 128), f32),
            pltpu.VMEM((n, slots, 128), f32),
            pltpu.VMEM((slots * n, ROWS, 3 * pw), bf16),
            pltpu.VMEM((NB, ROWS, 3 * pw), bf16),
            pltpu.VMEM((3, NB * (ROWS + 8), pw), f32),
            pltpu.VMEM((NF, NB // 4, 4 * NB), f32),
            pltpu.VMEM((total, NB // 4, 4 * NB), f32),
            pltpu.VMEM((NB // 2, 4 * NB), bf16),
            pltpu.VMEM((NF, NB // 2, 4 * NB), bf16),
            dma((1 + n // 2,)), dma((1,)), dma((n,)), dma((1,)), dma((1,)), dma((1,)), dma((n,)),
            dma((1,)), dma((2,)), dma((1,)), dma((1,)), dma((1,)), dma((1,)),
        ],
        compiler_params=pltpu.CompilerParams(
            collective_id=0, has_side_effects=True, vmem_limit_bytes=54_000_000),
    )(jnp.transpose(snapshots, (1, 0, 2)), jnp.concatenate([block_starts, freq_index]))
    modes, energy = pl.pallas_call(
        finish_kernel,
        out_shape=(jax.ShapeDtypeStruct((NF * NB * 6, pw), bf16), jax.ShapeDtypeStruct((1, NF), f32)),
        in_specs=[vmem, vmem],
        out_specs=[pl.BlockSpec(memory_space=pltpu.HBM)] * 2,
        scratch_shapes=[
            pltpu.VMEM((4, 6 * NB, pw), f32), pltpu.VMEM((NF * NB * 6, pw), bf16),
            pltpu.VMEM((1, NF), f32), dma((2,)),
        ],
        compiler_params=pltpu.CompilerParams(vmem_limit_bytes=8_000_000),
    )(spec, coefs)
    modes = modes.reshape(NF, NB, 3, 2, pw).transpose(0, 1, 3, 2, 4)
    return modes, energy.reshape(NF)


def solution(mesh):
    n, nf_dev = mesh.shape["tm"], mesh.shape["freq"]

    def body(snapshots, block_starts, freq_index):
        rows, _, wide = snapshots.shape
        chosen = plan(n, rows, n * nf_dev, wide // n)
        if chosen is None:
            return local(snapshots, block_starts, freq_index)
        return fused(n, nf_dev, chosen, snapshots, block_starts, freq_index)

    return jax.shard_map(
        body,
        mesh=mesh,
        in_specs=(P("tm", None, "freq"), P(), P()),
        out_specs=(P(None, None, None, None, ("freq", "tm")), P()),
        check_vma=False,
    )
```

```python
import functools
import math

import jax
import jax.numpy as jnp
import numpy as np
from jax import lax
from jax.experimental import pallas as pl
from jax.experimental.pallas import tpu as pltpu
from jax.sharding import PartitionSpec as P

NB = 32
NFFT = 256
NF = 16
NSIT = 6


def for_sending(shard):
    return jax.tree.map(lambda a: a.astype(jnp.bfloat16) if a.dtype == jnp.float32 else a, shard)


def dft_rows(freq_index):
    times_idx = jnp.arange(NFFT, dtype=jnp.int32)
    phase_int = freq_index[:, None] * times_idx[None, :] % NFFT
    angles = 2.0 * math.pi / NFFT * phase_int.astype(jnp.float32)
    window = 0.5 - 0.5 * jnp.cos(2.0 * math.pi / NFFT * times_idx.astype(jnp.float32))
    scaling = 1.0 / jnp.sqrt(jnp.sum(window * window))
    cosine = window[None, :] * jnp.cos(angles) * scaling
    sine_rows = -window[None, :] * jnp.sin(angles) * scaling
    return jnp.stack([cosine, sine_rows], 1).reshape(2 * NF, NFFT).astype(jnp.bfloat16)


def block_rows(block_starts):
    return block_starts[:, None] + jnp.arange(NFFT, dtype=jnp.int32)[None, :]


def matmul_batch(left, right):
    return jnp.einsum("fij,fjk->fik", left, right, precision=lax.Precision.HIGHEST)


def whiten(summed, points):
    gram_re = summed[:, 0]
    gram_im = summed[:, 1]
    top_rows = jnp.concatenate([gram_re, -gram_im], 2)
    low_rows = jnp.concatenate([gram_im, gram_re], 2)
    hermit = jnp.concatenate([top_rows, low_rows], 1)
    frob = jnp.sqrt(jnp.sum(hermit * hermit, axis=(1, 2)) + 1e-06)
    identity = jnp.eye(2 * NB, dtype=jnp.float32)[None]
    iterate = hermit / frob[:, None, None]
    inverse = jnp.broadcast_to(identity, hermit.shape)
    for iteration in range(NSIT):
        factor = 1.5 * identity - 0.5 * matmul_batch(inverse, iterate)
        iterate = matmul_batch(iterate, factor)
        inverse = matmul_batch(factor, inverse)
    columns = inverse[:, :, :NB] * jnp.sqrt(6.0 * points / frob)[:, None, None]
    upper = columns[:, :NB]
    lower = columns[:, NB:]
    coefficients = jnp.stack([jnp.stack([upper, -lower], 1), jnp.stack([lower, upper], 1)], 1)
    energy = jnp.trace(gram_re, axis1=1, axis2=2) / (3.0 * NB * points)
    return (coefficients, energy)


def local(snapshots, block_starts, freq_index):
    dft_table = dft_rows(freq_index)
    offsets = block_rows(block_starts)
    series = lax.all_to_all(snapshots, "tm", split_axis=2, concat_axis=0, tiled=True)
    count = series.shape[1]
    width = series.shape[2]
    columns_all = series.reshape(series.shape[0], count * width)
    windows = jnp.take(columns_all, offsets, axis=0)
    spectra_part = jnp.einsum(
        "rt,btn->rbn", dft_table, windows, preferred_element_type=jnp.float32
    ).astype(jnp.bfloat16)
    spectra = spectra_part.reshape(2 * NF, NB, count, width)
    width = spectra.shape[3]
    points = float(width * lax.axis_size("tm") * lax.axis_size("freq"))
    flat_spec = spectra.reshape(NF, 2, NB, 3 * width)
    real_part = flat_spec[:, 0]
    imag_part = flat_spec[:, 1]
    gram_re = jnp.einsum("fbn,fcn->fbc", real_part, real_part, preferred_element_type=jnp.float32)
    gram_re = gram_re + jnp.einsum(
        "fbn,fcn->fbc", imag_part, imag_part, preferred_element_type=jnp.float32
    )
    cross_terms = jnp.einsum(
        "fbn,fcn->fbc", real_part, imag_part, preferred_element_type=jnp.float32
    )
    partial_gram = jnp.stack([gram_re, cross_terms - jnp.swapaxes(cross_terms, 1, 2)], 1)
    shared = lax.psum_scatter(partial_gram, "freq", scatter_dimension=0, tiled=True)
    shared = lax.psum(shared, "tm")
    coef_part, energy_part = whiten(shared, points)
    coefficients, energy = (
        lax.all_gather(for_sending(coef_part), "freq", axis=0, tiled=True).astype(coef_part.dtype),
        lax.all_gather(for_sending(energy_part), "freq", axis=0, tiled=True).astype(
            energy_part.dtype
        ),
    )
    coef_bf = jnp.transpose(coefficients.astype(jnp.bfloat16), (0, 4, 1, 2, 3))
    modes = jnp.einsum(
        "fjorb,frbn->fjon", coef_bf, flat_spec, preferred_element_type=jnp.float32
    ).astype(jnp.bfloat16)
    return (modes.reshape(NF, NB, 2, 3, width), energy)


MESH = pl.DeviceIdType.MESH
ROWS = 2 * NF
HOP = 128
JIT = 64


def plan(n, rows, total, width):
    if n % 4 or NB % n or total % (2 * NF) or width != 128 or rows % 16:
        return None
    per = NB // n
    if per < 4 or per % 2:
        return None
    slots = per + 4
    whole = [[] for _ in range(slots)]
    shared = [[] for _ in range(slots)]
    holders = []
    for block in range(NB):
        touched = [
            dev for dev in range(n)
            if HOP * block < rows * (dev + 1) and HOP * block + JIT + NFFT > rows * dev
        ]
        holders.append(touched)
        if len(touched) > 2:
            return None
        for dev in touched:
            slot = block - per * dev + 2
            if not 0 <= slot < slots:
                return None
            if len(touched) == 2:
                if (slot < slots // 2) != (dev == touched[1]):
                    return None
                shared[slot].append(dev)
            else:
                whole[slot].append(dev)
    return per, whole, shared, holders


def base_table(ints_ref):
    row = lax.broadcasted_iota(jnp.int32, (ROWS, NFFT), 0)
    times_idx = lax.broadcasted_iota(jnp.int32, (ROWS, NFFT), 1)
    freqs = jnp.zeros((ROWS, NFFT), jnp.int32)
    for f in range(NF):
        freqs = jnp.where((row >> 1) == f, ints_ref[NB + f], freqs)
    phase = (freqs * times_idx) & (NFFT - 1)
    angles = 2.0 * math.pi / NFFT * phase.astype(jnp.float32)
    window = 0.5 - 0.5 * jnp.cos(2.0 * math.pi / NFFT * times_idx.astype(jnp.float32))
    hann = 0.5 - 0.5 * np.cos(2.0 * math.pi / NFFT * np.arange(NFFT))
    scaling = np.float32(1.0 / np.sqrt(np.sum(hann * hann)))
    cosine = window * jnp.cos(angles) * scaling
    sine = -window * jnp.sin(angles) * scaling
    return jnp.where((row & 1) == 1, sine, cosine).astype(jnp.bfloat16)


def shifted(base, shift, rows):
    source = lax.broadcasted_iota(jnp.int32, (NFFT, rows), 0)
    target = lax.broadcasted_iota(jnp.int32, (NFFT, rows), 1)
    pick = jnp.where(source - target == shift, 1.0, 0.0).astype(jnp.bfloat16)
    return jnp.dot(base, pick, preferred_element_type=jnp.float32).astype(jnp.bfloat16)


def member(index, devs):
    if not devs:
        return None
    if devs == list(range(devs[0], devs[-1] + 1)):
        return (index >= devs[0]) & (index <= devs[-1])
    hit = index == devs[0]
    for dev in devs[1:]:
        hit = hit | (index == dev)
    return hit


def division(n, tm, side, dest):
    edge, half = tm + side, n // 2
    middle = edge == half
    left = dest < half
    all_mine = middle & (left == (tm < half))
    theirs = (middle & (all_mine ^ True)) | ((middle ^ True) & (dest % 2 != tm % 2))
    return theirs, middle, all_mine


def kernel(n, nf_dev, per, whole, shared, holders, points, x_hbm, ints_hbm,
           spec, coefs_ref, ints_ref, t_ref, xv, parts,
           sendp, others, relayb, scales, oscales, sendb, recvb, spec32, gpart, gath, msg, crecv,
           load_sem, psend, precv, rrecv, fsend, ssend, srecv, asend, arecv, gsend, grecv, csend, crcv):
    tm = lax.axis_index("tm")
    fr = lax.axis_index("freq")
    total = n * nf_dev
    lin = tm * nf_dev + fr
    step, lowest = total // (2 * NF), total // 4
    slots = per + 4
    half_slots = slots // 2
    mine = (lin - lowest) // step
    owns = (lin >= lowest) & (lin < lowest + NF * step) & ((lin - lowest) % step == 0)
    half_n = n // 2
    parity = tm % 2
    rows = xv.shape[2]
    pw = xv.shape[3] // 2

    def owner(f):
        return lowest + f * step

    def where_is(index):
        return {"tm": index // nf_dev, "freq": index % nf_dev}

    def displaced(away):
        row, col = tm + away // nf_dev, fr + away % nf_dev
        return {"tm": jnp.where(row >= n, row - n, row),
                "freq": jnp.where(col >= nf_dev, col - nf_dev, col)}

    def group(k):
        return jnp.where(tm < half_n, half_n - 1 - k, k)

    def load(g, c):
        return pltpu.make_async_copy(
            x_hbm.at[c, :, pl.ds(pl.multiple_of(g * 2 * pw, 2 * pw), 2 * pw)], xv.at[g, c],
            load_sem.at[1 + g])

    small = pltpu.make_async_copy(ints_hbm, ints_ref, load_sem.at[0])
    small.start()
    for k in range(half_n):
        for c in range(3):
            load(group(k), c).start()
    barrier = pltpu.get_barrier_semaphore()

    for away in range(total - 1, 0, -1):
        pl.semaphore_signal(barrier, inc=1, device_id=displaced(away), device_id_type=MESH)

    small.wait()
    base = base_table(ints_ref)
    for slot in range(slots):
        block = per * tm + slot - 2
        start = ints_ref[jnp.clip(block, 0, NB - 1)]
        inside = (block >= 0) & (block < NB)
        shift = jnp.where(inside, rows * tm - start, 4 * (rows + NFFT))
        t_ref[slot * ROWS : (slot + 1) * ROWS, :] = shifted(base, shift, rows)
    scales[...] = jnp.zeros_like(scales)

    def low(slot):
        return slot < half_slots

    def pick(flag, yes, no):
        return (yes if flag else no) if isinstance(flag, bool) else jnp.where(flag, yes, no)

    def partner(slot):
        return pick(low(slot), (tm + n - 1) % n, (tm + 1) % n)

    def across(slot):
        return pick(low(slot), slot + per, slot - per)

    def is_shared(slot):
        block = per * tm + slot - 2
        edge = rows * (tm + pick(low(slot), 0, 1))
        inside = (block >= 0) & (block < NB) & (edge > 0) & (edge < rows * n)
        return inside & (HOP * block < edge) & (HOP * block + JIT + NFFT > edge)

    def is_theirs(slot, dest):
        return division(n, tm, slot // half_slots, dest)[0]

    def exchange(slot, length, dest):
        return pltpu.make_async_remote_copy(
            src_ref=sendp.at[pl.ds(dest * slots + slot, length)],
            dst_ref=others.at[pl.ds(dest * slots + across(slot), length)],
            send_sem=psend.at[0], recv_sem=precv.at[across(slot) // half_slots * half_n + dest // 2],
            device_id={"tm": partner(slot), "freq": fr}, device_id_type=MESH)

    def scale_copy(side, g):
        return pltpu.make_async_remote_copy(
            src_ref=scales.at[side * half_n + g], dst_ref=oscales.at[(1 - side) * half_n + g],
            send_sem=ssend.at[0], recv_sem=srecv.at[(1 - side) * half_n + g],
            device_id={"tm": partner(side * half_slots), "freq": fr}, device_id_type=MESH)

    def scatter(slot, length, dest):
        block = per * tm + slot - 2
        return pltpu.make_async_remote_copy(
            src_ref=sendb.at[pl.ds(dest * slots + slot, length)], dst_ref=recvb.at[pl.ds(block, length)],
            send_sem=asend.at[0], recv_sem=arecv.at[0],
            device_id={"tm": dest, "freq": fr}, device_id_type=MESH)

    def settle(ref, sem):
        pltpu.make_async_copy(ref, ref, sem).wait()

    def settle_count(ref, count, sem, options):
        for option in sorted(set(options)):
            @pl.when(count == option)
            def _(option=option):
                settle(ref.at[pl.ds(0, option)], sem)

    def edge_exists(side):
        return pick(side == 0, tm > 0, tm < n - 1)

    def sharing(side):
        return sum(jnp.where(is_shared(side * half_slots + k), 1, 0) for k in range(half_slots))

    def put(slot, dest, value):
        value = value.astype(jnp.bfloat16)

        @pl.when(dest == tm)
        def _():
            recvb[per * tm + slot - 2] = value

        @pl.when(dest != tm)
        def _():
            sendb[dest * slots + slot] = value

    def first_shared(side):
        flags = [is_shared(side * half_slots + k) for k in range(half_slots)]
        first = half_slots - 1
        for k in range(half_slots - 2, -1, -1):
            first = jnp.where(flags[k], k, first)
        return side * half_slots + first

    def runs(table):
        found = {}
        for tm_at in range(n):
            slot = 0
            while slot < slots:
                length = 0
                while slot + length < slots and tm_at in table[slot + length]:
                    length += 1
                if length:
                    found.setdefault((slot, length), []).append(tm_at)
                slot += length + 1
        return found

    def hops(dest):
        return ((tm == 1) & (dest >= half_n)) | ((tm == n - 2) & (dest < half_n))

    def relay_rank(dest):
        return dest // 2 % (half_n // 2)

    def to_relay(first, length, place, dest):
        return pltpu.make_async_remote_copy(
            src_ref=sendb.at[pl.ds(dest * slots + first, length)], dst_ref=relayb.at[pl.ds(place, length)],
            send_sem=asend.at[0], recv_sem=rrecv.at[0],
            device_id={"tm": tm + 1 - 2 * parity, "freq": fr}, device_id_type=MESH)

    def relay_runs(source):
        placed, place = [], 0
        for (first, length), devs in runs(whole).items():
            if source in devs:
                placed.append((first, length, place))
                place += length * (half_n // 2)
        return placed, place

    def send_to_relay(dest):
        for source in (1, n - 2):
            @pl.when((tm == source) & hops(dest))
            def _(source=source):
                for first, length, place in relay_runs(source)[0]:
                    for slot in range(first, first + length):
                        sendb[dest * slots + slot] = parts[dest, slot * ROWS : (slot + 1) * ROWS, :].astype(jnp.bfloat16)
                    to_relay(first, length, place + length * relay_rank(dest), dest).start()

    def relay():
        for me, source in ((0, 1), (n - 1, n - 2)):
            @pl.when(tm == me)
            def _(source=source):
                placed, amount = relay_runs(source)
                settle(relayb.at[pl.ds(0, amount)], rrecv.at[0])
                for first, length, place in placed:
                    for rank in range(half_n // 2):
                        dest = 2 * rank + (half_n if source == 1 else 0) + 1 - source % 2
                        spot = place + length * rank
                        pltpu.make_async_remote_copy(
                            src_ref=relayb.at[pl.ds(spot, length)],
                            dst_ref=recvb.at[pl.ds(per * source + first - 2, length)],
                            send_sem=fsend.at[0], recv_sem=arecv.at[0],
                            device_id={"tm": dest, "freq": fr}, device_id_type=MESH).start()

    def send_whole(dest, chosen):
        for (first, length), devs in runs(whole).items():
            @pl.when(member(tm, devs) & chosen)
            def _(first=first, length=length):
                for slot in range(first, first + length):
                    put(slot, dest, parts[dest, slot * ROWS : (slot + 1) * ROWS, :])

                @pl.when(dest != tm)
                def _():
                    scatter(first, length, dest).start()

    diagonal = (lax.broadcasted_iota(jnp.int32, (ROWS, 128), 0)
                == lax.broadcasted_iota(jnp.int32, (ROWS, 128), 1))

    def encode(slot, g, d):
        value = parts[2 * g + d, slot * ROWS : (slot + 1) * ROWS, :]
        peak = jnp.maximum(jnp.max(jnp.abs(value), axis=1, keepdims=True), 1e-30)
        whole_numbers = (value * (32767.0 / peak) + 12582912.0) - 12582912.0
        sendp[(2 * g + d) * slots + slot] = whole_numbers.astype(jnp.int32).astype(jnp.int16)
        line = jnp.sum(jnp.where(diagonal, peak, 0.0), axis=0, keepdims=True)
        row = 2 * (slot % half_slots) + d
        scales[slot // half_slots * half_n + g, row : row + 1, :] = line

    lengths = sorted({sum(tm_at in devs for devs in shared[side * half_slots : (side + 1) * half_slots])
                      for tm_at in range(n) for side in range(2)} - {0})

    @pl.loop(0, half_n)
    def _(k):
        g = group(k)
        settle(xv.at[g], load_sem.at[1 + g])
        for c in range(3):
            part = jnp.dot(t_ref[...], xv[g, c], preferred_element_type=jnp.float32)
            for d in range(2):
                parts[2 * g + d, :, c * pw : (c + 1) * pw] = part[:, d * pw : (d + 1) * pw]

        for d in range(2):
            for slot in range(slots):
                if shared[slot]:
                    @pl.when(member(tm, shared[slot]) & is_theirs(slot, 2 * g + d))
                    def _(slot=slot, d=d):
                        encode(slot, g, d)

        @pl.when(k == 0)
        def _():
            pl.semaphore_wait(barrier, total - 1)

        for side in range(2):
            _, whole_group, all_mine = division(n, tm, side, 2 * g)

            @pl.when(edge_exists(side) & jnp.logical_not(whole_group & all_mine))
            def _(side=side):
                scale_copy(side, g).start()

        def send_codes(want):
            for side in range(2):
                for d in range(2):
                    theirs = division(n, tm, side, 2 * g + d)[0]
                    for length in lengths:
                        @pl.when(edge_exists(side) & theirs & (parity == (want ^ side)) & (sharing(side) == length))
                        def _(side=side, d=d, length=length):
                            exchange(first_shared(side), length, 2 * g + d).start()

        send_codes(1)
        send_to_relay(2 * g + 1 - parity)
        for d in range(2):
            send_whole(2 * g + d, parity == d)
        send_codes(0)

    def send_crossing():
        @pl.loop(0, half_n)
        def _(k):
            dest = 2 * group(k) + 1 - parity
            send_whole(dest, jnp.logical_not(hops(dest)))

    counts = [sum(tm_at in devs for devs in shared) for tm_at in range(n)]

    @pl.loop(0, 2)
    def _(turn):
        side = jnp.where(turn == 0, 1 - parity, parity)

        @pl.loop(0, half_n)
        def _(k):
            g = group(k)
            _, whole_group, all_mine = division(n, tm, side, 2 * g)

            @pl.when(edge_exists(side) & (jnp.logical_not(whole_group) | all_mine))
            def _():
                settle(oscales.at[side * half_n + g], srecv.at[side * half_n + g])
                settle_count(others, sharing(side) * jnp.where(whole_group, 2, 1), precv.at[side * half_n + g],
                             [count * twice for count in range(1, half_slots + 1) for twice in (1, 2)])
                for d in range(2):
                    dest = 2 * g + d
                    for index in range(half_slots):
                        slot = side * half_slots + index

                        @pl.when(is_shared(slot) & jnp.logical_not(is_theirs(slot, dest)))
                        def _(slot=slot, dest=dest, row=2 * index + d):
                            line = oscales[side * half_n + g, row : row + 1, :]
                            peak = jnp.sum(jnp.where(diagonal, line, 0.0), axis=1, keepdims=True)
                            other = others[dest * slots + slot].astype(jnp.int32).astype(jnp.float32)
                            here = parts[dest, pl.ds(pl.multiple_of(slot * ROWS, ROWS), ROWS), :]
                            put(slot, dest, here + other * (peak * (1.0 / 32767.0)))

                    mine_here = jnp.logical_not(division(n, tm, side, dest)[0]) & (dest != tm)
                    for length in lengths:
                        @pl.when(mine_here & (sharing(side) == length))
                        def _(length=length, dest=dest):
                            scatter(first_shared(side), length, dest).start()


            @pl.when((turn == 0) & (k == 0))
            def _():
                relay()

            @pl.when((turn == 0) & (k == 0))
            def _():
                send_crossing()

    alone = [sum(tm_at in devs for devs in whole) for tm_at in range(n)]
    pitch = spec32.shape[1] // NB
    missing = [NB - alone[tm_at] - counts[tm_at] for tm_at in range(n)]
    settle_count(recvb, sum(jnp.where(tm == tm_at, missing[tm_at], 0) for tm_at in range(n)), arecv.at[0], missing)
    for block in range(NB):
        values = recvb[block]
        for c in range(3):
            spec32[c, block * pitch : block * pitch + ROWS, :] = values[:, c * 128 : (c + 1) * 128].astype(jnp.float32)
    for f in range(NF):
        for r in range(2):
            spec[f, r * NB : (r + 1) * NB, :] = jnp.concatenate([
                spec32[c, pl.ds(2 * f + r, NB, stride=pitch), :].astype(jnp.bfloat16)
                for c in range(3)], axis=1)

    def to_owner(k):
        first, last = owner(NF - 1 - k), owner(k)
        near_start = tm < half_n
        f = jnp.where(near_start, NF - 1 - k, k)
        place = {"tm": jnp.where(near_start, first // nf_dev, last // nf_dev),
                 "freq": jnp.where(near_start, first % nf_dev, last % nf_dev)}
        return f, pltpu.make_async_remote_copy(
            src_ref=gpart.at[f], dst_ref=gath.at[lin], send_sem=gsend.at[0],
            recv_sem=grecv.at[0], device_id=place, device_id_type=MESH)

    upper = lax.broadcasted_iota(jnp.int32, (NB, NB), 1) >= lax.broadcasted_iota(jnp.int32, (NB, NB), 0)
    for f in range(NF):
        real, imag = spec[f, :NB, :], spec[f, NB:, :]
        lhs = jnp.concatenate([real, imag], axis=1)
        rhs = jnp.concatenate([lhs, jnp.concatenate([imag, -real], axis=1)], axis=0)
        gram = lax.dot_general(lhs, rhs, (((1,), (1,)), ((), ())), preferred_element_type=jnp.float32)
        packed = jnp.where(upper, gram[:, :NB], gram[:, NB:])
        gpart[f] = jnp.concatenate([packed[8 * q : 8 * q + 8] for q in range(NB // 8)], axis=1)
        if f % 16 == 15:
            for sent in range(f - 15, f + 1):
                target, copy = to_owner(sent)

                @pl.when(lin != owner(target))
                def _(copy=copy):
                    copy.start()

    def coef_to(away):
        return pltpu.make_async_remote_copy(
            src_ref=msg, dst_ref=crecv.at[mine], send_sem=csend.at[0],
            recv_sem=crcv.at[0], device_id=displaced(away), device_id_type=MESH)

    @pl.when(owns)
    def _():
        gath[lin] = gpart[mine]

        settle(gath.at[pl.ds(0, total - 1)], grecv.at[0])
        packed = jnp.sum(gath[...], axis=0)
        square = jnp.concatenate([packed[:, q * NB : (q + 1) * NB] for q in range(NB // 8)], axis=0)
        flipped = jnp.transpose(square)
        ri = lax.broadcasted_iota(jnp.int32, (NB, NB), 0)
        ci = lax.broadcasted_iota(jnp.int32, (NB, NB), 1)
        gram_re = jnp.where(ci >= ri, square, flipped)
        gram_im = jnp.where(ci < ri, square, jnp.where(ci > ri, -flipped, 0.0))
        energy = jnp.sum(jnp.where(ri == ci, gram_re, 0.0), axis=(0, 1), keepdims=True) / (3.0 * NB * points)
        hermit = jnp.concatenate([
            jnp.concatenate([gram_re, -gram_im, gram_re, -gram_im], axis=1),
            jnp.concatenate([gram_im, gram_re, gram_im, gram_re], axis=1)], axis=0)
        frob = jnp.sqrt(0.5 * jnp.sum(hermit * hermit, axis=(0, 1), keepdims=True) + 1e-06)
        ri = lax.broadcasted_iota(jnp.int32, (2 * NB, 4 * NB), 0)
        ci = lax.broadcasted_iota(jnp.int32, (2 * NB, 4 * NB), 1)
        left = ci < 2 * NB
        identity = jnp.where(ri == (ci & (2 * NB - 1)), 1.0, 0.0).astype(jnp.float32)

        def pieces(a):
            high = a.astype(jnp.bfloat16)
            rest = a - high.astype(jnp.float32)
            mid = rest.astype(jnp.bfloat16)
            return high, mid, (rest - mid.astype(jnp.float32)).astype(jnp.bfloat16)

        def mul(a, b):
            ah, am, al = a
            bh, bm, bl = b
            lhs = jnp.concatenate([ah, am, jnp.where(left[: ah.shape[0]], ah, al)], axis=1)
            rhs = jnp.concatenate([bh, bm, bh, bm, bl, bh], axis=0)
            return jnp.dot(lhs, rhs, preferred_element_type=jnp.float32)

        iterate = hermit / frob
        inverse = identity
        for step in range(NSIT):
            it = pieces(iterate)
            if step:
                inv = pieces(inverse)
            factor = 1.5 * identity - 0.5 * (mul(inv, it) if step else iterate)
            fac = pieces(factor)
            if step < NSIT - 1:
                iterate = mul(it, fac)
                inverse = mul(fac, inv) if step else factor
            else:
                inverse = mul(tuple(piece[:NB] for piece in fac), inv)
        scaled = inverse * jnp.sqrt(6.0 * points / frob)
        high, mid, rest = [piece.astype(jnp.float32) for piece in pieces(energy)]
        top = ri[:NB]
        extra = jnp.where(top == 0, high, jnp.where(top == 1, mid, jnp.where(top == 2, rest, 0.0)))
        scaled = jnp.where((ci[:NB] & (2 * NB - 1)) == NB + top, extra, scaled)
        msg[...] = jnp.where(left[: NB // 2], scaled[: NB // 2], scaled[NB // 2 :]).astype(jnp.bfloat16)
        crecv[mine] = msg[...]

        for away in range(total - 1, 0, -1):
            coef_to(away).start()

    for tm_at in range(n):
        handed, groups = 0, 0
        for slot in range(slots):
            if tm_at in shared[slot]:
                handed += sum(division(n, tm_at, slot // half_slots, dest)[0] for dest in range(n))
        for side in range(2):
            if 0 < tm_at + side < n:
                for g in range(half_n):
                    _, whole_group, all_mine = division(n, tm_at, side, 2 * g)
                    groups += not (whole_group and all_mine)

        @pl.when(tm == tm_at)
        def _(tm_at=tm_at, handed=handed, groups=groups):
            settle(sendp.at[pl.ds(0, handed)], psend.at[0])
            own = n * (alone[tm_at] + counts[tm_at]) - handed
            settle(sendb.at[pl.ds(0, own - alone[tm_at] - counts[tm_at])], asend.at[0])
            settle(scales.at[pl.ds(0, groups)], ssend.at[0])
            if tm_at in (0, n - 1):
                settle(relayb.at[pl.ds(0, relay_runs(1 if tm_at == 0 else n - 2)[1])], fsend.at[0])

    sent = jnp.where(owns, NF - 1, NF)
    settle_count(gpart, sent, gsend.at[0], [NF - 1, NF])
    settle_count(crecv, sent, crcv.at[0], [NF - 1, NF])
    coefs_ref[...] = crecv[...]

    @pl.when(owns)
    def _():
        settle(gath.at[pl.ds(0, total - 1)], csend.at[0])


def finish_kernel(spec, crecv, modes_hbm, energy_hbm, stage, modes_ref, energy_ref, sem):
    pw = modes_ref.shape[1]

    lanes = lax.broadcasted_iota(jnp.int32, (NB, 2 * NB), 1)
    signs = jnp.where(lanes < NB, 1.0, -1.0).astype(jnp.bfloat16)
    hidden = lanes == NB + lax.broadcasted_iota(jnp.int32, (NB, 2 * NB), 0)
    tall_row = lax.broadcasted_iota(jnp.int32, (NF, 2 * NB), 0)
    energies = jnp.zeros((NF, 2 * NB), jnp.float32)
    for f in range(NF):
        pairs = crecv[f]
        straight = jnp.concatenate([pairs[:, : 2 * NB], pairs[:, 2 * NB :]], axis=0)
        found = jnp.sum(jnp.where(hidden, straight.astype(jnp.float32), 0.0), axis=0, keepdims=True)
        energies = jnp.where(tall_row == f, found, energies)
        straight = jnp.where(hidden, jnp.zeros_like(straight), straight)
        crossed = jnp.concatenate([straight[:, NB:], straight[:, :NB]], axis=1)
        stacked = jnp.concatenate([straight * signs, crossed], axis=0)
        out = jnp.dot(stacked, spec[f], preferred_element_type=jnp.float32)
        for c in range(3):
            for o in range(2):
                stage[f % 4, pl.ds(2 * c + o, NB, stride=6), :] = out[o * NB : (o + 1) * NB, c * pw : (c + 1) * pw]
        modes_ref[f * 6 * NB : (f + 1) * 6 * NB, :] = stage[f % 4].astype(jnp.bfloat16)
        part = pl.ds(f * 6 * NB, 6 * NB)
        pltpu.make_async_copy(modes_ref.at[part], modes_hbm.at[part], sem.at[0]).start()
    column = jnp.sum(energies, axis=1, keepdims=True)
    square = lax.broadcasted_iota(jnp.int32, (NF, NF), 0) == lax.broadcasted_iota(jnp.int32, (NF, NF), 1)
    energy_ref[...] = jnp.sum(jnp.where(square, column, 0.0), axis=0, keepdims=True)
    last = pltpu.make_async_copy(energy_ref, energy_hbm, sem.at[1])
    last.start()
    pltpu.make_async_copy(modes_ref, modes_hbm, sem.at[0]).wait()
    last.wait()


def fused(n, nf_dev, chosen, snapshots, block_starts, freq_index):
    per, whole, shared, holders = chosen
    rows, count, wide = snapshots.shape
    total = n * nf_dev
    pw = wide // n
    slots = per + 4
    f32, bf16 = jnp.float32, jnp.bfloat16
    dma = pltpu.SemaphoreType.DMA
    vmem = pl.BlockSpec(memory_space=pltpu.VMEM)
    spec, coefs = pl.pallas_call(
        functools.partial(kernel, n, nf_dev, per, whole, shared, holders, float(wide * nf_dev)),
        out_shape=(jax.ShapeDtypeStruct((NF, 2 * NB, 3 * pw), bf16),
                   jax.ShapeDtypeStruct((NF, NB // 2, 4 * NB), bf16)),
        in_specs=[pl.BlockSpec(memory_space=pltpu.HBM)] * 2,
        out_specs=(vmem, vmem),
        scratch_shapes=[
            pltpu.SMEM((NB + NF,), jnp.int32),
            pltpu.VMEM((slots * ROWS, rows), bf16),
            pltpu.VMEM((n // 2, 3, rows, 2 * pw), bf16),
            pltpu.VMEM((n, slots * ROWS, 3 * pw), f32),
            pltpu.VMEM((slots * n, ROWS, 3 * pw), jnp.int16),
            pltpu.VMEM((slots * n, ROWS, 3 * pw), jnp.int16),
            pltpu.VMEM((slots * n // 2, ROWS, 3 * pw), bf16),
            pltpu.VMEM((n, slots, 128), f32),
            pltpu.VMEM((n, slots, 128), f32),
            pltpu.VMEM((slots * n, ROWS, 3 * pw), bf16),
            pltpu.VMEM((NB, ROWS, 3 * pw), bf16),
            pltpu.VMEM((3, NB * (ROWS + 8), pw), f32),
            pltpu.VMEM((NF, NB // 4, 4 * NB), f32),
            pltpu.VMEM((total, NB // 4, 4 * NB), f32),
            pltpu.VMEM((NB // 2, 4 * NB), bf16),
            pltpu.VMEM((NF, NB // 2, 4 * NB), bf16),
            dma((1 + n // 2,)), dma((1,)), dma((n,)), dma((1,)), dma((1,)), dma((1,)), dma((n,)),
            dma((1,)), dma((1,)), dma((1,)), dma((1,)), dma((1,)), dma((1,)),
        ],
        compiler_params=pltpu.CompilerParams(
            collective_id=0, has_side_effects=True, vmem_limit_bytes=54_000_000),
    )(jnp.transpose(snapshots, (1, 0, 2)), jnp.concatenate([block_starts, freq_index]))
    modes, energy = pl.pallas_call(
        finish_kernel,
        out_shape=(jax.ShapeDtypeStruct((NF * NB * 6, pw), bf16), jax.ShapeDtypeStruct((1, NF), f32)),
        in_specs=[vmem, vmem],
        out_specs=[pl.BlockSpec(memory_space=pltpu.HBM)] * 2,
        scratch_shapes=[
            pltpu.VMEM((4, 6 * NB, pw), f32), pltpu.VMEM((NF * NB * 6, pw), bf16),
            pltpu.VMEM((1, NF), f32), dma((2,)),
        ],
        compiler_params=pltpu.CompilerParams(vmem_limit_bytes=8_000_000),
    )(spec, coefs)
    modes = modes.reshape(NF, NB, 3, 2, pw).transpose(0, 1, 3, 2, 4)
    return modes, energy.reshape(NF)


def solution(mesh):
    n, nf_dev = mesh.shape["tm"], mesh.shape["freq"]

    def body(snapshots, block_starts, freq_index):
        rows, _, wide = snapshots.shape
        chosen = plan(n, rows, n * nf_dev, wide // n)
        if chosen is None:
            return local(snapshots, block_starts, freq_index)
        return fused(n, nf_dev, chosen, snapshots, block_starts, freq_index)

    return jax.shard_map(
        body,
        mesh=mesh,
        in_specs=(P("tm", None, "freq"), P(), P()),
        out_specs=(P(None, None, None, None, ("freq", "tm")), P()),
        check_vma=False,
    )
```
